32 devices in a mesh: row: 8 (over y, x, core), col: 4 (over z).
Axes of the slice: x: 2, y: 2, z: 4, core: 2. Of those that a mesh axis runs over, the one named last changes fastest.
Arguments:
- design: bfloat16 [4096, 6144], P(('row', 'col')), may hold values from -0.09375 to 0.09375
- observations: float32 [4096], P(('row', 'col')), may hold values from -6 to 6
- gaps: int32 [4096], P(('row', 'col')), may hold values 0 or 1
- noise_var: float32 [4096], P(('row', 'col')), may hold values from 0.25 to 4
- arc_lengths: int32 [32, 4], P(('row', 'col')), may hold values from 1 to 64, 128 in all within a row
- arc_amp: float32 [32, 4], P(('row', 'col')), may hold values from 0.2 to 2
- arc_decay: float32 [32, 4], P(('row', 'col')), may hold values from 0.3 to 0.95
- plan: int32 [32], P(('row', 'col')), may hold values from 0 to 31, each once
- tile_map: int32 [48], replicated, may hold values from 0 to 47, each once
Outputs:
- gram: float32 [6144, 6144], P('row', 'col')
- normal_rhs: float32 [6144], P('row')
- balanced_obs: float32 [32, 128], P(('row', 'col'))
The draws below stay inside these ranges and needn't reach their ends.
Inputs may be any that keep to these rules, and one draw needn't show every extreme that they name: `plan`: a permutation of the blocks. `tile_map`: a permutation of the tiles. `arc_lengths`: each block's arc lengths sum to 128; some arc has 64 rows.
All inputs are finite; a program needn't handle non-finite values. No bound on the sum of `gaps` on one device may be relied on, other than what follows from the above.
Results may differ from the reference program's by a relative error of at most 0.004.
Values may be sent and summed in bfloat16 or wider, within the bound.
No kernel may reach another device: no remote copies, remote signals or barrier semaphores. Data moves between devices by JAX's collectives and lax.ppermute only.
A program may use at most 192 MiB of HBM per device.

```python
import math
import jax
import jax.numpy as jnp
import numpy as np
from jax import lax

U = 6144
TB = 128
SB = 128
ARCS = 4
MAXARC = 64
BLOCKS = 32
ROWS = 4096


def set_ends(values, rng, low, high):
    longest = values.shape.index(max(values.shape))
    spots = []
    for shift in (0, 1):
        where = [jax.random.randint(jax.random.fold_in(rng, axis), (), 0, length) for axis, length in enumerate(values.shape)]
        where[longest] = (where[longest] + shift) % values.shape[longest]
        spots.append(tuple(where))
    return values.at[spots[0]].set(low).at[spots[1]].set(high)


def level_of(rng, shape, cuts, smallest, high):
    factor_of, own = 1.0, jax.random.fold_in(rng, 6)
    for dim, blocks in cuts:
        draws = jnp.exp(jax.random.uniform(jax.random.fold_in(own, dim), (blocks,), jnp.float32, smallest / len(cuts), high / len(cuts)))
        factor_of = factor_of * jnp.repeat(draws, shape[dim] // blocks).reshape([-1 if axis == dim else 1 for axis in range(len(shape))])
    return factor_of


def profile(count, total, reach, slope):
    weights = [(1 << 20) // math.isqrt(grade ** slope) + 1 for grade in range(2, count + 1)]
    rest, given = total - reach - (count - 1), [1] * (count - 1)
    while rest > 0:
        candidates = [i for i in range(count - 1) if given[i] < reach]
        mass, budget = sum([weights[i] for i in candidates]), rest
        for i in candidates:
            extra = min(reach - given[i], max(1, budget * weights[i] // mass), rest)
            given[i] = given[i] + extra
            rest = rest - extra
    return np.array([reach] + given)


def uneven_parts(own_key, count, total, bound, skew):
    if count == 2:
        one = jax.random.randint(own_key, (), max(1, total - bound), min(bound, total - 1) + 1)
        return jnp.stack([one, total - one])
    sizes = jnp.asarray(profile(count, total, bound, skew), jnp.int32)
    pairs = (count - 1) // 2
    giver, receiver = sizes[1:1 + 2 * pairs:2], sizes[2:2 + 2 * pairs:2]
    room = jnp.minimum(giver - 1, bound - receiver)
    shifted = jax.random.randint(jax.random.fold_in(own_key, 1), (pairs,), 0, 1 << 20) % (room + 1)
    sizes = sizes.at[1:1 + 2 * pairs:2].set(giver - shifted).at[2:2 + 2 * pairs:2].set(receiver + shifted)
    return sizes[jax.random.permutation(jax.random.fold_in(own_key, 2), count)]


def gaussian(key, dims, deviation, most, split=(), held_as=jnp.bfloat16):
    array = jax.random.normal(key, dims, jnp.float32) * deviation
    if len(split) > 0:
        array = level_of(key, dims, split, -0.22, 0.18) * array
    return jnp.clip(array, min=-most, max=most).astype(held_as)


def setup_inputs(seed: int = 0) -> dict:
    key_list = jax.random.split(jax.random.key(seed), 10)
    return {
        "design": gaussian(key_list[0], (ROWS, U), (ROWS ** -0.5), 0.09375, ((0, 32),)),
        "observations": gaussian(key_list[1], (ROWS,), 1.0, 6.0, ((0, 32),), jnp.float32),
        "gaps": set_ends((jax.random.randint(key_list[2], (ROWS,), 0, 8) < 7).astype(jnp.int32), jax.random.fold_in(key_list[2], 1), 0, 1),
        "noise_var": jnp.clip(jnp.exp(math.log(4.0) - 2.7725887 * jax.random.uniform(key_list[3], (ROWS,), jnp.float32) ** level_of(key_list[3], (ROWS,), ((0, 32),), -0.2, 0.2)), 0.25, 4.0),
        "arc_lengths": jax.vmap(lambda own: uneven_parts(own, ARCS, SB, MAXARC, 2))(jax.random.split(key_list[4], BLOCKS)).reshape((BLOCKS, ARCS)).astype(jnp.int32),
        "arc_amp": jnp.clip(jnp.exp(math.log(2.0) - 2.3025851 * jax.random.uniform(key_list[5], (BLOCKS, ARCS), jnp.float32) ** level_of(key_list[5], (BLOCKS, ARCS), ((0, 32),), -0.2, 0.2)), 0.2, 2.0),
        "arc_decay": jnp.clip(0.3 + 0.65 * jax.random.uniform(key_list[6], (BLOCKS, ARCS), jnp.float32) ** level_of(key_list[6], (BLOCKS, ARCS), ((0, 32),), -0.2, 0.2), 0.3, 0.95),
        "plan": jax.random.permutation(key_list[7], BLOCKS).astype(jnp.int32),
        "tile_map": jax.random.permutation(key_list[8], U // TB).astype(jnp.int32),
    }


def whiten(block, obs_rows, live_rows, noise_rows, lengths, amplitude, decay):
    block_rows = block.shape[0]
    arc_count = lengths.shape[0]
    position = jnp.arange(block_rows, dtype=jnp.int32)
    arc_ends = jnp.cumsum(lengths).astype(jnp.int32)
    arc_id = jnp.sum((arc_ends[None, :] <= position[:, None]).astype(jnp.int32), axis=1)
    member = (arc_id[:, None] == jnp.arange(arc_count, dtype=jnp.int32)[None, :]).astype(jnp.float32)
    row_amp = jnp.sum(member * amplitude[None, :], axis=1)
    row_rate = jnp.sum(member * jnp.log(decay)[None, :], axis=1)
    same_arc = (arc_id[:, None] == arc_id[None, :]).astype(jnp.float32)
    row_lag = jnp.abs(position[:, None] - position[None, :]).astype(jnp.float32)
    kernel = row_amp[:, None] * jnp.exp(row_lag * row_rate[:, None]) * same_arc * live_rows[:, None] * live_rows[None, :]
    covariance = kernel + jnp.diag(noise_rows)
    factor = jnp.linalg.cholesky(covariance)
    solved = lax.linalg.triangular_solve(factor, block.astype(jnp.float32) * live_rows[:, None], left_side=True, lower=True)
    solved_obs = lax.linalg.triangular_solve(factor, (obs_rows * live_rows)[:, None], left_side=True, lower=True)
    return (solved.astype(jnp.bfloat16), solved_obs[:, 0])

def reference(design, observations, gaps, noise_var, arc_lengths, arc_amp, arc_decay, plan, tile_map):
    block_count = arc_lengths.shape[0]
    block_rows = design.shape[0] // block_count
    columns = design.shape[1]
    tile_count = tile_map.shape[0]
    tile_size = columns // tile_count
    live_rows = gaps.astype(jnp.float32)

    def one_block(inputs):
        return whiten(*inputs)
    white, white_obs = lax.map(one_block, (design.reshape(block_count, block_rows, columns), observations.reshape(block_count, block_rows), live_rows.reshape(block_count, block_rows), noise_var.reshape(block_count, block_rows), arc_lengths, arc_amp, arc_decay))
    slotted = white.reshape(-1, tile_count, tile_size)[:, tile_map, :].reshape(-1, columns)
    widened = slotted.astype(jnp.float32)
    gram = jnp.dot(widened.T, widened, precision=lax.Precision.HIGHEST)
    obs_half = white_obs.reshape(-1).astype(jnp.bfloat16)
    normal_rhs = jnp.dot(obs_half.astype(jnp.float32), slotted.astype(jnp.float32), preferred_element_type=jnp.float32)
    balanced_obs = white_obs[plan]
    return (gram, normal_rhs, balanced_obs)
```

```python
import functools

import jax
import jax.numpy as jnp
from jax import lax
from jax.experimental import pallas as pl
from jax.experimental.pallas import tpu as pltpu
from jax.sharding import PartitionSpec as P

F32, BF16 = jnp.float32, jnp.bfloat16
ANY = pl.BlockSpec(memory_space=pl.ANY)
VMEM = pl.BlockSpec(memory_space=pltpu.VMEM)
SMEM = pl.BlockSpec(memory_space=pltpu.SMEM)


def factor_inverse(obs_rows, live_rows, noise_rows, lengths, amplitude, decay):
    block_rows = obs_rows.shape[0]
    position = jnp.arange(block_rows, dtype=jnp.int32)
    arc_ends = jnp.cumsum(lengths)
    arc_id = jnp.sum((arc_ends[None, :] <= position[:, None]).astype(jnp.int32), axis=1)
    member = (arc_id[:, None] == jnp.arange(lengths.shape[0], dtype=jnp.int32)[None, :]).astype(F32)
    row_amp = jnp.sum(member * amplitude[None, :], axis=1)
    row_rate = jnp.sum(member * jnp.log(decay)[None, :], axis=1)
    same_arc = (arc_id[:, None] == arc_id[None, :]).astype(F32)
    row_lag = jnp.abs(position[:, None] - position[None, :]).astype(F32)
    kernel = (
        row_amp[:, None]
        * jnp.exp(row_lag * row_rate[:, None])
        * same_arc
        * live_rows[:, None]
        * live_rows[None, :]
    )
    factor = jnp.linalg.cholesky(kernel + jnp.diag(noise_rows))
    inverse = lax.linalg.triangular_solve(
        factor, jnp.eye(block_rows, dtype=F32), left_side=True, lower=True
    )
    scaled = inverse * live_rows[None, :]
    return scaled, jnp.sum(scaled * obs_rows[None, :], axis=1)


def split_dot(w, x):
    high = w.astype(BF16)
    low = (w - high.astype(F32)).astype(BF16)
    total = jnp.dot(high, x, preferred_element_type=F32)
    return (total + jnp.dot(low, x, preferred_element_type=F32)).astype(BF16)


def pack(chunk, weight, tile_map, where, rows_axis, cols_axis):
    block_rows, columns = chunk.shape
    tiles = tile_map.shape[0]
    size = columns // tiles
    pairs = rows_axis // 2
    per_row, per_col = tiles // rows_axis, tiles // cols_axis
    wide = (2 * per_row + per_col) * size

    def kernel(map_ref, where_ref, x_ref, *refs):
        outs = refs[-pairs - 1 : -1]
        held = refs[-1]
        row, col = where_ref[0], where_ref[1]

        def fetch(base, count, to):
            for j in range(count):
                at = pl.multiple_of(map_ref[base + j] * size, size)
                held[:, (to + j) * size : (to + j + 1) * size] = x_ref[:, pl.ds(at, size)]

        def finish(start, stop, targets):
            part = held[:, start:stop]
            if weight is not None:
                part = split_dot(refs[0][...], part)
            for target in targets:
                target[:, start:stop] = part

        own = per_row * size
        fetch(col * per_col, per_col, 2 * per_row)
        finish(2 * own, wide, outs)
        for n in range(pairs):
            there = jnp.bitwise_xor(row, 2 * n)
            fetch(there * per_row, per_row, 0)
            fetch(jnp.bitwise_xor(there, 1) * per_row, per_row, per_row)
            finish(0, 2 * own, [outs[n]])

    args = (tile_map, where, chunk) + (() if weight is None else (weight,))
    return pl.pallas_call(
        kernel,
        name="pack",
        in_specs=[SMEM, SMEM] + [VMEM] * (len(args) - 2),
        out_specs=[VMEM] * pairs,
        out_shape=[jax.ShapeDtypeStruct((block_rows, wide), BF16)] * pairs,
        scratch_shapes=[pltpu.VMEM((block_rows, wide), BF16)],
        cost_estimate=pl.CostEstimate(flops=10**9, bytes_accessed=5 * 10**6, transcendentals=0),
        compiler_params=pltpu.CompilerParams(vmem_limit_bytes=24 << 20),
    )(*args)


def gram_first(raw, weights, white, obs, rows_width, cols_width):
    block_rows, wide = raw[0].shape
    count = len(raw) + len(white)
    depth = count * block_rows
    half = rows_width // 2
    step = cols_width // 6 if cols_width % 6 == 0 and (cols_width // 6) % 128 == 0 else 128
    steps = cols_width // step

    def kernel(*refs):
        blocks = refs[:count]
        w_refs = refs[count : count + len(raw)]
        obs_ref = refs[count + len(raw)]
        keep_ref, give_ref, rhs_ref = refs[-7:-4]
        fresh, held, turned, sems = refs[-4:]

        @pl.when(pl.program_id(0) == 0)
        def _():
            copies = []
            for b in range(count):
                to = fresh.at[b] if b < len(raw) else held.at[pl.ds(b * block_rows, block_rows)]
                copies.append(pltpu.make_async_copy(blocks[b], to, sems.at[b]))
                copies[-1].start()
            for b in range(count):
                rows = slice(b * block_rows, (b + 1) * block_rows)
                copies[b].wait()
                if b < len(raw):
                    held[rows, :] = split_dot(w_refs[b][...], fresh[b])
                turned[:, rows] = held[rows, :rows_width].T
            spread = jnp.broadcast_to(obs_ref[...].astype(BF16), (16, depth))
            rhs_ref[...] = jnp.dot(spread, held[:, :rows_width], preferred_element_type=F32)

        at = pl.multiple_of(rows_width + pl.program_id(0) * step, 128)
        right = held[:, pl.ds(at, step)]
        keep_ref[...] = jnp.dot(turned[:half, :], right, preferred_element_type=F32)
        give_ref[...] = jnp.dot(turned[half:, :], right, preferred_element_type=F32)

    tile = pl.BlockSpec((half, step), lambda i: (0, i))
    return pl.pallas_call(
        kernel,
        name="gram_first",
        grid=(steps,),
        in_specs=[ANY] * count + [VMEM] * (len(raw) + 1),
        out_specs=[tile, tile, pl.BlockSpec((16, rows_width), lambda i: (0, 0))],
        out_shape=[jax.ShapeDtypeStruct((half, cols_width), F32)] * 2
        + [jax.ShapeDtypeStruct((16, rows_width), F32)],
        scratch_shapes=[
            pltpu.VMEM((len(raw), block_rows, wide), BF16),
            pltpu.VMEM((depth, wide), BF16),
            pltpu.VMEM((rows_width, depth), BF16),
            pltpu.SemaphoreType.DMA((count,)),
        ],
        cost_estimate=pl.CostEstimate(
            flops=2 * depth * rows_width * cols_width, bytes_accessed=2 * 10**7, transcendentals=0
        ),
        compiler_params=pltpu.CompilerParams(vmem_limit_bytes=48 << 20),
    )(*raw, *white, *weights, obs)


def gram_last(keep, other, mine, theirs, obs, rows_width, cols_width):
    block_rows, wide = mine[0].shape
    count = len(mine) + len(theirs)
    depth = count * block_rows
    half = rows_width // 2
    step = cols_width // 6 if cols_width % 6 == 0 and (cols_width // 6) % 128 == 0 else 128
    steps = cols_width // step

    def kernel(*refs):
        keep_ref, other_ref = refs[:2]
        blocks = refs[2 : 2 + count]
        obs_ref = refs[2 + count]
        out_ref, rhs_ref = refs[-5:-3]
        held, turned, sems = refs[-3:]

        @pl.when(pl.program_id(0) == 0)
        def _():
            copies = []
            for b in range(count):
                to = held.at[pl.ds(b * block_rows, block_rows)]
                copies.append(pltpu.make_async_copy(blocks[b], to, sems.at[b]))
                copies[-1].start()
            total = jnp.zeros((16, half), F32)
            for b in range(count):
                rows = slice(b * block_rows, (b + 1) * block_rows)
                lead = 0 if b < len(mine) else half
                copies[b].wait()
                left = held[rows, lead : lead + half]
                turned[:, rows] = left.T
                spread = jnp.broadcast_to(obs_ref[:, rows].astype(BF16), (16, block_rows))
                total = total + jnp.dot(spread, left, preferred_element_type=F32)
            rhs_ref[...] = total

        at = pl.multiple_of(rows_width + pl.program_id(0) * step, 128)
        right = held[:, pl.ds(at, step)]
        out_ref[...] = (keep_ref[...] + other_ref[...]) + jnp.dot(
            turned[...], right, preferred_element_type=F32
        )

    tile = pl.BlockSpec((half, step), lambda i: (0, i))
    return pl.pallas_call(
        kernel,
        name="gram_last",
        grid=(steps,),
        in_specs=[tile, tile] + [ANY] * count + [VMEM],
        out_specs=[tile, pl.BlockSpec((16, half), lambda i: (0, 0))],
        out_shape=[
            jax.ShapeDtypeStruct((half, cols_width), F32),
            jax.ShapeDtypeStruct((16, half), F32),
        ],
        scratch_shapes=[
            pltpu.VMEM((depth, wide), BF16),
            pltpu.VMEM((half, depth), BF16),
            pltpu.SemaphoreType.DMA((count,)),
        ],
        cost_estimate=pl.CostEstimate(
            flops=2 * depth * half * cols_width, bytes_accessed=2 * 10**7, transcendentals=0
        ),
        compiler_params=pltpu.CompilerParams(vmem_limit_bytes=48 << 20),
    )(keep, other, *mine, *theirs, obs)


def on_device(
    rows_axis,
    cols_axis,
    design,
    observations,
    gaps,
    noise_var,
    arc_lengths,
    arc_amp,
    arc_decay,
    plan,
    tile_map,
):
    columns = design.shape[1]
    tiles = tile_map.shape[0]
    size = columns // tiles
    pairs = rows_axis // 2
    rows_width = 2 * (tiles // rows_axis) * size
    cols_width = (tiles // cols_axis) * size
    row, col = lax.axis_index("row"), lax.axis_index("col")
    where = jnp.stack([row, col]).astype(jnp.int32)

    def ring(x, shift):
        return lax.ppermute(x, "col", [(c, (c + shift) % cols_axis) for c in range(cols_axis)])

    def swap(x, mask):
        return lax.ppermute(x, "row", [(r, r ^ mask) for r in range(rows_axis)])

    def spread(parts):
        return [parts[0]] + [swap(parts[n], 2 * n) for n in range(1, pairs)]

    chunks = [design]
    for _ in range(1, cols_axis):
        chunks.append(ring(chunks[-1], 1))

    live = gaps.astype(F32)
    weight, white_obs = factor_inverse(
        observations, live, noise_var, arc_lengths[0], arc_amp[0], arc_decay[0]
    )
    near = jnp.concatenate([weight, white_obs[None, :]], axis=0)
    line = [near] + [ring(near, s) for s in range(1, cols_axis)]
    block_rows = weight.shape[0]
    line_obs = jnp.stack([part[block_rows] for part in line])
    obs_all = jnp.stack([line_obs] + [swap(line_obs, m) for m in range(1, rows_axis)])

    packed = [spread(pack(design, None, tile_map, where, rows_axis, cols_axis))]
    for s in range(1, cols_axis):
        weight_s = line[s][:block_rows]
        packed.append(spread(pack(chunks[s], weight_s, tile_map, where, rows_axis, cols_axis)))

    weights = [weight] + [swap(weight, 2 * n) for n in range(1, pairs)]
    obs_first = obs_all[::2, : cols_axis - 1].swapaxes(0, 1).reshape(1, -1)
    keep, give, rhs_first = gram_first(
        packed[0],
        weights,
        [block for s in range(1, cols_axis - 1) for block in packed[s]],
        obs_first,
        rows_width,
        cols_width,
    )
    half = rows_width // 2
    other = swap(give, 1)
    other_rhs = swap(rhs_first[0, half:], 1)
    theirs = [swap(block, 1) for block in packed[-1]]
    obs_last = jnp.concatenate([obs_all[::2, -1], obs_all[1::2, -1]], axis=0).reshape(1, -1)
    gram, rhs_last = gram_last(
        keep, other, packed[-1], theirs, obs_last, rows_width, cols_width
    )
    normal_rhs = rhs_first[0, :half] + other_rhs + rhs_last[0]
    from_row, from_col = plan // cols_axis, plan % cols_axis
    ahead = (col - from_col + cols_axis) % cols_axis
    place = jnp.bitwise_xor(from_row, row) * cols_axis + ahead
    balanced_obs = jnp.take(obs_all.reshape(-1, block_rows), place, axis=0)
    return (gram, normal_rhs, balanced_obs)


def solution(mesh):
    placed = (
        P(("row", "col"), None),
        P(("row", "col")),
        P(("row", "col")),
        P(("row", "col")),
        P(("row", "col"), None),
        P(("row", "col"), None),
        P(("row", "col"), None),
        P(("row", "col")),
        P(),
    )
    return jax.shard_map(
        functools.partial(on_device, mesh.shape["row"], mesh.shape["col"]),
        mesh=mesh,
        in_specs=placed,
        out_specs=(P("row", "col"), P("row"), P(("row", "col"), None)),
        check_vma=False,
    )
```

```python
import jax
import jax.numpy as jnp
from jax import lax
from jax.experimental import pallas as pl
from jax.experimental.pallas import tpu as pltpu
from jax.sharding import PartitionSpec as P


F32, BF16 = jnp.float32, jnp.bfloat16
ANY = pl.BlockSpec(memory_space=pl.ANY)
VMEM = pl.BlockSpec(memory_space=pltpu.VMEM)
SMEM = pl.BlockSpec(memory_space=pltpu.SMEM)


def factor_inverse(obs_rows, live_rows, noise_rows, lengths, amplitude, decay):
    block_rows = obs_rows.shape[0]
    position = jnp.arange(block_rows, dtype=jnp.int32)
    arc_ends = jnp.cumsum(lengths)
    arc_id = jnp.sum((arc_ends[None, :] <= position[:, None]).astype(jnp.int32), axis=1)
    member = (arc_id[:, None] == jnp.arange(lengths.shape[0], dtype=jnp.int32)[None, :]).astype(F32)
    row_amp = jnp.sum(member * amplitude[None, :], axis=1)
    row_rate = jnp.sum(member * jnp.log(decay)[None, :], axis=1)
    same_arc = (arc_id[:, None] == arc_id[None, :]).astype(F32)
    row_lag = jnp.abs(position[:, None] - position[None, :]).astype(F32)
    kernel = (
        row_amp[:, None]
        * jnp.exp(row_lag * row_rate[:, None])
        * same_arc
        * live_rows[:, None]
        * live_rows[None, :]
    )
    factor = jnp.linalg.cholesky(kernel + jnp.diag(noise_rows))
    inverse = lax.linalg.triangular_solve(
        factor, jnp.eye(block_rows, dtype=F32), left_side=True, lower=True
    )
    scaled = inverse * live_rows[None, :]
    return scaled, jnp.sum(scaled * obs_rows[None, :], axis=1)


def split_dot(w, x):
    high = w.astype(BF16)
    low = (w - high.astype(F32)).astype(BF16)
    total = jnp.dot(high, x, preferred_element_type=F32)
    return (total + jnp.dot(low, x, preferred_element_type=F32)).astype(BF16)


def pack(chunk, weight, tile_map, where, rows_axis, cols_axis):
    block_rows, columns = chunk.shape
    tiles = tile_map.shape[0]
    size = columns // tiles
    pairs = rows_axis // 2
    per_row, per_col = tiles // rows_axis, tiles // cols_axis
    wide = (2 * per_row + per_col) * size

    def kernel(map_ref, where_ref, x_ref, *refs):
        outs = refs[-pairs - 1 : -1]
        held = refs[-1]
        row, col = where_ref[0], where_ref[1]

        def fetch(base, count, to):
            for j in range(count):
                at = pl.multiple_of(map_ref[base + j] * size, size)
                held[:, (to + j) * size : (to + j + 1) * size] = x_ref[:, pl.ds(at, size)]

        def finish(start, stop, targets):
            part = held[:, start:stop]
            if weight is not None:
                part = split_dot(refs[0][...], part)
            for target in targets:
                target[:, start:stop] = part

        own = per_row * size
        fetch(col * per_col, per_col, 2 * per_row)
        finish(2 * own, wide, outs)
        for n in range(pairs):
            there = jnp.bitwise_xor(row, 2 * n)
            fetch(there * per_row, per_row, 0)
            fetch(jnp.bitwise_xor(there, 1) * per_row, per_row, per_row)
            finish(0, 2 * own, [outs[n]])

    args = (tile_map, where, chunk) + (() if weight is None else (weight,))
    return pl.pallas_call(
        kernel,
        name="pack",
        in_specs=[SMEM, SMEM] + [VMEM] * (len(args) - 2),
        out_specs=[VMEM] * pairs,
        out_shape=[jax.ShapeDtypeStruct((block_rows, wide), BF16)] * pairs,
        scratch_shapes=[pltpu.VMEM((block_rows, wide), BF16)],
        cost_estimate=pl.CostEstimate(flops=10**9, bytes_accessed=5 * 10**6, transcendentals=0),
        compiler_params=pltpu.CompilerParams(vmem_limit_bytes=24 << 20),
    )(*args)


def gram_first(raw, weights, white, obs, rows_width, cols_width):
    block_rows, wide = raw[0].shape
    count = len(raw) + len(white)
    depth = count * block_rows
    half = rows_width // 2
    step = cols_width // 6 if cols_width % 6 == 0 and (cols_width // 6) % 128 == 0 else 128
    steps = cols_width // step

    def kernel(*refs):
        blocks = refs[:count]
        w_refs = refs[count : count + len(raw)]
        obs_ref = refs[count + len(raw)]
        keep_ref, give_ref, rhs_ref = refs[-7:-4]
        fresh, held, turned, sems = refs[-4:]

        @pl.when(pl.program_id(0) == 0)
        def _():
            copies = []
            for b in range(count):
                to = fresh.at[b] if b < len(raw) else held.at[pl.ds(b * block_rows, block_rows)]
                copies.append(pltpu.make_async_copy(blocks[b], to, sems.at[b]))
                copies[-1].start()
            for b in range(count):
                rows = slice(b * block_rows, (b + 1) * block_rows)
                copies[b].wait()
                if b < len(raw):
                    held[rows, :] = split_dot(w_refs[b][...], fresh[b])
                turned[:, rows] = held[rows, :rows_width].T
            spread = jnp.broadcast_to(obs_ref[...].astype(BF16), (16, depth))
            rhs_ref[...] = jnp.dot(spread, held[:, :rows_width], preferred_element_type=F32)

        at = pl.multiple_of(rows_width + pl.program_id(0) * step, 128)
        right = held[:, pl.ds(at, step)]
        keep_ref[...] = jnp.dot(turned[:half, :], right, preferred_element_type=F32)
        give_ref[...] = jnp.dot(turned[half:, :], right, preferred_element_type=F32)

    tile = pl.BlockSpec((half, step), lambda i: (0, i))
    return pl.pallas_call(
        kernel,
        name="gram_first",
        grid=(steps,),
        in_specs=[ANY] * count + [VMEM] * (len(raw) + 1),
        out_specs=[tile, tile, pl.BlockSpec((16, rows_width), lambda i: (0, 0))],
        out_shape=[jax.ShapeDtypeStruct((half, cols_width), F32)] * 2
        + [jax.ShapeDtypeStruct((16, rows_width), F32)],
        scratch_shapes=[
            pltpu.VMEM((len(raw), block_rows, wide), BF16),
            pltpu.VMEM((depth, wide), BF16),
            pltpu.VMEM((rows_width, depth), BF16),
            pltpu.SemaphoreType.DMA((count,)),
        ],
        cost_estimate=pl.CostEstimate(
            flops=2 * depth * rows_width * cols_width, bytes_accessed=2 * 10**7, transcendentals=0
        ),
        compiler_params=pltpu.CompilerParams(vmem_limit_bytes=48 << 20),
    )(*raw, *white, *weights, obs)


def gram_last(keep, other, mine, theirs, obs, rows_width, cols_width):
    block_rows, wide = mine[0].shape
    count = len(mine) + len(theirs)
    depth = count * block_rows
    half = rows_width // 2
    step = cols_width // 6 if cols_width % 6 == 0 and (cols_width // 6) % 128 == 0 else 128
    steps = cols_width // step

    def kernel(*refs):
        keep_ref, other_ref = refs[:2]
        blocks = refs[2 : 2 + count]
        obs_ref = refs[2 + count]
        out_ref, rhs_ref = refs[-5:-3]
        held, turned, sems = refs[-3:]

        @pl.when(pl.program_id(0) == 0)
        def _():
            copies = []
            for b in range(count):
                to = held.at[pl.ds(b * block_rows, block_rows)]
                copies.append(pltpu.make_async_copy(blocks[b], to, sems.at[b]))
                copies[-1].start()
            total = jnp.zeros((16, half), F32)
            for b in range(count):
                rows = slice(b * block_rows, (b + 1) * block_rows)
                lead = 0 if b < len(mine) else half
                copies[b].wait()
                left = held[rows, lead : lead + half]
                turned[:, rows] = left.T
                spread = jnp.broadcast_to(obs_ref[:, rows].astype(BF16), (16, block_rows))
                total = total + jnp.dot(spread, left, preferred_element_type=F32)
            rhs_ref[...] = total

        at = pl.multiple_of(rows_width + pl.program_id(0) * step, 128)
        right = held[:, pl.ds(at, step)]
        out_ref[...] = (keep_ref[...] + other_ref[...]) + jnp.dot(
            turned[...], right, preferred_element_type=F32
        )

    tile = pl.BlockSpec((half, step), lambda i: (0, i))
    return pl.pallas_call(
        kernel,
        name="gram_last",
        grid=(steps,),
        in_specs=[tile, tile] + [ANY] * count + [VMEM],
        out_specs=[tile, pl.BlockSpec((16, half), lambda i: (0, 0))],
        out_shape=[
            jax.ShapeDtypeStruct((half, cols_width), F32),
            jax.ShapeDtypeStruct((16, half), F32),
        ],
        scratch_shapes=[
            pltpu.VMEM((depth, wide), BF16),
            pltpu.VMEM((half, depth), BF16),
            pltpu.SemaphoreType.DMA((count,)),
        ],
        cost_estimate=pl.CostEstimate(
            flops=2 * depth * half * cols_width, bytes_accessed=2 * 10**7, transcendentals=0
        ),
        compiler_params=pltpu.CompilerParams(vmem_limit_bytes=48 << 20),
    )(keep, other, *mine, *theirs, obs)


def on_device_any(
    rows_axis,
    cols_axis,
    design,
    observations,
    gaps,
    noise_var,
    arc_lengths,
    arc_amp,
    arc_decay,
    plan,
    tile_map,
):
    columns = design.shape[1]
    tiles = tile_map.shape[0]
    size = columns // tiles
    pairs = rows_axis // 2
    rows_width = 2 * (tiles // rows_axis) * size
    cols_width = (tiles // cols_axis) * size
    row, col = lax.axis_index("row"), lax.axis_index("col")
    where = jnp.stack([row, col]).astype(jnp.int32)

    def ring(x, shift):
        return lax.ppermute(x, "col", [(c, (c + shift) % cols_axis) for c in range(cols_axis)])

    def swap(x, mask):
        return lax.ppermute(x, "row", [(r, r ^ mask) for r in range(rows_axis)])

    def spread(parts):
        return [parts[0]] + [swap(parts[n], 2 * n) for n in range(1, pairs)]

    chunks = [design]
    for _ in range(1, cols_axis):
        chunks.append(ring(chunks[-1], 1))

    live = gaps.astype(F32)
    weight, white_obs = factor_inverse(
        observations, live, noise_var, arc_lengths[0], arc_amp[0], arc_decay[0]
    )
    near = jnp.concatenate([weight, white_obs[None, :]], axis=0)
    line = [near] + [ring(near, s) for s in range(1, cols_axis)]
    block_rows = weight.shape[0]
    line_obs = jnp.stack([part[block_rows] for part in line])
    obs_all = jnp.stack([line_obs] + [swap(line_obs, m) for m in range(1, rows_axis)])

    packed = [spread(pack(design, None, tile_map, where, rows_axis, cols_axis))]
    for s in range(1, cols_axis):
        weight_s = line[s][:block_rows]
        packed.append(spread(pack(chunks[s], weight_s, tile_map, where, rows_axis, cols_axis)))

    weights = [weight] + [swap(weight, 2 * n) for n in range(1, pairs)]
    obs_first = obs_all[::2, : cols_axis - 1].swapaxes(0, 1).reshape(1, -1)
    keep, give, rhs_first = gram_first(
        packed[0],
        weights,
        [block for s in range(1, cols_axis - 1) for block in packed[s]],
        obs_first,
        rows_width,
        cols_width,
    )
    half = rows_width // 2
    other = swap(give, 1)
    other_rhs = swap(rhs_first[0, half:], 1)
    theirs = [swap(block, 1) for block in packed[-1]]
    obs_last = jnp.concatenate([obs_all[::2, -1], obs_all[1::2, -1]], axis=0).reshape(1, -1)
    gram, rhs_last = gram_last(
        keep, other, packed[-1], theirs, obs_last, rows_width, cols_width
    )
    normal_rhs = rhs_first[0, :half] + other_rhs + rhs_last[0]
    from_row, from_col = plan // cols_axis, plan % cols_axis
    ahead = (col - from_col + cols_axis) % cols_axis
    place = jnp.bitwise_xor(from_row, row) * cols_axis + ahead
    balanced_obs = jnp.take(obs_all.reshape(-1, block_rows), place, axis=0)
    return (gram, normal_rhs, balanced_obs)


def pack_cut(chunk, weight, tile_map, where, rows_axis, cols_axis):
    block_rows, columns = chunk.shape
    tiles = tile_map.shape[0]
    size = columns // tiles
    per_row, per_col = tiles // rows_axis, tiles // cols_axis
    own = per_row * size
    rows_width, cols_width = 2 * own, per_col * size
    half = cols_width // 2

    def kernel(map_ref, where_ref, x_ref, *refs):
        across_a, across_b, along_a, along_b, keep, held = refs[-6:]
        row, col = where_ref[0], where_ref[1]

        def fetch(base, count, width):
            for j in range(count):
                at = pl.multiple_of(map_ref[base + j] * size, size)
                held[:, j * size : (j + 1) * size] = x_ref[:, pl.ds(at, size)]
            return whiten(held[:, :width])

        def whiten(part):
            return part if weight is None else split_dot(refs[0][:block_rows], part)

        def rows_of(n, core):
            there = jnp.bitwise_xor(row, 2 * n + core)
            return fetch(there * per_row, per_row, own)

        part = fetch(col * per_col, per_col, cols_width)
        keep[:, rows_width:] = part
        across_a[:, own:] = part[:, :half]
        along_b[:, rows_width:] = part[:, :half]
        across_b[:, rows_width:] = part[:, half:]
        along_a[:, own:] = part[:, half:]
        across_a[:, :own] = rows_of(3, 0)
        along_a[:, :own] = rows_of(3, 1)
        for n, target in ((1, across_b), (2, along_b), (0, keep)):
            target[:, :own] = rows_of(n, 0)
            target[:, own:rows_width] = rows_of(n, 1)

    args = (tile_map, where, chunk) + (() if weight is None else (weight,))
    widths = (own + half, rows_width + half, own + half, rows_width + half, rows_width + cols_width)
    return pl.pallas_call(
        kernel,
        name="pack_cut",
        in_specs=[SMEM, SMEM] + [VMEM] * (len(args) - 2),
        out_specs=[VMEM] * 5,
        out_shape=[jax.ShapeDtypeStruct((block_rows, w), BF16) for w in widths],
        scratch_shapes=[pltpu.VMEM((block_rows, max(rows_width, cols_width)), BF16)],
        cost_estimate=pl.CostEstimate(flops=10**9, bytes_accessed=5 * 10**6, transcendentals=0),
        compiler_params=pltpu.CompilerParams(vmem_limit_bytes=24 << 20),
    )(*args)


def whiten_plane(parts, weights, design, near, tile_map, where, cols_axis):
    block_rows, columns = design.shape
    tiles = tile_map.shape[0]
    size = columns // tiles
    per_col = tiles // cols_axis
    cols_width = per_col * size
    half = cols_width // 2
    own = parts[1].shape[1] - half
    rows_width = parts[2].shape[1] - half
    own = rows_width // 2
    depth = 4 * block_rows

    def kernel(map_ref, where_ref, x_ref, near_ref, *refs):
        keep, xa, xb, ya, yb, fa, fb = refs[:7]
        w1, w2, w3 = refs[7:10]
        lead_ref, rest_ref, cols_ref, before_ref, held = refs[10:]
        col = where_ref[1]
        w0 = near_ref[:block_rows]

        def put(n, weight, lead, rest, left, right):
            rows = slice(n * block_rows, (n + 1) * block_rows)
            lead_ref[rows, :] = split_dot(weight, lead)
            rest_ref[rows, :] = split_dot(weight, rest)
            cols_ref[rows, :half] = split_dot(weight, left)
            cols_ref[rows, half:] = split_dot(weight, right)

        def four(ref):
            return ref[:, :own], ref[:, own:rows_width]

        put(0, w0, *four(keep), keep[:, rows_width : rows_width + half], keep[:, rows_width + half :])
        put(1, w1[...], *four(xb), xa[:, own:], xb[:, rows_width:])
        put(2, w2[...], *four(yb), yb[:, rows_width:], ya[:, own:])
        put(3, w3[...], fa[:, :own], fb[:, :own], fa[:, own:], fb[:, own:])
        base = jnp.where(col == 0, cols_axis - 1, col - 1) * per_col
        for j in range(per_col):
            at = pl.multiple_of(map_ref[base + j] * size, size)
            held[:, j * size : (j + 1) * size] = x_ref[:, pl.ds(at, size)]
        before_ref[...] = split_dot(w0, held[...])

    return pl.pallas_call(
        kernel,
        name="whiten_plane",
        in_specs=[SMEM, SMEM] + [VMEM] * 12,
        out_specs=[VMEM] * 4,
        out_shape=[
            jax.ShapeDtypeStruct((depth, own), BF16),
            jax.ShapeDtypeStruct((depth, own), BF16),
            jax.ShapeDtypeStruct((depth, cols_width), BF16),
            jax.ShapeDtypeStruct((block_rows, cols_width), BF16),
        ],
        scratch_shapes=[pltpu.VMEM((block_rows, cols_width), BF16)],
        cost_estimate=pl.CostEstimate(flops=10**9, bytes_accessed=5 * 10**6, transcendentals=0),
        compiler_params=pltpu.CompilerParams(vmem_limit_bytes=32 << 20),
    )(tile_map, where, design, near, *parts, *weights)


def gram_step(pieces, operands, before, obs, places, depth, rows_width, cols_width):
    half = rows_width // 2
    count = len(operands)
    block_rows = depth // len(places)
    step = cols_width // 6 if cols_width % 6 == 0 and (cols_width // 6) % 128 == 0 else 128
    steps = cols_width // step

    def kernel(*refs):
        sources = refs[:count]
        obs_refs = refs[count : count + len(obs)]
        sums = refs[count + len(obs) : count + len(obs) + len(before)]
        keep_ref, give_ref, keep_rhs, give_rhs, held, turned, sems = refs[-7:]

        @pl.when(pl.program_id(0) == 0)
        def _():
            copies = []
            for k, (which, src, to_row, to_col) in enumerate(pieces):
                source = sources[which].at[:, pl.ds(src[0], src[1])]
                target = held.at[pl.ds(to_row, operands[which].shape[0]), pl.ds(to_col, src[1])]
                copies.append(pltpu.make_async_copy(source, target, sems.at[k]))
                copies[-1].start()
            for copy in copies:
                copy.wait()
            total = jnp.zeros((8, rows_width), F32)
            for b, (m, s) in enumerate(places):
                rows = slice(b * block_rows, (b + 1) * block_rows)
                left = held[rows, :rows_width]
                turned[:, rows] = left.T
                spread = jnp.broadcast_to(obs_refs[m][s : s + 1, :], (8, block_rows)).astype(BF16)
                total = total + jnp.dot(spread, left, preferred_element_type=F32)
            if before:
                keep_rhs[...] = sums[2][...] + total[:, :half]
                give_rhs[...] = sums[3][...] + total[:, half:]
            else:
                keep_rhs[...] = total[:, :half]
                give_rhs[...] = total[:, half:]

        at = pl.multiple_of(rows_width + pl.program_id(0) * step, 128)
        right = held[:, pl.ds(at, step)]
        lead = jnp.dot(turned[:half, :], right, preferred_element_type=F32)
        rest = jnp.dot(turned[half:, :], right, preferred_element_type=F32)
        keep_ref[...] = sums[0][...] + lead if before else lead
        give_ref[...] = sums[1][...] + rest if before else rest

    tile = pl.BlockSpec((half, step), lambda i: (0, i))
    whole = pl.BlockSpec((8, half), lambda i: (0, 0))
    return pl.pallas_call(
        kernel,
        grid=(steps,),
        in_specs=[ANY] * count
        + [VMEM] * len(obs)
        + ([tile, tile, whole, whole] if before else []),
        out_specs=[tile, tile, whole, whole],
        out_shape=[jax.ShapeDtypeStruct((half, cols_width), F32)] * 2
        + [jax.ShapeDtypeStruct((8, half), F32)] * 2,
        scratch_shapes=[
            pltpu.VMEM((depth, rows_width + cols_width), BF16),
            pltpu.VMEM((rows_width, depth), BF16),
            pltpu.SemaphoreType.DMA((len(pieces),)),
        ],
        cost_estimate=pl.CostEstimate(
            flops=2 * depth * rows_width * cols_width, bytes_accessed=2 * 10**7, transcendentals=0
        ),
        compiler_params=pltpu.CompilerParams(vmem_limit_bytes=40 << 20),
    )(*operands, *obs, *before)


def gram_end(pieces, operands, sums, obs, places, source, depth, half, cols_width):
    count = len(operands)
    block_rows = depth // len(places)
    step = cols_width // 6 if cols_width % 6 == 0 and (cols_width // 6) % 128 == 0 else 128
    steps = cols_width // step

    def kernel(source_ref, *refs):
        sources = refs[:count]
        obs_refs = refs[count : count + len(obs)]
        one, two, one_rhs, two_rhs = refs[count + len(obs) : count + len(obs) + 4]
        out_ref, rhs_ref, picked_ref, held, turned, sems = refs[-6:]

        @pl.when(pl.program_id(0) == 0)
        def _():
            copies = []
            for k, (which, src, to_row, to_col) in enumerate(pieces):
                origin = sources[which].at[:, pl.ds(src[0], src[1])]
                target = held.at[pl.ds(to_row, operands[which].shape[0]), pl.ds(to_col, src[1])]
                copies.append(pltpu.make_async_copy(origin, target, sems.at[k]))
                copies[-1].start()
            picked = jnp.zeros((1, block_rows), F32)
            for m in range(len(obs)):
                picked = jnp.where(source_ref[0] == m, obs_refs[m][pl.ds(source_ref[1], 1), :], picked)
            picked_ref[...] = picked
            for copy in copies:
                copy.wait()
            total = one_rhs[...] + two_rhs[...]
            for b, (m, s) in enumerate(places):
                rows = slice(b * block_rows, (b + 1) * block_rows)
                left = held[rows, :half]
                turned[:, rows] = left.T
                spread = jnp.broadcast_to(obs_refs[m][s : s + 1, :], (8, block_rows)).astype(BF16)
                total = total + jnp.dot(spread, left, preferred_element_type=F32)
            rhs_ref[...] = total

        at = pl.multiple_of(half + pl.program_id(0) * step, 128)
        out_ref[...] = (one[...] + two[...]) + jnp.dot(
            turned[...], held[:, pl.ds(at, step)], preferred_element_type=F32
        )

    tile = pl.BlockSpec((half, step), lambda i: (0, i))
    whole = pl.BlockSpec((8, half), lambda i: (0, 0))
    return pl.pallas_call(
        kernel,
        name="gram_end",
        grid=(steps,),
        in_specs=[SMEM] + [ANY] * count + [VMEM] * len(obs) + [tile, tile, whole, whole],
        out_specs=[tile, whole, pl.BlockSpec((1, block_rows), lambda i: (0, 0))],
        out_shape=[
            jax.ShapeDtypeStruct((half, cols_width), F32),
            jax.ShapeDtypeStruct((8, half), F32),
            jax.ShapeDtypeStruct((1, block_rows), F32),
        ],
        scratch_shapes=[
            pltpu.VMEM((depth, half + cols_width), BF16),
            pltpu.VMEM((half, depth), BF16),
            pltpu.SemaphoreType.DMA((len(pieces),)),
        ],
        cost_estimate=pl.CostEstimate(
            flops=2 * depth * half * cols_width, bytes_accessed=2 * 10**7, transcendentals=0
        ),
        compiler_params=pltpu.CompilerParams(vmem_limit_bytes=40 << 20),
    )(source, *operands, *obs, *sums)


def on_device_square(
    rows_axis,
    cols_axis,
    design,
    observations,
    gaps,
    noise_var,
    arc_lengths,
    arc_amp,
    arc_decay,
    plan,
    tile_map,
):
    block_rows, columns = design.shape
    tiles = tile_map.shape[0]
    size = columns // tiles
    own = (tiles // rows_axis) * size
    rows_width = 2 * own
    cols_width = (tiles // cols_axis) * size
    half = cols_width // 2
    row, col = lax.axis_index("row"), lax.axis_index("col")
    where = jnp.stack([row, col]).astype(jnp.int32)

    def ring(x, shift):
        return lax.ppermute(x, "col", [(c, (c + shift) % cols_axis) for c in range(cols_axis)])

    def swap(x, mask):
        return lax.ppermute(x, "row", [(r, r ^ mask) for r in range(rows_axis)])

    last = cols_axis - 1
    live = gaps.astype(F32)
    weight, white_obs = factor_inverse(
        observations, live, noise_var, arc_lengths[0], arc_amp[0], arc_decay[0]
    )
    near = jnp.concatenate([weight, white_obs[None, :]], axis=0)
    line = [near] + [ring(near, s) for s in range(1, cols_axis)]
    weights = [swap(weight, 2 * n) for n in range(1, 4)]
    line_obs = jnp.stack([part[block_rows] for part in line])
    obs = [line_obs] + [swap(line_obs, m) for m in range(1, rows_axis)]

    chunks = [design]
    for _ in range(1, last):
        chunks.append(ring(chunks[-1], 1))
    traded = []
    for s in range(last):
        xa, xb, ya, yb, keep = pack_cut(
            chunks[s], line[s] if s else None, tile_map, where, rows_axis, cols_axis
        )
        xa, ya = swap(xa, 2), swap(ya, 4)
        xb, yb = swap(xb, 2), swap(yb, 4)
        fa, fb = swap(xa, 4), swap(ya, 2)
        traded.append((keep, xa, xb, ya, yb, fa, fb))
    lead, rest, plane_cols, before = whiten_plane(
        traded[0], weights, design, near, tile_map, where, cols_axis
    )
    far_cols = ring(before, last)
    far_rest = ring(rest, last)
    far_lead = ring(lead, last)

    wide = rows_width
    pieces = [
        (0, (0, own), 0, 0),
        (1, (0, own), 0, own),
        (2, (0, cols_width), 0, wide),
    ]
    operands = [lead, rest, plane_cols]
    places = [(2 * n, 0) for n in range(4)]

    def chunk_pieces(start, first):
        out = []
        for k, (src, at, block) in (
            (0, ((0, wide + cols_width), 0, 0)),
            (1, ((own, half), wide, 1)),
            (2, ((0, wide), 0, 1)),
            (2, ((wide, half), wide + half, 1)),
            (3, ((own, half), wide + half, 2)),
            (4, ((0, wide + half), 0, 2)),
            (5, ((0, own), 0, 3)),
            (5, ((own, half), wide, 3)),
            (6, ((0, own), own, 3)),
            (6, ((own, half), wide + half, 3)),
        ):
            out.append((first + k, src, start + block * block_rows, at))
        return out

    sums = ()
    for s in range(1, last):
        start = len(places) * block_rows
        pieces += chunk_pieces(start, len(operands))
        operands += list(traded[s])
        places += [(2 * n, s) for n in range(4)]
        sums = gram_step(
            pieces, operands, sums, obs, places, len(places) * block_rows, rows_width, cols_width
        )
        pieces, operands, places = [], [], []
    keep, give, keep_rhs, give_rhs = sums
    other = swap(give, 1)
    other_rhs = swap(give_rhs, 1)

    x3, y3 = swap(far_cols, 2), swap(far_cols, 4)
    fa3 = swap(x3[:, :half], 4)
    fb3 = swap(y3[:, half:], 2)
    mine = [far_cols, x3, y3, fa3, fb3]
    theirs = [swap(v, 1) for v in mine]
    their_rows = swap(far_rest, 1)
    pieces = [(0, (0, own), 0, 0), (1, (0, own), 4 * block_rows, 0)]
    operands = [far_lead, their_rows]
    for start, group in ((0, mine), (4 * block_rows, theirs)):
        first = len(operands)
        operands += group
        pieces += [
            (first, (0, cols_width), start, own),
            (first + 1, (0, cols_width), start + block_rows, own),
            (first + 2, (0, cols_width), start + 2 * block_rows, own),
            (first + 3, (0, half), start + 3 * block_rows, own),
            (first + 4, (0, half), start + 3 * block_rows, own + half),
        ]
    places = [(2 * n, last) for n in range(4)] + [(2 * n + 1, last) for n in range(4)]
    from_row, from_col = plan[0] // cols_axis, plan[0] % cols_axis
    source = jnp.stack(
        [jnp.bitwise_xor(from_row, row), (col - from_col + cols_axis) % cols_axis]
    ).astype(jnp.int32)
    gram, rhs, balanced_obs = gram_end(
        pieces,
        operands,
        (keep, other, keep_rhs, other_rhs),
        obs,
        places,
        source,
        8 * block_rows,
        own,
        cols_width,
    )
    return (gram, rhs[0], balanced_obs)


def solution(mesh):
    placed = (
        P(("row", "col"), None),
        P(("row", "col")),
        P(("row", "col")),
        P(("row", "col")),
        P(("row", "col"), None),
        P(("row", "col"), None),
        P(("row", "col"), None),
        P(("row", "col")),
        P(),
    )
    rows_axis, cols_axis = mesh.shape["row"], mesh.shape["col"]
    square = rows_axis == 2**3 and cols_axis > 2

    def body(*args):
        if not square:
            return on_device_any(rows_axis, cols_axis, *args)
        return on_device_square(rows_axis, cols_axis, *args)

    return jax.shard_map(
        body,
        mesh=mesh,
        in_specs=placed,
        out_specs=(P("row", "col"), P("row"), P(("row", "col"), None)),
        check_vma=False,
    )
```

```python
import jax
import jax.numpy as jnp
from jax import lax
from jax.experimental import pallas as pl
from jax.experimental.pallas import tpu as pltpu
from jax.sharding import PartitionSpec as P


F32, BF16 = jnp.float32, jnp.bfloat16
ANY = pl.BlockSpec(memory_space=pl.ANY)
VMEM = pl.BlockSpec(memory_space=pltpu.VMEM)
SMEM = pl.BlockSpec(memory_space=pltpu.SMEM)


def factor_kernel(observations, gaps, noise_var, arc_lengths, arc_amp, arc_decay):
    n = observations.shape[0]
    arcs = arc_lengths.shape[1]

    def kernel(len_ref, amp_ref, decay_ref, obs_ref, gap_ref, noise_ref, out_ref):
        lane = lax.broadcasted_iota(jnp.int32, (8, n), 1)
        live = jnp.broadcast_to(gap_ref[...].astype(F32), (8, n))
        noise = jnp.broadcast_to(noise_ref[...], (8, n))
        big_line = lax.broadcasted_iota(jnp.int32, (n, n), 0)
        big_lane = lax.broadcasted_iota(jnp.int32, (n, n), 1)
        arc = jnp.zeros((8, n), jnp.int32)
        first = lane == 0
        arc_line = jnp.zeros((n, n), jnp.int32)
        end = 0
        for k in range(arcs):
            end = end + len_ref[0, k]
            arc = arc + (lane >= end).astype(jnp.int32)
            arc_line = arc_line + (big_line >= end).astype(jnp.int32)
            first = jnp.logical_or(first, lane == end)
        amp = jnp.zeros((8, n), F32)
        decay = jnp.ones((8, n), F32)
        for k in range(arcs):
            amp = jnp.where(arc == k, amp_ref[0, k], amp)
            decay = jnp.where(arc == k, decay_ref[0, k], decay)

        def back(x, shift):
            return pltpu.roll(x, shift, axis=1)

        fresh = (1.0 - decay * decay) * amp
        a = back(decay * decay * noise + fresh * live, 1)
        b = back(fresh * noise, 1)
        c = back(live, 1)
        d = back(noise, 1)
        a = jnp.where(first, 0.0, a)
        b = jnp.where(first, amp, b)
        c = jnp.where(first, 0.0, c)
        d = jnp.where(first, 1.0, d)
        shift = 1
        while shift < n:
            ok = lane >= shift
            pa, pb = jnp.where(ok, back(a, shift), 1.0), jnp.where(ok, back(b, shift), 0.0)
            pc, pd = jnp.where(ok, back(c, shift), 0.0), jnp.where(ok, back(d, shift), 1.0)
            a, b, c, d = a * pa + b * pc, a * pb + b * pd, c * pa + d * pc, c * pb + d * pd
            level = 1.0 / (a + b + c + d)
            a, b, c, d = a * level, b * level, c * level, d * level
            shift *= 2
        variance = b / d
        total = live * variance + noise
        root = 1.0 / jnp.sqrt(total)
        fade = jnp.log(decay * noise / total)
        gain = decay * variance * live / total
        below = big_lane < big_line
        fades = jnp.where(below, jnp.broadcast_to(fade[:1], (n, n)), 0.0)
        mask = below.astype(BF16)
        spans = jnp.zeros((n, n), F32)
        for _ in range(3):
            part = fades.astype(BF16)
            spans = spans + jnp.dot(part, mask, preferred_element_type=F32)
            fades = fades - part.astype(F32)
        diagonal = big_line == big_lane

        def upright(x):
            return jnp.sum(jnp.where(diagonal, jnp.broadcast_to(x[:1], (n, n)), 0.0), axis=1, keepdims=True)

        left = upright(live * root)
        same = jnp.logical_and(below, arc_line == jnp.broadcast_to(arc[:1], (n, n)))
        weight = jnp.where(same, -left * jnp.exp(spans) * jnp.broadcast_to(gain[:1], (n, n)), 0.0)
        weight = jnp.where(diagonal, left, weight)
        out_ref[:n, :] = weight
        white = jnp.sum(weight * jnp.broadcast_to(obs_ref[...], (n, n)), axis=1, keepdims=True)
        white_row = jnp.sum(jnp.where(diagonal, white, 0.0), axis=0, keepdims=True)
        out_ref[n:, :] = jnp.broadcast_to(white_row, (8, n))

    row = (1, n)
    return pl.pallas_call(
        kernel,
        name="factor",
        in_specs=[SMEM] * 3 + [VMEM] * 3,
        out_specs=VMEM,
        out_shape=jax.ShapeDtypeStruct((n + 8, n), F32),
        cost_estimate=pl.CostEstimate(flops=10**8, bytes_accessed=10**5, transcendentals=0),
        compiler_params=pltpu.CompilerParams(vmem_limit_bytes=4 << 20),
    )(
        arc_lengths,
        arc_amp,
        arc_decay,
        observations.reshape(row),
        gaps.reshape(row),
        noise_var.reshape(row),
    )


def split_dot(w, x):
    high = w.astype(BF16)
    low = (w - high.astype(F32)).astype(BF16)
    total = jnp.dot(high, x, preferred_element_type=F32)
    return (total + jnp.dot(low, x, preferred_element_type=F32)).astype(BF16)


def pack(chunk, weight, tile_map, where, rows_axis, cols_axis):
    block_rows, columns = chunk.shape
    tiles = tile_map.shape[0]
    size = columns // tiles
    pairs = rows_axis // 2
    per_row, per_col = tiles // rows_axis, tiles // cols_axis
    wide = (2 * per_row + per_col) * size

    def kernel(map_ref, where_ref, x_ref, *refs):
        outs = refs[-pairs - 1 : -1]
        held = refs[-1]
        row, col = where_ref[0], where_ref[1]

        def fetch(base, count, to):
            for j in range(count):
                at = pl.multiple_of(map_ref[base + j] * size, size)
                held[:, (to + j) * size : (to + j + 1) * size] = x_ref[:, pl.ds(at, size)]

        def finish(start, stop, targets):
            part = held[:, start:stop]
            if weight is not None:
                part = split_dot(refs[0][...], part)
            for target in targets:
                target[:, start:stop] = part

        own = per_row * size
        fetch(col * per_col, per_col, 2 * per_row)
        finish(2 * own, wide, outs)
        for n in range(pairs):
            there = jnp.bitwise_xor(row, 2 * n)
            fetch(there * per_row, per_row, 0)
            fetch(jnp.bitwise_xor(there, 1) * per_row, per_row, per_row)
            finish(0, 2 * own, [outs[n]])

    args = (tile_map, where, chunk) + (() if weight is None else (weight,))
    return pl.pallas_call(
        kernel,
        name="pack",
        in_specs=[SMEM, SMEM] + [VMEM] * (len(args) - 2),
        out_specs=[VMEM] * pairs,
        out_shape=[jax.ShapeDtypeStruct((block_rows, wide), BF16)] * pairs,
        scratch_shapes=[pltpu.VMEM((block_rows, wide), BF16)],
        cost_estimate=pl.CostEstimate(flops=10**9, bytes_accessed=5 * 10**6, transcendentals=0),
        compiler_params=pltpu.CompilerParams(vmem_limit_bytes=24 << 20),
    )(*args)


def gram_first(raw, weights, white, obs, rows_width, cols_width):
    block_rows, wide = raw[0].shape
    count = len(raw) + len(white)
    depth = count * block_rows
    half = rows_width // 2
    step = cols_width // 6 if cols_width % 6 == 0 and (cols_width // 6) % 128 == 0 else 128
    steps = cols_width // step

    def kernel(*refs):
        blocks = refs[:count]
        w_refs = refs[count : count + len(raw)]
        obs_ref = refs[count + len(raw)]
        keep_ref, give_ref, rhs_ref = refs[-7:-4]
        fresh, held, turned, sems = refs[-4:]

        @pl.when(pl.program_id(0) == 0)
        def _():
            copies = []
            for b in range(count):
                to = fresh.at[b] if b < len(raw) else held.at[pl.ds(b * block_rows, block_rows)]
                copies.append(pltpu.make_async_copy(blocks[b], to, sems.at[b]))
                copies[-1].start()
            for b in range(count):
                rows = slice(b * block_rows, (b + 1) * block_rows)
                copies[b].wait()
                if b < len(raw):
                    held[rows, :] = split_dot(w_refs[b][...], fresh[b])
                turned[:, rows] = held[rows, :rows_width].T
            spread = jnp.broadcast_to(obs_ref[...].astype(BF16), (16, depth))
            rhs_ref[...] = jnp.dot(spread, held[:, :rows_width], preferred_element_type=F32)

        at = pl.multiple_of(rows_width + pl.program_id(0) * step, 128)
        right = held[:, pl.ds(at, step)]
        keep_ref[...] = jnp.dot(turned[:half, :], right, preferred_element_type=F32)
        give_ref[...] = jnp.dot(turned[half:, :], right, preferred_element_type=F32)

    tile = pl.BlockSpec((half, step), lambda i: (0, i))
    return pl.pallas_call(
        kernel,
        name="gram_first",
        grid=(steps,),
        in_specs=[ANY] * count + [VMEM] * (len(raw) + 1),
        out_specs=[tile, tile, pl.BlockSpec((16, rows_width), lambda i: (0, 0))],
        out_shape=[jax.ShapeDtypeStruct((half, cols_width), F32)] * 2
        + [jax.ShapeDtypeStruct((16, rows_width), F32)],
        scratch_shapes=[
            pltpu.VMEM((len(raw), block_rows, wide), BF16),
            pltpu.VMEM((depth, wide), BF16),
            pltpu.VMEM((rows_width, depth), BF16),
            pltpu.SemaphoreType.DMA((count,)),
        ],
        cost_estimate=pl.CostEstimate(
            flops=2 * depth * rows_width * cols_width, bytes_accessed=2 * 10**7, transcendentals=0
        ),
        compiler_params=pltpu.CompilerParams(vmem_limit_bytes=48 << 20),
    )(*raw, *white, *weights, obs)


def gram_last(keep, other, mine, theirs, obs, rows_width, cols_width):
    block_rows, wide = mine[0].shape
    count = len(mine) + len(theirs)
    depth = count * block_rows
    half = rows_width // 2
    step = cols_width // 6 if cols_width % 6 == 0 and (cols_width // 6) % 128 == 0 else 128
    steps = cols_width // step

    def kernel(*refs):
        keep_ref, other_ref = refs[:2]
        blocks = refs[2 : 2 + count]
        obs_ref = refs[2 + count]
        out_ref, rhs_ref = refs[-5:-3]
        held, turned, sems = refs[-3:]

        @pl.when(pl.program_id(0) == 0)
        def _():
            copies = []
            for b in range(count):
                to = held.at[pl.ds(b * block_rows, block_rows)]
                copies.append(pltpu.make_async_copy(blocks[b], to, sems.at[b]))
                copies[-1].start()
            total = jnp.zeros((16, half), F32)
            for b in range(count):
                rows = slice(b * block_rows, (b + 1) * block_rows)
                lead = 0 if b < len(mine) else half
                copies[b].wait()
                left = held[rows, lead : lead + half]
                turned[:, rows] = left.T
                spread = jnp.broadcast_to(obs_ref[:, rows].astype(BF16), (16, block_rows))
                total = total + jnp.dot(spread, left, preferred_element_type=F32)
            rhs_ref[...] = total

        at = pl.multiple_of(rows_width + pl.program_id(0) * step, 128)
        right = held[:, pl.ds(at, step)]
        out_ref[...] = (keep_ref[...] + other_ref[...]) + jnp.dot(
            turned[...], right, preferred_element_type=F32
        )

    tile = pl.BlockSpec((half, step), lambda i: (0, i))
    return pl.pallas_call(
        kernel,
        name="gram_last",
        grid=(steps,),
        in_specs=[tile, tile] + [ANY] * count + [VMEM],
        out_specs=[tile, pl.BlockSpec((16, half), lambda i: (0, 0))],
        out_shape=[
            jax.ShapeDtypeStruct((half, cols_width), F32),
            jax.ShapeDtypeStruct((16, half), F32),
        ],
        scratch_shapes=[
            pltpu.VMEM((depth, wide), BF16),
            pltpu.VMEM((half, depth), BF16),
            pltpu.SemaphoreType.DMA((count,)),
        ],
        cost_estimate=pl.CostEstimate(
            flops=2 * depth * half * cols_width, bytes_accessed=2 * 10**7, transcendentals=0
        ),
        compiler_params=pltpu.CompilerParams(vmem_limit_bytes=48 << 20),
    )(keep, other, *mine, *theirs, obs)


def on_device_any(
    rows_axis,
    cols_axis,
    design,
    observations,
    gaps,
    noise_var,
    arc_lengths,
    arc_amp,
    arc_decay,
    plan,
    tile_map,
):
    columns = design.shape[1]
    tiles = tile_map.shape[0]
    size = columns // tiles
    pairs = rows_axis // 2
    rows_width = 2 * (tiles // rows_axis) * size
    cols_width = (tiles // cols_axis) * size
    row, col = lax.axis_index("row"), lax.axis_index("col")
    where = jnp.stack([row, col]).astype(jnp.int32)

    def ring(x, shift):
        return lax.ppermute(x, "col", [(c, (c + shift) % cols_axis) for c in range(cols_axis)])

    def swap(x, mask):
        return lax.ppermute(x, "row", [(r, r ^ mask) for r in range(rows_axis)])

    def spread(parts):
        return [parts[0]] + [swap(parts[n], 2 * n) for n in range(1, pairs)]

    chunks = [design]
    for _ in range(1, cols_axis):
        chunks.append(ring(chunks[-1], 1))

    block_rows = design.shape[0]
    near = factor_kernel(observations, gaps, noise_var, arc_lengths, arc_amp, arc_decay)
    weight = near[:block_rows]
    line = [near] + [ring(near, s) for s in range(1, cols_axis)]
    line_obs = jnp.stack([part[block_rows] for part in line])
    obs_all = jnp.stack([line_obs] + [swap(line_obs, m) for m in range(1, rows_axis)])

    packed = [spread(pack(design, None, tile_map, where, rows_axis, cols_axis))]
    for s in range(1, cols_axis):
        weight_s = line[s][:block_rows]
        packed.append(spread(pack(chunks[s], weight_s, tile_map, where, rows_axis, cols_axis)))

    weights = [weight] + [swap(weight, 2 * n) for n in range(1, pairs)]
    obs_first = obs_all[::2, : cols_axis - 1].swapaxes(0, 1).reshape(1, -1)
    keep, give, rhs_first = gram_first(
        packed[0],
        weights,
        [block for s in range(1, cols_axis - 1) for block in packed[s]],
        obs_first,
        rows_width,
        cols_width,
    )
    half = rows_width // 2
    other = swap(give, 1)
    other_rhs = swap(rhs_first[0, half:], 1)
    theirs = [swap(block, 1) for block in packed[-1]]
    obs_last = jnp.concatenate([obs_all[::2, -1], obs_all[1::2, -1]], axis=0).reshape(1, -1)
    gram, rhs_last = gram_last(
        keep, other, packed[-1], theirs, obs_last, rows_width, cols_width
    )
    normal_rhs = rhs_first[0, :half] + other_rhs + rhs_last[0]
    from_row, from_col = plan // cols_axis, plan % cols_axis
    ahead = (col - from_col + cols_axis) % cols_axis
    place = jnp.bitwise_xor(from_row, row) * cols_axis + ahead
    balanced_obs = jnp.take(obs_all.reshape(-1, block_rows), place, axis=0)
    return (gram, normal_rhs, balanced_obs)


def pack_cut(chunk, near, tile_map, where, rows_axis, cols_axis, first):
    block_rows, columns = chunk.shape
    tiles = tile_map.shape[0]
    size = columns // tiles
    per_row, per_col = tiles // rows_axis, tiles // cols_axis
    own = per_row * size
    rows_width, cols_width = 2 * own, per_col * size
    half = cols_width // 2

    def kernel(map_ref, where_ref, x_ref, near_ref, *refs):
        across_a, across_b, along_a, along_b, keep = refs[:5]
        held = refs[-1]
        row, col = where_ref[0], where_ref[1]
        weight = near_ref[:block_rows]

        def fetch(base, count, width):
            for j in range(count):
                at = pl.multiple_of(map_ref[base + j] * size, size)
                held[:, j * size : (j + 1) * size] = x_ref[:, pl.ds(at, size)]
            return split_dot(weight, held[:, :width])

        def rows_of(n, core):
            there = jnp.bitwise_xor(row, 2 * n + core)
            return fetch(there * per_row, per_row, own)

        part = fetch(col * per_col, per_col, cols_width)
        keep[:, rows_width:] = part
        across_a[:, own:] = part[:, :half]
        along_b[:, rows_width:] = part[:, :half]
        across_b[:, rows_width:] = part[:, half:]
        along_a[:, own:] = part[:, half:]
        across_a[:, :own] = rows_of(3, 0)
        along_a[:, :own] = rows_of(3, 1)
        for n, target in ((1, across_b), (2, along_b), (0, keep)):
            target[:, :own] = rows_of(n, 0)
            target[:, own:rows_width] = rows_of(n, 1)
        if first:
            before = jnp.where(col == 0, cols_axis - 1, col - 1)
            refs[5][...] = fetch(before * per_col, per_col, cols_width)

    widths = [own + half, rows_width + half, own + half, rows_width + half, rows_width + cols_width]
    widths += [cols_width] if first else []
    return pl.pallas_call(
        kernel,
        name="pack_cut",
        in_specs=[SMEM, SMEM, VMEM, VMEM],
        out_specs=[VMEM] * len(widths),
        out_shape=[jax.ShapeDtypeStruct((block_rows, w), BF16) for w in widths],
        scratch_shapes=[pltpu.VMEM((block_rows, max(rows_width, cols_width)), BF16)],
        cost_estimate=pl.CostEstimate(flops=10**9, bytes_accessed=5 * 10**6, transcendentals=0),
        compiler_params=pltpu.CompilerParams(vmem_limit_bytes=8 << 20),
    )(tile_map, where, chunk, near)


def row_parts(keep, xb, yb, fa, fb, own):
    block_rows = keep.shape[0]

    def kernel(keep_ref, xb_ref, yb_ref, fa_ref, fb_ref, lead_ref, rest_ref):
        for n, ref in enumerate((keep_ref, xb_ref, yb_ref)):
            lead_ref[n * block_rows : (n + 1) * block_rows, :] = ref[:, :own]
            rest_ref[n * block_rows : (n + 1) * block_rows, :] = ref[:, own : 2 * own]
        lead_ref[3 * block_rows :, :] = fa_ref[:, :own]
        rest_ref[3 * block_rows :, :] = fb_ref[:, :own]

    return pl.pallas_call(
        kernel,
        name="row_parts",
        in_specs=[VMEM] * 5,
        out_specs=[VMEM] * 2,
        out_shape=[jax.ShapeDtypeStruct((4 * block_rows, own), BF16)] * 2,
        cost_estimate=pl.CostEstimate(flops=10**9, bytes_accessed=5 * 10**6, transcendentals=0),
        compiler_params=pltpu.CompilerParams(vmem_limit_bytes=4 << 20),
    )(keep, xb, yb, fa, fb)


def obs_rows(obs, places, plan, where, cols_axis):
    block_rows = obs[0].shape[1]

    def kernel(plan_ref, where_ref, *refs):
        sources, (rows_ref, picked_ref) = refs[:-2], refs[-2:]
        for b, (m, s) in enumerate(places):
            line = jnp.broadcast_to(sources[m][s : s + 1, :], (8, block_rows))
            rows_ref[:, b * block_rows : (b + 1) * block_rows] = line
        from_row = lax.div(plan_ref[0], cols_axis)
        from_col = lax.rem(plan_ref[0], cols_axis)
        mask = jnp.bitwise_xor(from_row, where_ref[0])
        step = lax.rem(where_ref[1] - from_col + cols_axis, cols_axis)
        picked = jnp.zeros((1, block_rows), F32)
        for m, source in enumerate(sources):
            picked = jnp.where(mask == m, source[pl.ds(step, 1), :], picked)
        picked_ref[...] = picked

    return pl.pallas_call(
        kernel,
        name="obs_rows",
        in_specs=[SMEM, SMEM] + [VMEM] * len(obs),
        out_specs=[VMEM] * 2,
        out_shape=[
            jax.ShapeDtypeStruct((8, len(places) * block_rows), F32),
            jax.ShapeDtypeStruct((1, block_rows), F32),
        ],
        cost_estimate=pl.CostEstimate(flops=10**7, bytes_accessed=10**5, transcendentals=0),
        compiler_params=pltpu.CompilerParams(vmem_limit_bytes=4 << 20),
    )(plan, where, *obs)


def gram_tiles(pieces, operands, rows, at_row, depth, left_width, cols_width, before):
    count = len(operands)
    halves = 1 if before else 2
    width = left_width // halves
    step = cols_width // 6 if cols_width % 6 == 0 and (cols_width // 6) % 128 == 0 else 128
    steps = cols_width // step
    block_rows = 128 if depth % 128 == 0 else depth

    def kernel(*refs):
        sources = refs[:count]
        rows_ref = refs[count]
        sums = refs[count + 1 : count + 1 + len(before)]
        outs = refs[count + 1 + len(before) : -4]
        held, turned, seen, sems = refs[-4:]

        @pl.when(pl.program_id(0) == 0)
        def _():
            copies = [
                pltpu.make_async_copy(
                    rows_ref.at[:, pl.ds(at_row, depth)], seen, sems.at[len(pieces)]
                )
            ]
            copies[0].start()
            for k, (which, src, to_row, to_col) in enumerate(pieces):
                source = sources[which].at[:, pl.ds(src[0], src[1])]
                target = held.at[pl.ds(to_row, operands[which].shape[0]), pl.ds(to_col, src[1])]
                copies.append(pltpu.make_async_copy(source, target, sems.at[k]))
                copies[-1].start()
            for copy in copies:
                copy.wait()
            for b in range(depth // block_rows):
                part = slice(b * block_rows, (b + 1) * block_rows)
                turned[:, part] = held[part, :left_width].T
            total = jnp.dot(
                seen[...].astype(BF16), held[:, :left_width], preferred_element_type=F32
            )
            if before:
                outs[1][...] = total + (sums[2][...] + sums[3][...])
            else:
                outs[2][...] = total[:, :width]
                outs[3][...] = total[:, width:]

        at = pl.multiple_of(left_width + pl.program_id(0) * step, 128)
        right = held[:, pl.ds(at, step)]
        for h in range(halves):
            part = jnp.dot(
                turned[h * width : (h + 1) * width, :], right, preferred_element_type=F32
            )
            outs[h][...] = part + (sums[0][...] + sums[1][...]) if before else part

    tile = pl.BlockSpec((width, step), lambda i: (0, i))
    whole = pl.BlockSpec((8, width), lambda i: (0, 0))
    held_bytes = 2 * depth * (2 * left_width + cols_width)
    tile_bytes = 4 * width * step * 2 * (len(before) // 2 + halves)
    return pl.pallas_call(
        kernel,
        grid=(steps,),
        in_specs=[ANY] * (count + 1) + ([tile, tile, whole, whole] if before else []),
        out_specs=[tile] * halves + [whole] * halves,
        out_shape=[jax.ShapeDtypeStruct((width, cols_width), F32)] * halves
        + [jax.ShapeDtypeStruct((8, width), F32)] * halves,
        scratch_shapes=[
            pltpu.VMEM((depth, left_width + cols_width), BF16),
            pltpu.VMEM((left_width, depth), BF16),
            pltpu.VMEM((8, depth), F32),
            pltpu.SemaphoreType.DMA((len(pieces) + 1,)),
        ],
        cost_estimate=pl.CostEstimate(
            flops=2 * depth * left_width * cols_width, bytes_accessed=2 * 10**7, transcendentals=0
        ),
        compiler_params=pltpu.CompilerParams(
            vmem_limit_bytes=held_bytes + tile_bytes + (6 << 20)
        ),
    )(*operands, rows, *before)


def on_device_square(
    rows_axis,
    cols_axis,
    design,
    observations,
    gaps,
    noise_var,
    arc_lengths,
    arc_amp,
    arc_decay,
    plan,
    tile_map,
):
    block_rows, columns = design.shape
    tiles = tile_map.shape[0]
    size = columns // tiles
    own = (tiles // rows_axis) * size
    wide = 2 * own
    cols_width = (tiles // cols_axis) * size
    half = cols_width // 2
    row, col = lax.axis_index("row"), lax.axis_index("col")
    where = jnp.stack([row, col]).astype(jnp.int32)
    last = cols_axis - 1

    def ring(x, shift):
        return lax.ppermute(x, "col", [(c, (c + shift) % cols_axis) for c in range(cols_axis)])

    def swap(x, mask):
        return lax.ppermute(x, "row", [(r, r ^ mask) for r in range(rows_axis)])

    chunks = [design]
    for _ in range(1, last):
        chunks.append(ring(chunks[-1], 1))
    near = factor_kernel(observations, gaps, noise_var, arc_lengths, arc_amp, arc_decay)
    line = [near] + [ring(near, s) for s in range(1, cols_axis)]
    line_obs = jnp.stack([part[block_rows] for part in line])
    obs = [line_obs] + [swap(line_obs, m) for m in range(1, rows_axis)]

    traded = []
    for s in range(last):
        parts = pack_cut(
            chunks[s], line[s], tile_map, where, rows_axis, cols_axis, s == 0
        )
        if s == 0:
            before = parts[5]
        xa, xb, ya, yb, keep = parts[:5]
        xa, ya = swap(xa, 2), swap(ya, 4)
        xb, yb = swap(xb, 2), swap(yb, 4)
        fa, fb = swap(xa, 4), swap(ya, 2)
        traded.append((keep, xa, xb, ya, yb, fa, fb))

    keep, xa, xb, ya, yb, fa, fb = traded[0]
    lead, rest = row_parts(keep, xb, yb, fa, fb, own)
    far_cols = ring(before, last)
    far_rest = ring(rest, last)
    far_lead = ring(lead, last)
    x3, y3 = swap(far_cols, 2), swap(far_cols, 4)
    fa3 = swap(x3[:, :half], 4)
    fb3 = swap(y3[:, half:], 2)

    early = [(2 * n, s) for s in range(last - 1) for n in range(4)]
    late = [(2 * n + core, s) for s in (last - 1, last) for core in (0, 1) for n in range(4)]
    rows, balanced_obs = obs_rows(obs, early + late, plan, where, cols_axis)

    def chunk_pieces(start, first, lefts, to_cols):
        out = []
        for block, (source, begin, length, to) in (
            [(n, (k, *lefts)) for n, k in ((0, 0), (1, 2), (2, 4))]
            + [
                (0, (0, wide, cols_width, to_cols)),
                (1, (1, own, half, to_cols)),
                (1, (2, wide, half, to_cols + half)),
                (2, (4, wide, half, to_cols)),
                (2, (3, own, half, to_cols + half)),
                (3, (5, own, half, to_cols)),
                (3, (6, own, half, to_cols + half)),
            ]
        ):
            out.append((first + source, (begin, length), start + block * block_rows, to))
        return out

    pieces, operands = [], []
    for s in range(last - 1):
        start, first = 4 * s * block_rows, len(operands)
        pieces += chunk_pieces(start, first, (0, wide, 0), wide)
        pieces += [
            (first + 5, (0, own), start + 3 * block_rows, 0),
            (first + 6, (0, own), start + 3 * block_rows, own),
        ]
        operands += list(traded[s])
    keep, give, keep_rhs, give_rhs = gram_tiles(
        pieces, operands, rows, 0, len(early) * block_rows, wide, cols_width, ()
    )
    other = swap(give, 1)
    other_rhs = swap(give_rhs, 1)

    mine = list(traded[last - 1])
    theirs = [swap(v, 1) for v in mine]
    mine_far = [far_cols, x3, y3, fa3, fb3]
    theirs_far = [swap(v, 1) for v in mine_far]
    their_rest = swap(far_rest, 1)
    quad = 4 * block_rows
    operands = mine + theirs
    pieces = chunk_pieces(0, 0, (0, own, 0), own)
    pieces.append((5, (0, own), 3 * block_rows, 0))
    pieces += chunk_pieces(quad, 7, (own, own, 0), own)
    pieces.append((7 + 6, (0, own), quad + 3 * block_rows, 0))
    for start, left, group in ((2 * quad, far_lead, mine_far), (3 * quad, their_rest, theirs_far)):
        first = len(operands)
        operands += [left] + group
        pieces.append((first, (0, own), start, 0))
        for n, (k, length, to) in enumerate(
            ((1, cols_width, own), (2, cols_width, own), (3, cols_width, own), (4, half, own))
        ):
            pieces.append((first + k, (0, length), start + n * block_rows, to))
        pieces.append((first + 5, (0, half), start + 3 * block_rows, own + half))
    gram, rhs = gram_tiles(
        pieces,
        operands,
        rows,
        len(early) * block_rows,
        len(late) * block_rows,
        own,
        cols_width,
        (keep, other, keep_rhs, other_rhs),
    )
    return (gram, rhs[0], balanced_obs)


def solution(mesh):
    placed = (
        P(("row", "col"), None),
        P(("row", "col")),
        P(("row", "col")),
        P(("row", "col")),
        P(("row", "col"), None),
        P(("row", "col"), None),
        P(("row", "col"), None),
        P(("row", "col")),
        P(),
    )
    rows_axis, cols_axis = mesh.shape["row"], mesh.shape["col"]
    square = rows_axis == 2**3 and cols_axis > 2

    def body(*args):
        if not square:
            return on_device_any(rows_axis, cols_axis, *args)
        return on_device_square(rows_axis, cols_axis, *args)

    return jax.shard_map(
        body,
        mesh=mesh,
        in_specs=placed,
        out_specs=(P("row", "col"), P("row"), P(("row", "col"), None)),
        check_vma=False,
    )
```

```python
import jax
import jax.numpy as jnp
from jax import lax
from jax.experimental import pallas as pl
from jax.experimental.pallas import tpu as pltpu
from jax.sharding import PartitionSpec as P


F32, BF16 = jnp.float32, jnp.bfloat16
ANY = pl.BlockSpec(memory_space=pl.ANY)
VMEM = pl.BlockSpec(memory_space=pltpu.VMEM)
SMEM = pl.BlockSpec(memory_space=pltpu.SMEM)


def factor_math(n, arcs, len_ref, amp_ref, decay_ref, obs_ref, gap_ref, noise_ref):
    lane = lax.broadcasted_iota(jnp.int32, (8, n), 1)
    live = jnp.broadcast_to(gap_ref[...].astype(F32), (8, n))
    noise = jnp.broadcast_to(noise_ref[...], (8, n))
    big_line = lax.broadcasted_iota(jnp.int32, (n, n), 0)
    big_lane = lax.broadcasted_iota(jnp.int32, (n, n), 1)
    arc = jnp.zeros((8, n), jnp.int32)
    first = lane == 0
    arc_line = jnp.zeros((n, n), jnp.int32)
    end = 0
    for k in range(arcs):
        end = end + len_ref[0, k]
        arc = arc + (lane >= end).astype(jnp.int32)
        arc_line = arc_line + (big_line >= end).astype(jnp.int32)
        first = jnp.logical_or(first, lane == end)
    amp = jnp.zeros((8, n), F32)
    decay = jnp.ones((8, n), F32)
    for k in range(arcs):
        amp = jnp.where(arc == k, amp_ref[0, k], amp)
        decay = jnp.where(arc == k, decay_ref[0, k], decay)

    def back(x, shift):
        return pltpu.roll(x, shift, axis=1)

    fresh = (1.0 - decay * decay) * amp
    a = back(decay * decay * noise + fresh * live, 1)
    b = back(fresh * noise, 1)
    c = back(live, 1)
    d = back(noise, 1)
    a = jnp.where(first, 0.0, a)
    b = jnp.where(first, amp, b)
    c = jnp.where(first, 0.0, c)
    d = jnp.where(first, 1.0, d)
    shift = 1
    while shift < n:
        ok = lane >= shift
        pa, pb = jnp.where(ok, back(a, shift), 1.0), jnp.where(ok, back(b, shift), 0.0)
        pc, pd = jnp.where(ok, back(c, shift), 0.0), jnp.where(ok, back(d, shift), 1.0)
        a, b, c, d = a * pa + b * pc, a * pb + b * pd, c * pa + d * pc, c * pb + d * pd
        level = 1.0 / (a + b + c + d)
        a, b, c, d = a * level, b * level, c * level, d * level
        shift *= 2
    variance = b / d
    total = live * variance + noise
    root = 1.0 / jnp.sqrt(total)
    fade = jnp.log(decay * noise / total)
    gain = decay * variance * live / total
    below = big_lane < big_line
    fades = jnp.where(below, jnp.broadcast_to(fade[:1], (n, n)), 0.0)
    mask = below.astype(BF16)
    spans = jnp.zeros((n, n), F32)
    for _ in range(3):
        part = fades.astype(BF16)
        spans = spans + jnp.dot(part, mask, preferred_element_type=F32)
        fades = fades - part.astype(F32)
    diagonal = big_line == big_lane

    def upright(x):
        return jnp.sum(jnp.where(diagonal, jnp.broadcast_to(x[:1], (n, n)), 0.0), axis=1, keepdims=True)

    left = upright(live * root)
    same = jnp.logical_and(below, arc_line == jnp.broadcast_to(arc[:1], (n, n)))
    weight = jnp.where(same, -left * jnp.exp(spans) * jnp.broadcast_to(gain[:1], (n, n)), 0.0)
    weight = jnp.where(diagonal, left, weight)
    white = jnp.sum(weight * jnp.broadcast_to(obs_ref[...], (n, n)), axis=1, keepdims=True)
    white_row = jnp.sum(jnp.where(diagonal, white, 0.0), axis=0, keepdims=True)
    return weight, jnp.broadcast_to(white_row, (8, n))


def factor_kernel(observations, gaps, noise_var, arc_lengths, arc_amp, arc_decay):
    n = observations.shape[0]
    arcs = arc_lengths.shape[1]

    def kernel(len_ref, amp_ref, decay_ref, obs_ref, gap_ref, noise_ref, out_ref):
        out_ref[:n, :], out_ref[n:, :] = factor_math(
            n, arcs, len_ref, amp_ref, decay_ref, obs_ref, gap_ref, noise_ref
        )

    row = (1, n)
    return pl.pallas_call(
        kernel,
        name="factor",
        in_specs=[SMEM] * 3 + [VMEM] * 3,
        out_specs=VMEM,
        out_shape=jax.ShapeDtypeStruct((n + 8, n), F32),
        cost_estimate=pl.CostEstimate(flops=10**8, bytes_accessed=10**5, transcendentals=0),
        compiler_params=pltpu.CompilerParams(vmem_limit_bytes=4 << 20),
    )(
        arc_lengths,
        arc_amp,
        arc_decay,
        observations.reshape(row),
        gaps.reshape(row),
        noise_var.reshape(row),
    )


def split_dot(w, x):
    high = w.astype(BF16)
    low = (w - high.astype(F32)).astype(BF16)
    total = jnp.dot(high, x, preferred_element_type=F32)
    return (total + jnp.dot(low, x, preferred_element_type=F32)).astype(BF16)


def pack(chunk, weight, tile_map, where, rows_axis, cols_axis):
    block_rows, columns = chunk.shape
    tiles = tile_map.shape[0]
    size = columns // tiles
    pairs = rows_axis // 2
    per_row, per_col = tiles // rows_axis, tiles // cols_axis
    wide = (2 * per_row + per_col) * size

    def kernel(map_ref, where_ref, x_ref, *refs):
        outs = refs[-pairs - 1 : -1]
        held = refs[-1]
        row, col = where_ref[0], where_ref[1]

        def fetch(base, count, to):
            for j in range(count):
                at = pl.multiple_of(map_ref[base + j] * size, size)
                held[:, (to + j) * size : (to + j + 1) * size] = x_ref[:, pl.ds(at, size)]

        def finish(start, stop, targets):
            part = held[:, start:stop]
            if weight is not None:
                part = split_dot(refs[0][...], part)
            for target in targets:
                target[:, start:stop] = part

        own = per_row * size
        fetch(col * per_col, per_col, 2 * per_row)
        finish(2 * own, wide, outs)
        for n in range(pairs):
            there = jnp.bitwise_xor(row, 2 * n)
            fetch(there * per_row, per_row, 0)
            fetch(jnp.bitwise_xor(there, 1) * per_row, per_row, per_row)
            finish(0, 2 * own, [outs[n]])

    args = (tile_map, where, chunk) + (() if weight is None else (weight,))
    return pl.pallas_call(
        kernel,
        name="pack",
        in_specs=[SMEM, SMEM] + [VMEM] * (len(args) - 2),
        out_specs=[VMEM] * pairs,
        out_shape=[jax.ShapeDtypeStruct((block_rows, wide), BF16)] * pairs,
        scratch_shapes=[pltpu.VMEM((block_rows, wide), BF16)],
        cost_estimate=pl.CostEstimate(flops=10**9, bytes_accessed=5 * 10**6, transcendentals=0),
        compiler_params=pltpu.CompilerParams(vmem_limit_bytes=24 << 20),
    )(*args)


def gram_first(raw, weights, white, obs, rows_width, cols_width):
    block_rows, wide = raw[0].shape
    count = len(raw) + len(white)
    depth = count * block_rows
    half = rows_width // 2
    step = cols_width // 6 if cols_width % 6 == 0 and (cols_width // 6) % 128 == 0 else 128
    steps = cols_width // step

    def kernel(*refs):
        blocks = refs[:count]
        w_refs = refs[count : count + len(raw)]
        obs_ref = refs[count + len(raw)]
        keep_ref, give_ref, rhs_ref = refs[-7:-4]
        fresh, held, turned, sems = refs[-4:]

        @pl.when(pl.program_id(0) == 0)
        def _():
            copies = []
            for b in range(count):
                to = fresh.at[b] if b < len(raw) else held.at[pl.ds(b * block_rows, block_rows)]
                copies.append(pltpu.make_async_copy(blocks[b], to, sems.at[b]))
                copies[-1].start()
            for b in range(count):
                rows = slice(b * block_rows, (b + 1) * block_rows)
                copies[b].wait()
                if b < len(raw):
                    held[rows, :] = split_dot(w_refs[b][...], fresh[b])
                turned[:, rows] = held[rows, :rows_width].T
            spread = jnp.broadcast_to(obs_ref[...].astype(BF16), (16, depth))
            rhs_ref[...] = jnp.dot(spread, held[:, :rows_width], preferred_element_type=F32)

        at = pl.multiple_of(rows_width + pl.program_id(0) * step, 128)
        right = held[:, pl.ds(at, step)]
        keep_ref[...] = jnp.dot(turned[:half, :], right, preferred_element_type=F32)
        give_ref[...] = jnp.dot(turned[half:, :], right, preferred_element_type=F32)

    tile = pl.BlockSpec((half, step), lambda i: (0, i))
    return pl.pallas_call(
        kernel,
        name="gram_first",
        grid=(steps,),
        in_specs=[ANY] * count + [VMEM] * (len(raw) + 1),
        out_specs=[tile, tile, pl.BlockSpec((16, rows_width), lambda i: (0, 0))],
        out_shape=[jax.ShapeDtypeStruct((half, cols_width), F32)] * 2
        + [jax.ShapeDtypeStruct((16, rows_width), F32)],
        scratch_shapes=[
            pltpu.VMEM((len(raw), block_rows, wide), BF16),
            pltpu.VMEM((depth, wide), BF16),
            pltpu.VMEM((rows_width, depth), BF16),
            pltpu.SemaphoreType.DMA((count,)),
        ],
        cost_estimate=pl.CostEstimate(
            flops=2 * depth * rows_width * cols_width, bytes_accessed=2 * 10**7, transcendentals=0
        ),
        compiler_params=pltpu.CompilerParams(vmem_limit_bytes=48 << 20),
    )(*raw, *white, *weights, obs)


def gram_last(keep, other, mine, theirs, obs, rows_width, cols_width):
    block_rows, wide = mine[0].shape
    count = len(mine) + len(theirs)
    depth = count * block_rows
    half = rows_width // 2
    step = cols_width // 6 if cols_width % 6 == 0 and (cols_width // 6) % 128 == 0 else 128
    steps = cols_width // step

    def kernel(*refs):
        keep_ref, other_ref = refs[:2]
        blocks = refs[2 : 2 + count]
        obs_ref = refs[2 + count]
        out_ref, rhs_ref = refs[-5:-3]
        held, turned, sems = refs[-3:]

        @pl.when(pl.program_id(0) == 0)
        def _():
            copies = []
            for b in range(count):
                to = held.at[pl.ds(b * block_rows, block_rows)]
                copies.append(pltpu.make_async_copy(blocks[b], to, sems.at[b]))
                copies[-1].start()
            total = jnp.zeros((16, half), F32)
            for b in range(count):
                rows = slice(b * block_rows, (b + 1) * block_rows)
                lead = 0 if b < len(mine) else half
                copies[b].wait()
                left = held[rows, lead : lead + half]
                turned[:, rows] = left.T
                spread = jnp.broadcast_to(obs_ref[:, rows].astype(BF16), (16, block_rows))
                total = total + jnp.dot(spread, left, preferred_element_type=F32)
            rhs_ref[...] = total

        at = pl.multiple_of(rows_width + pl.program_id(0) * step, 128)
        right = held[:, pl.ds(at, step)]
        out_ref[...] = (keep_ref[...] + other_ref[...]) + jnp.dot(
            turned[...], right, preferred_element_type=F32
        )

    tile = pl.BlockSpec((half, step), lambda i: (0, i))
    return pl.pallas_call(
        kernel,
        name="gram_last",
        grid=(steps,),
        in_specs=[tile, tile] + [ANY] * count + [VMEM],
        out_specs=[tile, pl.BlockSpec((16, half), lambda i: (0, 0))],
        out_shape=[
            jax.ShapeDtypeStruct((half, cols_width), F32),
            jax.ShapeDtypeStruct((16, half), F32),
        ],
        scratch_shapes=[
            pltpu.VMEM((depth, wide), BF16),
            pltpu.VMEM((half, depth), BF16),
            pltpu.SemaphoreType.DMA((count,)),
        ],
        cost_estimate=pl.CostEstimate(
            flops=2 * depth * half * cols_width, bytes_accessed=2 * 10**7, transcendentals=0
        ),
        compiler_params=pltpu.CompilerParams(vmem_limit_bytes=48 << 20),
    )(keep, other, *mine, *theirs, obs)


def on_device_any(
    rows_axis,
    cols_axis,
    design,
    observations,
    gaps,
    noise_var,
    arc_lengths,
    arc_amp,
    arc_decay,
    plan,
    tile_map,
):
    columns = design.shape[1]
    tiles = tile_map.shape[0]
    size = columns // tiles
    pairs = rows_axis // 2
    rows_width = 2 * (tiles // rows_axis) * size
    cols_width = (tiles // cols_axis) * size
    row, col = lax.axis_index("row"), lax.axis_index("col")
    where = jnp.stack([row, col]).astype(jnp.int32)

    def ring(x, shift):
        return lax.ppermute(x, "col", [(c, (c + shift) % cols_axis) for c in range(cols_axis)])

    def swap(x, mask):
        return lax.ppermute(x, "row", [(r, r ^ mask) for r in range(rows_axis)])

    def spread(parts):
        return [parts[0]] + [swap(parts[n], 2 * n) for n in range(1, pairs)]

    chunks = [design]
    for _ in range(1, cols_axis):
        chunks.append(ring(chunks[-1], 1))

    block_rows = design.shape[0]
    near = factor_kernel(observations, gaps, noise_var, arc_lengths, arc_amp, arc_decay)
    weight = near[:block_rows]
    line = [near] + [ring(near, s) for s in range(1, cols_axis)]
    line_obs = jnp.stack([part[block_rows] for part in line])
    obs_all = jnp.stack([line_obs] + [swap(line_obs, m) for m in range(1, rows_axis)])

    packed = [spread(pack(design, None, tile_map, where, rows_axis, cols_axis))]
    for s in range(1, cols_axis):
        weight_s = line[s][:block_rows]
        packed.append(spread(pack(chunks[s], weight_s, tile_map, where, rows_axis, cols_axis)))

    weights = [weight] + [swap(weight, 2 * n) for n in range(1, pairs)]
    obs_first = obs_all[::2, : cols_axis - 1].swapaxes(0, 1).reshape(1, -1)
    keep, give, rhs_first = gram_first(
        packed[0],
        weights,
        [block for s in range(1, cols_axis - 1) for block in packed[s]],
        obs_first,
        rows_width,
        cols_width,
    )
    half = rows_width // 2
    other = swap(give, 1)
    other_rhs = swap(rhs_first[0, half:], 1)
    theirs = [swap(block, 1) for block in packed[-1]]
    obs_last = jnp.concatenate([obs_all[::2, -1], obs_all[1::2, -1]], axis=0).reshape(1, -1)
    gram, rhs_last = gram_last(
        keep, other, packed[-1], theirs, obs_last, rows_width, cols_width
    )
    normal_rhs = rhs_first[0, :half] + other_rhs + rhs_last[0]
    from_row, from_col = plan // cols_axis, plan % cols_axis
    ahead = (col - from_col + cols_axis) % cols_axis
    place = jnp.bitwise_xor(from_row, row) * cols_axis + ahead
    balanced_obs = jnp.take(obs_all.reshape(-1, block_rows), place, axis=0)
    return (gram, normal_rhs, balanced_obs)


def cut_columns(sizes, fetch, row, outs):
    per_row, per_col, own, half, base = sizes
    across_a, across_b, along_a, along_b, keep = outs
    rows_width = 2 * own

    def rows_of(n, core):
        there = jnp.bitwise_xor(row, 2 * n + core)
        return fetch(there * per_row, per_row)

    part = fetch(base, per_col)
    keep[:, rows_width:] = part
    across_a[:, own:] = part[:, :half]
    along_b[:, rows_width:] = part[:, :half]
    across_b[:, rows_width:] = part[:, half:]
    along_a[:, own:] = part[:, half:]
    across_a[:, :own] = rows_of(3, 0)
    along_a[:, :own] = rows_of(3, 1)
    for n, target in ((1, across_b), (2, along_b), (0, keep)):
        target[:, :own] = rows_of(n, 0)
        target[:, own:rows_width] = rows_of(n, 1)


def cut_widths(own, cols_width):
    half = cols_width // 2
    return [own + half, 2 * own + half, own + half, 2 * own + half, 2 * own + cols_width]


def head(design, small, tables, tile_map, where, rows_axis, cols_axis):
    block_rows, columns = design.shape
    tiles = tile_map.shape[0]
    size = columns // tiles
    per_row, per_col = tiles // rows_axis, tiles // cols_axis
    own, cols_width = per_row * size, per_col * size
    arcs = tables[0].shape[1]

    def kernel(where_ref, *refs):
        sources = refs[:8]
        near_ref = refs[8]
        outs = refs[9:14]
        before_ref = refs[14]
        x_ref, obs_ref, gap_ref, noise_ref, len_ref, amp_ref, decay_ref, map_ref, held, sems = refs[15:]
        targets = (x_ref, obs_ref, gap_ref, noise_ref, len_ref, amp_ref, decay_ref, map_ref)
        copies = [
            pltpu.make_async_copy(source, target, sems.at[k])
            for k, (source, target) in enumerate(zip(sources, targets))
        ]
        for copy in copies[1:] + copies[:1]:
            copy.start()
        for copy in copies[1:]:
            copy.wait()
        weight, white = factor_math(
            block_rows, arcs, len_ref, amp_ref, decay_ref, obs_ref, gap_ref, noise_ref
        )
        near_ref[:block_rows, :] = weight
        near_ref[block_rows:, :] = white
        copies[0].wait()
        row, col = where_ref[0], where_ref[1]

        def fetch(base, count):
            for j in range(count):
                at = pl.multiple_of(map_ref[0, base + j] * size, size)
                held[:, j * size : (j + 1) * size] = x_ref[:, pl.ds(at, size)]
            return split_dot(near_ref[:block_rows, :], held[:, : count * size])

        cut_columns((per_row, per_col, own, cols_width // 2, col * per_col), fetch, row, outs)
        before = jnp.where(col == 0, cols_axis - 1, col - 1)
        before_ref[...] = fetch(before * per_col, per_col)

    line = pltpu.VMEM((1, block_rows), F32)
    outs = [(block_rows + 8, block_rows, F32)]
    outs += [(block_rows, w, BF16) for w in cut_widths(own, cols_width) + [cols_width]]
    return pl.pallas_call(
        kernel,
        name="head",
        in_specs=[SMEM] + [ANY] * 8,
        out_specs=[VMEM] * 7,
        out_shape=[jax.ShapeDtypeStruct((h, w), t) for h, w, t in outs],
        scratch_shapes=[
            pltpu.VMEM((block_rows, columns), BF16),
            line,
            pltpu.VMEM((1, block_rows), jnp.int32),
            line,
            pltpu.SMEM((1, arcs), jnp.int32),
            pltpu.SMEM((1, arcs), F32),
            pltpu.SMEM((1, arcs), F32),
            pltpu.SMEM((1, tiles), jnp.int32),
            pltpu.VMEM((block_rows, max(2 * own, cols_width)), BF16),
            pltpu.SemaphoreType.DMA((8,)),
        ],
        cost_estimate=pl.CostEstimate(flops=10**9, bytes_accessed=5 * 10**6, transcendentals=0),
        compiler_params=pltpu.CompilerParams(vmem_limit_bytes=10 << 20),
    )(where, design, *[v.reshape(1, -1) for v in small], *tables, tile_map.reshape(1, -1))


def pack_cut(chunks, near, tile_map, where, rows_axis, cols_axis, begin):
    height, columns = chunks[-1].shape
    tiles = tile_map.shape[0]
    size = columns // tiles
    per_row, per_col = tiles // rows_axis, tiles // cols_axis
    own, cols_width = per_row * size, per_col * size
    depth = begin + height

    def kernel(map_ref, where_ref, near_ref, *refs):
        raw = refs[: len(chunks)]
        outs = refs[len(chunks) : -1]
        held = refs[-1]
        row, col = where_ref[0], where_ref[1]
        weight = near_ref[begin:depth, :depth]

        def fetch(base, count):
            for j in range(count):
                at = pl.multiple_of(map_ref[base + j] * size, size)
                top = 0
                for piece in raw:
                    end = top + piece.shape[0]
                    held[top:end, j * size : (j + 1) * size] = piece[:, pl.ds(at, size)]
                    top = end
            return split_dot(weight, held[:, : count * size])

        cut_columns((per_row, per_col, own, cols_width // 2, col * per_col), fetch, row, outs)

    return pl.pallas_call(
        kernel,
        name="pack_cut",
        in_specs=[SMEM, SMEM, VMEM] + [VMEM] * len(chunks),
        out_specs=[VMEM] * 5,
        out_shape=[jax.ShapeDtypeStruct((height, w), BF16) for w in cut_widths(own, cols_width)],
        scratch_shapes=[pltpu.VMEM((depth, max(own, cols_width)), BF16)],
        cost_estimate=pl.CostEstimate(flops=10**9, bytes_accessed=5 * 10**6, transcendentals=0),
        compiler_params=pltpu.CompilerParams(vmem_limit_bytes=8 << 20),
    )(tile_map, where, near, *chunks)


def row_parts(keep, xb, yb, fa, fb, own):
    block_rows = keep.shape[0]

    def kernel(keep_ref, xb_ref, yb_ref, fa_ref, fb_ref, lead_ref, rest_ref):
        for n, ref in enumerate((keep_ref, xb_ref, yb_ref)):
            lead_ref[n * block_rows : (n + 1) * block_rows, :] = ref[:, :own]
            rest_ref[n * block_rows : (n + 1) * block_rows, :] = ref[:, own : 2 * own]
        lead_ref[3 * block_rows :, :] = fa_ref[:, :own]
        rest_ref[3 * block_rows :, :] = fb_ref[:, :own]

    return pl.pallas_call(
        kernel,
        name="row_parts",
        in_specs=[VMEM] * 5,
        out_specs=[VMEM] * 2,
        out_shape=[jax.ShapeDtypeStruct((4 * block_rows, own), BF16)] * 2,
        cost_estimate=pl.CostEstimate(flops=10**9, bytes_accessed=5 * 10**6, transcendentals=0),
        compiler_params=pltpu.CompilerParams(vmem_limit_bytes=4 << 20),
    )(keep, xb, yb, fa, fb)


def obs_rows(obs, places, plan, where, cols_axis):
    block_rows = obs[0].shape[1]

    def kernel(plan_ref, where_ref, *refs):
        sources, (rows_ref, picked_ref) = refs[:-2], refs[-2:]
        at = 0
        for m, s, (begin, end) in places:
            line = jnp.broadcast_to(sources[m][s : s + 1, :], (8, block_rows))
            rows_ref[:, at : at + end - begin] = line[:, begin:end]
            at += end - begin
        from_row = lax.div(plan_ref[0], cols_axis)
        from_col = lax.rem(plan_ref[0], cols_axis)
        mask = jnp.bitwise_xor(from_row, where_ref[0])
        step = lax.rem(where_ref[1] - from_col + cols_axis, cols_axis)
        picked = jnp.zeros((1, block_rows), F32)
        for m, source in enumerate(sources):
            picked = jnp.where(mask == m, source[pl.ds(step, 1), :], picked)
        picked_ref[...] = picked

    return pl.pallas_call(
        kernel,
        name="obs_rows",
        in_specs=[SMEM, SMEM] + [VMEM] * len(obs),
        out_specs=[VMEM] * 2,
        out_shape=[
            jax.ShapeDtypeStruct((8, sum(end - begin for _, _, (begin, end) in places)), F32),
            jax.ShapeDtypeStruct((1, block_rows), F32),
        ],
        cost_estimate=pl.CostEstimate(flops=10**7, bytes_accessed=10**5, transcendentals=0),
        compiler_params=pltpu.CompilerParams(vmem_limit_bytes=4 << 20),
    )(plan, where, *obs)


def gram_direct(blocks, operands, rows, at_row, left_width, cols_width, before, halves, out_far):
    count = len(operands)
    width = left_width // halves
    step = cols_width // 6 if cols_width % 6 == 0 and (cols_width // 6) % 128 == 0 else 128
    steps = cols_width // step
    depth = sum(block[0] for block in blocks)

    def kernel(*refs):
        sources = refs[:count]
        rows_ref = refs[count]
        sums = refs[count + 1 : count + 1 + len(before)]
        outs = refs[count + 1 + len(before) : count + 1 + len(before) + 2 * halves]
        scratch = refs[count + 1 + len(before) + 2 * halves :]
        turned = scratch[0]
        total = jnp.zeros((8, left_width), F32)
        top = 0
        for height, lefts, _ in blocks:
            seen = rows_ref[:, at_row + top : at_row + top + height].astype(BF16)
            for which, first, begin, length, to in lefts:
                left = sources[which][first : first + height, begin : begin + length]
                turned[to : to + length, top : top + height] = left.T
            left = jnp.concatenate(
                [
                    sources[which][first : first + height, begin : begin + length]
                    for which, first, begin, length, _ in sorted(lefts, key=lambda p: p[4])
                ],
                axis=1,
            )
            total = total + jnp.dot(seen, left, preferred_element_type=F32)
            top += height
        half_sums = len(before) // 2
        for h in range(halves):
            part = total[:, h * width : (h + 1) * width]
            for extra in sums[half_sums:]:
                part = part + extra[...]
            outs[halves + h][...] = part
        copies = [None, None]
        for t in range(steps):
            begin = t * step
            pieces = []
            for height, _, cols in blocks:
                for which, first, start, length, to in cols:
                    if to <= begin < to + length:
                        at = start + begin - to
                        pieces.append(sources[which][first : first + height, at : at + step])
            right = jnp.concatenate(pieces, axis=0)
            for h in range(halves):
                part = jnp.dot(
                    turned[h * width : (h + 1) * width, :], right, preferred_element_type=F32
                )
                for extra in sums[:half_sums]:
                    part = part + extra[:, begin : begin + step]
                if not out_far:
                    outs[h][:, begin : begin + step] = part
                    continue
                tile, sems = scratch[1:]
                slot = t % 2
                if copies[slot] is not None:
                    copies[slot].wait()
                tile[slot] = part
                copies[slot] = pltpu.make_async_copy(
                    tile.at[slot], outs[0].at[:, pl.ds(begin, step)], sems.at[slot]
                )
                copies[slot].start()
        for copy in copies:
            if copy is not None:
                copy.wait()

    scratch_shapes = [pltpu.VMEM((left_width, depth), BF16)]
    scratch_bytes = 2 * left_width * depth
    if out_far:
        scratch_shapes += [pltpu.VMEM((2, width, step), F32), pltpu.SemaphoreType.DMA((2,))]
        scratch_bytes += 8 * width * step
    return pl.pallas_call(
        kernel,
        in_specs=[VMEM] * (count + 1 + len(before)),
        out_specs=[ANY if out_far else VMEM] * halves + [VMEM] * halves,
        out_shape=[jax.ShapeDtypeStruct((width, cols_width), F32)] * halves
        + [jax.ShapeDtypeStruct((8, width), F32)] * halves,
        scratch_shapes=scratch_shapes,
        cost_estimate=pl.CostEstimate(
            flops=2 * depth * left_width * cols_width, bytes_accessed=2 * 10**7, transcendentals=0
        ),
        compiler_params=pltpu.CompilerParams(vmem_limit_bytes=scratch_bytes + (4 << 20)),
    )(*operands, rows, *before)


def on_device_square(
    rows_axis,
    cols_axis,
    design,
    observations,
    gaps,
    noise_var,
    arc_lengths,
    arc_amp,
    arc_decay,
    plan,
    tile_map,
):
    block_rows, columns = design.shape
    tiles = tile_map.shape[0]
    size = columns // tiles
    own = (tiles // rows_axis) * size
    wide = 2 * own
    cols_width = (tiles // cols_axis) * size
    half = cols_width // 2
    row, col = lax.axis_index("row"), lax.axis_index("col")
    where = jnp.stack([row, col]).astype(jnp.int32)
    last = cols_axis - 1

    def ring(x, shift):
        return lax.ppermute(x, "col", [(c, (c + shift) % cols_axis) for c in range(cols_axis)])

    def swap(x, mask):
        return lax.ppermute(x, "row", [(r, r ^ mask) for r in range(rows_axis)])

    middle = block_rows // 2
    chunks = [design]
    for _ in range(1, last - 1):
        chunks.append(ring(chunks[-1], 1))
    halves = [ring(chunks[-1][:middle], 1), ring(chunks[-1][middle:], 1)]
    near, *parts = head(
        design,
        (observations, gaps, noise_var),
        (arc_lengths, arc_amp, arc_decay),
        tile_map,
        where,
        rows_axis,
        cols_axis,
    )
    line = [near] + [ring(near, s) for s in range(1, cols_axis)]
    line_obs = jnp.stack([part[block_rows] for part in line])
    obs = [line_obs] + [swap(line_obs, m) for m in range(1, rows_axis)]

    def trade(xa, xb, ya, yb, keep):
        xa, ya = swap(xa, 2), swap(ya, 4)
        xb, yb = swap(xb, 2), swap(yb, 4)
        return keep, xa, xb, ya, yb, swap(xa, 4), swap(ya, 2)

    traded = [trade(*parts[:5])]
    for s in range(1, last - 1):
        cut = pack_cut([chunks[s]], line[s], tile_map, where, rows_axis, cols_axis, 0)
        traded.append(trade(*cut))
    for k, begin in enumerate((0, middle)):
        cut = pack_cut(
            halves[: k + 1], line[last - 1], tile_map, where, rows_axis, cols_axis, begin
        )
        traded.append(trade(*cut))

    keep, _, xb, _, yb, fa, fb = traded[0]
    lead, rest = row_parts(keep, xb, yb, fa, fb, own)
    far_cols = ring(parts[5], last)
    far_rest = ring(rest, last)
    far_lead = ring(lead, last)
    x3, y3 = swap(far_cols, 2), swap(far_cols, 4)
    fa3 = swap(x3[:, :half], 4)
    fb3 = swap(y3[:, half:], 2)

    def part_blocks(first, height, left, both):
        wide_left = wide if both else own
        begin = 0 if both else left * own
        blocks = []
        for k in (0, 2, 4):
            blocks.append([height, [(first + k, 0, begin, wide_left, 0)], []])
        corner = [(first + 5 + left, 0, 0, own, 0)]
        if both:
            corner.append((first + 6, 0, 0, own, own))
        blocks.append([height, corner, []])
        for n, k, begin, length, to in (
            (0, 0, wide, cols_width, 0),
            (1, 1, own, half, 0),
            (1, 2, wide, half, half),
            (2, 4, wide, half, 0),
            (2, 3, own, half, half),
            (3, 5, own, half, 0),
            (3, 6, own, half, half),
        ):
            blocks[n][2].append((first + k, 0, begin, length, to))
        return blocks

    def seen(count, core, s, rows):
        return [(2 * n + core, s, rows) for n in range(count)]

    whole = (0, block_rows)
    parts_of = ((0, middle), (middle, block_rows))
    early, mid, late = [], [], []
    for s in range(last - 1):
        early += seen(4, 0, s, whole)
    for rows in parts_of:
        for core in (0, 1):
            mid += seen(4, core, last - 1, rows)
    for core in (0, 1):
        late += seen(4, core, last, whole)
    rows, balanced_obs = obs_rows(obs, early + mid + late, plan, where, cols_axis)

    blocks, operands = [], []
    for s in range(last - 1):
        blocks += part_blocks(len(operands), block_rows, 0, True)
        operands += list(traded[s])
    keep, give, keep_rhs, give_rhs = gram_direct(
        blocks, operands, rows, 0, wide, cols_width, (), 2, False
    )
    other = swap(give, 1)
    other_rhs = swap(give_rhs, 1)

    at_row = 4 * (last - 1) * block_rows
    blocks, operands = [], []
    for k in (last - 1, last):
        mine = list(traded[k])
        theirs = [swap(v, 1) for v in mine]
        blocks += part_blocks(len(operands), middle, 0, False)
        blocks += part_blocks(len(operands) + 7, middle, 1, False)
        operands += mine + theirs
    most, most_rhs = gram_direct(
        blocks,
        operands,
        rows,
        at_row,
        own,
        cols_width,
        (keep, other, keep_rhs, other_rhs),
        1,
        False,
    )
    at_row += 8 * block_rows
    mine = [far_cols, x3, y3, fa3, fb3]
    theirs = [swap(v, 1) for v in mine]
    their_rest = swap(far_rest, 1)
    blocks, operands = [], []
    for left, group in ((far_lead, mine), (their_rest, theirs)):
        first = len(operands)
        operands += [left] + group
        for n in range(4):
            cols = [(first + 1 + n, 0, 0, cols_width, 0)]
            if n == 3:
                cols = [(first + 4, 0, 0, half, 0), (first + 5, 0, 0, half, half)]
            blocks.append((block_rows, [(first, n * block_rows, 0, own, 0)], cols))
    gram, rhs = gram_direct(
        blocks, operands, rows, at_row, own, cols_width, (most, most_rhs), 1, True
    )
    return (gram, rhs[0], balanced_obs)


def solution(mesh):
    placed = (
        P(("row", "col"), None),
        P(("row", "col")),
        P(("row", "col")),
        P(("row", "col")),
        P(("row", "col"), None),
        P(("row", "col"), None),
        P(("row", "col"), None),
        P(("row", "col")),
        P(),
    )
    rows_axis, cols_axis = mesh.shape["row"], mesh.shape["col"]
    square = rows_axis == 2**3 and cols_axis > 2

    def body(*args):
        if not square:
            return on_device_any(rows_axis, cols_axis, *args)
        return on_device_square(rows_axis, cols_axis, *args)

    return jax.shard_map(
        body,
        mesh=mesh,
        in_specs=placed,
        out_specs=(P("row", "col"), P("row"), P(("row", "col"), None)),
        check_vma=False,
    )
```

```python
import jax
import jax.numpy as jnp
from jax import lax
from jax.experimental import pallas as pl
from jax.experimental.pallas import tpu as pltpu
from jax.sharding import PartitionSpec as P


F32, BF16 = jnp.float32, jnp.bfloat16
ANY = pl.BlockSpec(memory_space=pl.ANY)
VMEM = pl.BlockSpec(memory_space=pltpu.VMEM)
SMEM = pl.BlockSpec(memory_space=pltpu.SMEM)
HBM = pl.BlockSpec(memory_space=pltpu.HBM)
SPLITS = 1


def factor_math(n, arcs, len_ref, amp_ref, decay_ref, obs_ref, gap_ref, noise_ref):
    lane = lax.broadcasted_iota(jnp.int32, (8, n), 1)
    live = jnp.broadcast_to(gap_ref[...].astype(F32), (8, n))
    noise = jnp.broadcast_to(noise_ref[...], (8, n))
    big_line = lax.broadcasted_iota(jnp.int32, (n, n), 0)
    big_lane = lax.broadcasted_iota(jnp.int32, (n, n), 1)
    arc = jnp.zeros((8, n), jnp.int32)
    first = lane == 0
    arc_line = jnp.zeros((n, n), jnp.int32)
    end = 0
    for k in range(arcs):
        end = end + len_ref[0, k]
        arc = arc + (lane >= end).astype(jnp.int32)
        arc_line = arc_line + (big_line >= end).astype(jnp.int32)
        first = jnp.logical_or(first, lane == end)
    amp = jnp.zeros((8, n), F32)
    decay = jnp.ones((8, n), F32)
    for k in range(arcs):
        amp = jnp.where(arc == k, amp_ref[0, k], amp)
        decay = jnp.where(arc == k, decay_ref[0, k], decay)

    def back(x, shift):
        return pltpu.roll(x, shift, axis=1)

    fresh = (1.0 - decay * decay) * amp
    a = back(decay * decay * noise + fresh * live, 1)
    b = back(fresh * noise, 1)
    c = back(live, 1)
    d = back(noise, 1)
    a = jnp.where(first, 0.0, a)
    b = jnp.where(first, amp, b)
    c = jnp.where(first, 0.0, c)
    d = jnp.where(first, 1.0, d)
    shift = 1
    while shift < n:
        ok = lane >= shift
        pa, pb = jnp.where(ok, back(a, shift), 1.0), jnp.where(ok, back(b, shift), 0.0)
        pc, pd = jnp.where(ok, back(c, shift), 0.0), jnp.where(ok, back(d, shift), 1.0)
        a, b, c, d = a * pa + b * pc, a * pb + b * pd, c * pa + d * pc, c * pb + d * pd
        level = 1.0 / (a + b + c + d)
        a, b, c, d = a * level, b * level, c * level, d * level
        shift *= 2
    variance = b / d
    total = live * variance + noise
    root = 1.0 / jnp.sqrt(total)
    fade = jnp.log(decay * noise / total)
    gain = decay * variance * live / total
    below = big_lane < big_line
    fades = jnp.where(below, jnp.broadcast_to(fade[:1], (n, n)), 0.0)
    mask = below.astype(BF16)
    spans = jnp.zeros((n, n), F32)
    for _ in range(3):
        part = fades.astype(BF16)
        spans = spans + jnp.dot(part, mask, preferred_element_type=F32)
        fades = fades - part.astype(F32)
    diagonal = big_line == big_lane

    def upright(x):
        return jnp.sum(jnp.where(diagonal, jnp.broadcast_to(x[:1], (n, n)), 0.0), axis=1, keepdims=True)

    left = upright(live * root)
    same = jnp.logical_and(below, arc_line == jnp.broadcast_to(arc[:1], (n, n)))
    weight = jnp.where(same, -left * jnp.exp(spans) * jnp.broadcast_to(gain[:1], (n, n)), 0.0)
    weight = jnp.where(diagonal, left, weight)
    white = jnp.sum(weight * jnp.broadcast_to(obs_ref[...], (n, n)), axis=1, keepdims=True)
    white_row = jnp.sum(jnp.where(diagonal, white, 0.0), axis=0, keepdims=True)
    return weight, jnp.broadcast_to(white_row, (8, n))


def factor_kernel(observations, gaps, noise_var, arc_lengths, arc_amp, arc_decay):
    n = observations.shape[0]
    arcs = arc_lengths.shape[1]

    def kernel(len_ref, amp_ref, decay_ref, obs_ref, gap_ref, noise_ref, out_ref):
        out_ref[:n, :], out_ref[n:, :] = factor_math(
            n, arcs, len_ref, amp_ref, decay_ref, obs_ref, gap_ref, noise_ref
        )

    row = (1, n)
    return pl.pallas_call(
        kernel,
        name="factor",
        in_specs=[SMEM] * 3 + [VMEM] * 3,
        out_specs=VMEM,
        out_shape=jax.ShapeDtypeStruct((n + 8, n), F32),
        cost_estimate=pl.CostEstimate(flops=10**8, bytes_accessed=10**5, transcendentals=0),
        compiler_params=pltpu.CompilerParams(vmem_limit_bytes=4 << 20),
    )(
        arc_lengths,
        arc_amp,
        arc_decay,
        observations.reshape(row),
        gaps.reshape(row),
        noise_var.reshape(row),
    )


def split_dot(w, x):
    high = w.astype(BF16)
    low = (w - high.astype(F32)).astype(BF16)
    total = jnp.dot(high, x, preferred_element_type=F32)
    return (total + jnp.dot(low, x, preferred_element_type=F32)).astype(BF16)


def pack(chunk, weight, tile_map, where, rows_axis, cols_axis):
    block_rows, columns = chunk.shape
    tiles = tile_map.shape[0]
    size = columns // tiles
    pairs = rows_axis // 2
    per_row, per_col = tiles // rows_axis, tiles // cols_axis
    wide = (2 * per_row + per_col) * size

    def kernel(map_ref, where_ref, x_ref, *refs):
        outs = refs[-pairs - 1 : -1]
        held = refs[-1]
        row, col = where_ref[0], where_ref[1]

        def fetch(base, count, to):
            for j in range(count):
                at = pl.multiple_of(map_ref[base + j] * size, size)
                held[:, (to + j) * size : (to + j + 1) * size] = x_ref[:, pl.ds(at, size)]

        def finish(start, stop, targets):
            part = held[:, start:stop]
            if weight is not None:
                part = split_dot(refs[0][...], part)
            for target in targets:
                target[:, start:stop] = part

        own = per_row * size
        fetch(col * per_col, per_col, 2 * per_row)
        finish(2 * own, wide, outs)
        for n in range(pairs):
            there = jnp.bitwise_xor(row, 2 * n)
            fetch(there * per_row, per_row, 0)
            fetch(jnp.bitwise_xor(there, 1) * per_row, per_row, per_row)
            finish(0, 2 * own, [outs[n]])

    args = (tile_map, where, chunk) + (() if weight is None else (weight,))
    return pl.pallas_call(
        kernel,
        name="pack",
        in_specs=[SMEM, SMEM] + [VMEM] * (len(args) - 2),
        out_specs=[VMEM] * pairs,
        out_shape=[jax.ShapeDtypeStruct((block_rows, wide), BF16)] * pairs,
        scratch_shapes=[pltpu.VMEM((block_rows, wide), BF16)],
        cost_estimate=pl.CostEstimate(flops=10**9, bytes_accessed=5 * 10**6, transcendentals=0),
        compiler_params=pltpu.CompilerParams(vmem_limit_bytes=24 << 20),
    )(*args)


def gram_first(raw, weights, white, obs, rows_width, cols_width):
    block_rows, wide = raw[0].shape
    count = len(raw) + len(white)
    depth = count * block_rows
    half = rows_width // 2
    step = cols_width // 6 if cols_width % 6 == 0 and (cols_width // 6) % 128 == 0 else 128
    steps = cols_width // step

    def kernel(*refs):
        blocks = refs[:count]
        w_refs = refs[count : count + len(raw)]
        obs_ref = refs[count + len(raw)]
        keep_ref, give_ref, rhs_ref = refs[-7:-4]
        fresh, held, turned, sems = refs[-4:]

        @pl.when(pl.program_id(0) == 0)
        def _():
            copies = []
            for b in range(count):
                to = fresh.at[b] if b < len(raw) else held.at[pl.ds(b * block_rows, block_rows)]
                copies.append(pltpu.make_async_copy(blocks[b], to, sems.at[b]))
                copies[-1].start()
            for b in range(count):
                rows = slice(b * block_rows, (b + 1) * block_rows)
                copies[b].wait()
                if b < len(raw):
                    held[rows, :] = split_dot(w_refs[b][...], fresh[b])
                turned[:, rows] = held[rows, :rows_width].T
            spread = jnp.broadcast_to(obs_ref[...].astype(BF16), (16, depth))
            rhs_ref[...] = jnp.dot(spread, held[:, :rows_width], preferred_element_type=F32)

        at = pl.multiple_of(rows_width + pl.program_id(0) * step, 128)
        right = held[:, pl.ds(at, step)]
        keep_ref[...] = jnp.dot(turned[:half, :], right, preferred_element_type=F32)
        give_ref[...] = jnp.dot(turned[half:, :], right, preferred_element_type=F32)

    tile = pl.BlockSpec((half, step), lambda i: (0, i))
    return pl.pallas_call(
        kernel,
        name="gram_first",
        grid=(steps,),
        in_specs=[ANY] * count + [VMEM] * (len(raw) + 1),
        out_specs=[tile, tile, pl.BlockSpec((16, rows_width), lambda i: (0, 0))],
        out_shape=[jax.ShapeDtypeStruct((half, cols_width), F32)] * 2
        + [jax.ShapeDtypeStruct((16, rows_width), F32)],
        scratch_shapes=[
            pltpu.VMEM((len(raw), block_rows, wide), BF16),
            pltpu.VMEM((depth, wide), BF16),
            pltpu.VMEM((rows_width, depth), BF16),
            pltpu.SemaphoreType.DMA((count,)),
        ],
        cost_estimate=pl.CostEstimate(
            flops=2 * depth * rows_width * cols_width, bytes_accessed=2 * 10**7, transcendentals=0
        ),
        compiler_params=pltpu.CompilerParams(vmem_limit_bytes=48 << 20),
    )(*raw, *white, *weights, obs)


def gram_last(keep, other, mine, theirs, obs, rows_width, cols_width):
    block_rows, wide = mine[0].shape
    count = len(mine) + len(theirs)
    depth = count * block_rows
    half = rows_width // 2
    step = cols_width // 6 if cols_width % 6 == 0 and (cols_width // 6) % 128 == 0 else 128
    steps = cols_width // step

    def kernel(*refs):
        keep_ref, other_ref = refs[:2]
        blocks = refs[2 : 2 + count]
        obs_ref = refs[2 + count]
        out_ref, rhs_ref = refs[-5:-3]
        held, turned, sems = refs[-3:]

        @pl.when(pl.program_id(0) == 0)
        def _():
            copies = []
            for b in range(count):
                to = held.at[pl.ds(b * block_rows, block_rows)]
                copies.append(pltpu.make_async_copy(blocks[b], to, sems.at[b]))
                copies[-1].start()
            total = jnp.zeros((16, half), F32)
            for b in range(count):
                rows = slice(b * block_rows, (b + 1) * block_rows)
                lead = 0 if b < len(mine) else half
                copies[b].wait()
                left = held[rows, lead : lead + half]
                turned[:, rows] = left.T
                spread = jnp.broadcast_to(obs_ref[:, rows].astype(BF16), (16, block_rows))
                total = total + jnp.dot(spread, left, preferred_element_type=F32)
            rhs_ref[...] = total

        at = pl.multiple_of(rows_width + pl.program_id(0) * step, 128)
        right = held[:, pl.ds(at, step)]
        out_ref[...] = (keep_ref[...] + other_ref[...]) + jnp.dot(
            turned[...], right, preferred_element_type=F32
        )

    tile = pl.BlockSpec((half, step), lambda i: (0, i))
    return pl.pallas_call(
        kernel,
        name="gram_last",
        grid=(steps,),
        in_specs=[tile, tile] + [ANY] * count + [VMEM],
        out_specs=[tile, pl.BlockSpec((16, half), lambda i: (0, 0))],
        out_shape=[
            jax.ShapeDtypeStruct((half, cols_width), F32),
            jax.ShapeDtypeStruct((16, half), F32),
        ],
        scratch_shapes=[
            pltpu.VMEM((depth, wide), BF16),
            pltpu.VMEM((half, depth), BF16),
            pltpu.SemaphoreType.DMA((count,)),
        ],
        cost_estimate=pl.CostEstimate(
            flops=2 * depth * half * cols_width, bytes_accessed=2 * 10**7, transcendentals=0
        ),
        compiler_params=pltpu.CompilerParams(vmem_limit_bytes=48 << 20),
    )(keep, other, *mine, *theirs, obs)


def on_device_any(
    rows_axis,
    cols_axis,
    design,
    observations,
    gaps,
    noise_var,
    arc_lengths,
    arc_amp,
    arc_decay,
    plan,
    tile_map,
):
    columns = design.shape[1]
    tiles = tile_map.shape[0]
    size = columns // tiles
    pairs = rows_axis // 2
    rows_width = 2 * (tiles // rows_axis) * size
    cols_width = (tiles // cols_axis) * size
    row, col = lax.axis_index("row"), lax.axis_index("col")
    where = jnp.stack([row, col]).astype(jnp.int32)

    def ring(x, shift):
        return lax.ppermute(x, "col", [(c, (c + shift) % cols_axis) for c in range(cols_axis)])

    def swap(x, mask):
        return lax.ppermute(x, "row", [(r, r ^ mask) for r in range(rows_axis)])

    def spread(parts):
        return [parts[0]] + [swap(parts[n], 2 * n) for n in range(1, pairs)]

    chunks = [design]
    for _ in range(1, cols_axis):
        chunks.append(ring(chunks[-1], 1))

    block_rows = design.shape[0]
    near = factor_kernel(observations, gaps, noise_var, arc_lengths, arc_amp, arc_decay)
    weight = near[:block_rows]
    line = [near] + [ring(near, s) for s in range(1, cols_axis)]
    line_obs = jnp.stack([part[block_rows] for part in line])
    obs_all = jnp.stack([line_obs] + [swap(line_obs, m) for m in range(1, rows_axis)])

    packed = [spread(pack(design, None, tile_map, where, rows_axis, cols_axis))]
    for s in range(1, cols_axis):
        weight_s = line[s][:block_rows]
        packed.append(spread(pack(chunks[s], weight_s, tile_map, where, rows_axis, cols_axis)))

    weights = [weight] + [swap(weight, 2 * n) for n in range(1, pairs)]
    obs_first = obs_all[::2, : cols_axis - 1].swapaxes(0, 1).reshape(1, -1)
    keep, give, rhs_first = gram_first(
        packed[0],
        weights,
        [block for s in range(1, cols_axis - 1) for block in packed[s]],
        obs_first,
        rows_width,
        cols_width,
    )
    half = rows_width // 2
    other = swap(give, 1)
    other_rhs = swap(rhs_first[0, half:], 1)
    theirs = [swap(block, 1) for block in packed[-1]]
    obs_last = jnp.concatenate([obs_all[::2, -1], obs_all[1::2, -1]], axis=0).reshape(1, -1)
    gram, rhs_last = gram_last(
        keep, other, packed[-1], theirs, obs_last, rows_width, cols_width
    )
    normal_rhs = rhs_first[0, :half] + other_rhs + rhs_last[0]
    from_row, from_col = plan // cols_axis, plan % cols_axis
    ahead = (col - from_col + cols_axis) % cols_axis
    place = jnp.bitwise_xor(from_row, row) * cols_axis + ahead
    balanced_obs = jnp.take(obs_all.reshape(-1, block_rows), place, axis=0)
    return (gram, normal_rhs, balanced_obs)


def cut_columns(sizes, fetch, row, outs):
    per_row, per_col, own, half, base = sizes
    across_a, across_b, along_a, along_b, keep = outs
    rows_width = 2 * own

    def rows_of(n, core):
        there = jnp.bitwise_xor(row, 2 * n + core)
        return fetch(there * per_row, per_row)

    part = fetch(base, per_col)
    keep[:, rows_width:] = part
    across_a[:, own:] = part[:, :half]
    along_b[:, rows_width:] = part[:, :half]
    across_b[:, rows_width:] = part[:, half:]
    along_a[:, own:] = part[:, half:]
    across_a[:, :own] = rows_of(3, 0)
    along_a[:, :own] = rows_of(3, 1)
    for n, target in ((1, across_b), (2, along_b), (0, keep)):
        target[:, :own] = rows_of(n, 0)
        target[:, own:rows_width] = rows_of(n, 1)


def cut_widths(own, cols_width):
    half = cols_width // 2
    return [own + half, 2 * own + half, own + half, 2 * own + half, 2 * own + cols_width]


def head(design, small, tables, tile_map, where, rows_axis, cols_axis):
    block_rows, columns = design.shape
    tiles = tile_map.shape[0]
    size = columns // tiles
    per_row, per_col = tiles // rows_axis, tiles // cols_axis
    own, cols_width = per_row * size, per_col * size
    arcs = tables[0].shape[1]

    def kernel(where_ref, *refs):
        sources = refs[:8]
        near_ref = refs[8]
        outs = refs[9:14]
        before_ref = refs[14]
        x_ref, obs_ref, gap_ref, noise_ref, len_ref, amp_ref, decay_ref, map_ref, held, sems = refs[15:]
        targets = (x_ref, obs_ref, gap_ref, noise_ref, len_ref, amp_ref, decay_ref, map_ref)
        copies = [
            pltpu.make_async_copy(source, target, sems.at[k])
            for k, (source, target) in enumerate(zip(sources, targets))
        ]
        for copy in copies[1:] + copies[:1]:
            copy.start()
        for copy in copies[1:]:
            copy.wait()
        weight, white = factor_math(
            block_rows, arcs, len_ref, amp_ref, decay_ref, obs_ref, gap_ref, noise_ref
        )
        near_ref[:block_rows, :] = weight
        near_ref[block_rows:, :] = white
        copies[0].wait()
        row, col = where_ref[0], where_ref[1]

        def fetch(base, count):
            for j in range(count):
                at = pl.multiple_of(map_ref[0, base + j] * size, size)
                held[:, j * size : (j + 1) * size] = x_ref[:, pl.ds(at, size)]
            return split_dot(near_ref[:block_rows, :], held[:, : count * size])

        cut_columns((per_row, per_col, own, cols_width // 2, col * per_col), fetch, row, outs)
        before = jnp.where(col == 0, cols_axis - 1, col - 1)
        before_ref[...] = fetch(before * per_col, per_col)

    line = pltpu.VMEM((1, block_rows), F32)
    outs = [(block_rows + 8, block_rows, F32)]
    outs += [(block_rows, w, BF16) for w in cut_widths(own, cols_width) + [cols_width]]
    return pl.pallas_call(
        kernel,
        name="head",
        in_specs=[SMEM] + [HBM] * 8,
        out_specs=[VMEM] * 7,
        out_shape=[jax.ShapeDtypeStruct((h, w), t) for h, w, t in outs],
        scratch_shapes=[
            pltpu.VMEM((block_rows, columns), BF16),
            line,
            pltpu.VMEM((1, block_rows), jnp.int32),
            line,
            pltpu.SMEM((1, arcs), jnp.int32),
            pltpu.SMEM((1, arcs), F32),
            pltpu.SMEM((1, arcs), F32),
            pltpu.SMEM((1, tiles), jnp.int32),
            pltpu.VMEM((block_rows, max(2 * own, cols_width)), BF16),
            pltpu.SemaphoreType.DMA((8,)),
        ],
        cost_estimate=pl.CostEstimate(flops=10**9, bytes_accessed=5 * 10**6, transcendentals=0),
        compiler_params=pltpu.CompilerParams(vmem_limit_bytes=10 << 20),
    )(where, design, *[v.reshape(1, -1) for v in small], *tables, tile_map.reshape(1, -1))


def pack_cut(chunks, near, tile_map, where, rows_axis, cols_axis, begin):
    height, columns = chunks[-1].shape
    tiles = tile_map.shape[0]
    size = columns // tiles
    per_row, per_col = tiles // rows_axis, tiles // cols_axis
    own, cols_width = per_row * size, per_col * size
    depth = begin + height

    def kernel(map_ref, where_ref, near_ref, *refs):
        raw = refs[: len(chunks)]
        outs = refs[len(chunks) : -1]
        held = refs[-1]
        row, col = where_ref[0], where_ref[1]
        weight = near_ref[begin:depth, :depth]

        def fetch(base, count):
            for j in range(count):
                at = pl.multiple_of(map_ref[base + j] * size, size)
                top = 0
                for piece in raw:
                    end = top + piece.shape[0]
                    held[top:end, j * size : (j + 1) * size] = piece[:, pl.ds(at, size)]
                    top = end
            return split_dot(weight, held[:, : count * size])

        cut_columns((per_row, per_col, own, cols_width // 2, col * per_col), fetch, row, outs)

    return pl.pallas_call(
        kernel,
        name="pack_cut",
        in_specs=[SMEM, SMEM, VMEM] + [VMEM] * len(chunks),
        out_specs=[VMEM] * 5,
        out_shape=[jax.ShapeDtypeStruct((height, w), BF16) for w in cut_widths(own, cols_width)],
        scratch_shapes=[pltpu.VMEM((depth, max(own, cols_width)), BF16)],
        cost_estimate=pl.CostEstimate(flops=10**9, bytes_accessed=5 * 10**6, transcendentals=0),
        compiler_params=pltpu.CompilerParams(vmem_limit_bytes=8 << 20),
    )(tile_map, where, near, *chunks)


def row_parts(keep, xb, yb, fa, fb, own):
    block_rows = keep.shape[0]

    def kernel(keep_ref, xb_ref, yb_ref, fa_ref, fb_ref, lead_ref, rest_ref):
        for n, ref in enumerate((keep_ref, xb_ref, yb_ref)):
            lead_ref[n * block_rows : (n + 1) * block_rows, :] = ref[:, :own]
            rest_ref[n * block_rows : (n + 1) * block_rows, :] = ref[:, own : 2 * own]
        lead_ref[3 * block_rows :, :] = fa_ref[:, :own]
        rest_ref[3 * block_rows :, :] = fb_ref[:, :own]

    return pl.pallas_call(
        kernel,
        name="row_parts",
        in_specs=[VMEM] * 5,
        out_specs=[VMEM] * 2,
        out_shape=[jax.ShapeDtypeStruct((4 * block_rows, own), BF16)] * 2,
        cost_estimate=pl.CostEstimate(flops=10**9, bytes_accessed=5 * 10**6, transcendentals=0),
        compiler_params=pltpu.CompilerParams(vmem_limit_bytes=4 << 20),
    )(keep, xb, yb, fa, fb)


def obs_rows(obs, places, plan, where, cols_axis):
    block_rows = obs[0].shape[1]

    def kernel(plan_ref, where_ref, *refs):
        sources, (rows_ref, picked_ref, held) = refs[:-3], refs[-3:]
        at = 0
        for source in sources:
            held[at : at + source.shape[0], :] = source[...]
            at += source.shape[0]
        at = 0
        for m, s, (begin, end) in places:
            line = m * cols_axis + s
            wide = jnp.broadcast_to(held[line : line + 1, :], (8, block_rows))
            rows_ref[:, at : at + end - begin] = wide[:, begin:end]
            at += end - begin
        from_row = lax.div(plan_ref[0], cols_axis)
        from_col = lax.rem(plan_ref[0], cols_axis)
        mask = jnp.bitwise_xor(from_row, where_ref[0])
        step = lax.rem(where_ref[1] - from_col + cols_axis, cols_axis)
        picked_ref[...] = held[pl.ds(mask * cols_axis + step, 1), :]

    return pl.pallas_call(
        kernel,
        name="obs_rows",
        in_specs=[SMEM, SMEM] + [VMEM] * len(obs),
        out_specs=[VMEM] * 2,
        out_shape=[
            jax.ShapeDtypeStruct((8, sum(end - begin for _, _, (begin, end) in places)), F32),
            jax.ShapeDtypeStruct((1, block_rows), F32),
        ],
        scratch_shapes=[pltpu.VMEM((sum(v.shape[0] for v in obs), block_rows), F32)],
        cost_estimate=pl.CostEstimate(flops=10**7, bytes_accessed=10**5, transcendentals=0),
        compiler_params=pltpu.CompilerParams(vmem_limit_bytes=4 << 20),
    )(plan, where, *obs)


def gram_direct(blocks, operands, rows, at_row, left_width, cols_width, before, halves, out_far):
    count = len(operands)
    width = left_width // halves
    step = cols_width // 6 if cols_width % 6 == 0 and (cols_width // 6) % 128 == 0 else 128
    steps = cols_width // step
    depth = sum(block[0] for block in blocks)

    def kernel(*refs):
        sources = refs[:count]
        rows_ref = refs[count]
        sums = refs[count + 1 : count + 1 + len(before)]
        outs = refs[count + 1 + len(before) : count + 1 + len(before) + 2 * halves]
        scratch = refs[count + 1 + len(before) + 2 * halves :]
        turned = scratch[0]
        total = jnp.zeros((8, left_width), F32)
        top = 0
        for height, lefts, _ in blocks:
            seen = rows_ref[:, at_row + top : at_row + top + height].astype(BF16)
            for which, first, begin, length, to in lefts:
                left = sources[which][first : first + height, begin : begin + length]
                turned[to : to + length, top : top + height] = left.T
            left = jnp.concatenate(
                [
                    sources[which][first : first + height, begin : begin + length]
                    for which, first, begin, length, _ in sorted(lefts, key=lambda p: p[4])
                ],
                axis=1,
            )
            total = total + jnp.dot(seen, left, preferred_element_type=F32)
            top += height
        half_sums = len(before) // 2
        for h in range(halves):
            part = total[:, h * width : (h + 1) * width]
            for extra in sums[half_sums:]:
                part = part + extra[...]
            outs[halves + h][...] = part
        copies = [None, None]
        for t in range(steps):
            begin = t * step
            pieces = []
            for height, _, cols in blocks:
                for which, first, start, length, to in cols:
                    if to <= begin < to + length:
                        at = start + begin - to
                        pieces.append(sources[which][first : first + height, at : at + step])
            right = jnp.concatenate(pieces, axis=0)
            for h in range(halves):
                part = jnp.dot(
                    turned[h * width : (h + 1) * width, :], right, preferred_element_type=F32
                )
                for extra in sums[:half_sums]:
                    part = part + extra[:, begin : begin + step]
                if not out_far:
                    outs[h][:, begin : begin + step] = part
                    continue
                tile, sems = scratch[1:]
                slot = t % 2
                if copies[slot] is not None:
                    copies[slot].wait()
                tile[slot] = part
                copies[slot] = pltpu.make_async_copy(
                    tile.at[slot], outs[0].at[:, pl.ds(begin, step)], sems.at[slot]
                )
                copies[slot].start()
        for copy in copies:
            if copy is not None:
                copy.wait()

    scratch_shapes = [pltpu.VMEM((left_width, depth), BF16)]
    scratch_bytes = 2 * left_width * depth
    if out_far:
        scratch_shapes += [pltpu.VMEM((2, width, step), F32), pltpu.SemaphoreType.DMA((2,))]
        scratch_bytes += 8 * width * step
    return pl.pallas_call(
        kernel,
        in_specs=[VMEM] * (count + 1 + len(before)),
        out_specs=[ANY if out_far else VMEM] * halves + [VMEM] * halves,
        out_shape=[jax.ShapeDtypeStruct((width, cols_width), F32)] * halves
        + [jax.ShapeDtypeStruct((8, width), F32)] * halves,
        scratch_shapes=scratch_shapes,
        cost_estimate=pl.CostEstimate(
            flops=2 * depth * left_width * cols_width, bytes_accessed=2 * 10**7, transcendentals=0
        ),
        compiler_params=pltpu.CompilerParams(vmem_limit_bytes=scratch_bytes + (4 << 20)),
    )(*operands, rows, *before)


def on_device_square(
    rows_axis,
    cols_axis,
    design,
    observations,
    gaps,
    noise_var,
    arc_lengths,
    arc_amp,
    arc_decay,
    plan,
    tile_map,
):
    block_rows, columns = design.shape
    tiles = tile_map.shape[0]
    size = columns // tiles
    own = (tiles // rows_axis) * size
    wide = 2 * own
    cols_width = (tiles // cols_axis) * size
    half = cols_width // 2
    row, col = lax.axis_index("row"), lax.axis_index("col")
    where = jnp.stack([row, col]).astype(jnp.int32)
    last = cols_axis - 1

    def ring(x, shift):
        return lax.ppermute(x, "col", [(c, (c + shift) % cols_axis) for c in range(cols_axis)])

    def swap(x, mask):
        return lax.ppermute(x, "row", [(r, r ^ mask) for r in range(rows_axis)])

    cuts = [(k * block_rows // SPLITS, (k + 1) * block_rows // SPLITS) for k in range(SPLITS)]
    chunks = [design]
    for _ in range(1, last - 1):
        chunks.append(ring(chunks[-1], 1))
    pieces = [ring(chunks[-1][a:b], 1) for a, b in cuts]
    near, *parts = head(
        design,
        (observations, gaps, noise_var),
        (arc_lengths, arc_amp, arc_decay),
        tile_map,
        where,
        rows_axis,
        cols_axis,
    )
    line = [near] + [ring(near, s) for s in range(1, cols_axis)]
    line_obs = jnp.stack([part[block_rows] for part in line])
    obs = [line_obs]
    mask = 1
    while mask < rows_axis:
        obs.append(swap(jnp.concatenate(obs, axis=0), mask))
        mask *= 2

    def trade(xa, xb, ya, yb, keep):
        xa, ya = swap(xa, 2), swap(ya, 4)
        xb, yb = swap(xb, 2), swap(yb, 4)
        return keep, xa, xb, ya, yb, swap(xa, 4), swap(ya, 2)

    traded = [trade(*parts[:5])]
    for s in range(1, last - 1):
        cut = pack_cut([chunks[s]], line[s], tile_map, where, rows_axis, cols_axis, 0)
        traded.append(trade(*cut))
    for k, (begin, _) in enumerate(cuts):
        cut = pack_cut(
            pieces[: k + 1], line[last - 1], tile_map, where, rows_axis, cols_axis, begin
        )
        traded.append(trade(*cut))

    keep, _, xb, _, yb, fa, fb = traded[0]
    lead, rest = row_parts(keep, xb, yb, fa, fb, own)
    far_cols = ring(parts[5], last)
    far_rest = ring(rest, last)
    far_lead = ring(lead, last)
    x3, y3 = swap(far_cols, 2), swap(far_cols, 4)
    fa3 = swap(x3[:, :half], 4)
    fb3 = swap(y3[:, half:], 2)

    def part_blocks(first, height, left, both):
        wide_left = wide if both else own
        begin = 0 if both else left * own
        blocks = []
        for k in (0, 2, 4):
            blocks.append([height, [(first + k, 0, begin, wide_left, 0)], []])
        corner = [(first + 5 + left, 0, 0, own, 0)]
        if both:
            corner.append((first + 6, 0, 0, own, own))
        blocks.append([height, corner, []])
        for n, k, begin, length, to in (
            (0, 0, wide, cols_width, 0),
            (1, 1, own, half, 0),
            (1, 2, wide, half, half),
            (2, 4, wide, half, 0),
            (2, 3, own, half, half),
            (3, 5, own, half, 0),
            (3, 6, own, half, half),
        ):
            blocks[n][2].append((first + k, 0, begin, length, to))
        return blocks

    def seen(count, core, s, rows):
        return [(2 * n + core, s, rows) for n in range(count)]

    whole = (0, block_rows)
    early, mid, late = [], [], []
    for s in range(last - 1):
        early += seen(4, 0, s, whole)
    for rows in cuts:
        for core in (0, 1):
            mid += seen(4, core, last - 1, rows)
    for core in (0, 1):
        late += seen(4, core, last, whole)
    rows, balanced_obs = obs_rows(obs, early + mid + late, plan, where, cols_axis)

    blocks, operands = [], []
    for s in range(last - 1):
        blocks += part_blocks(len(operands), block_rows, 0, True)
        operands += list(traded[s])
    keep, give, keep_rhs, give_rhs = gram_direct(
        blocks, operands, rows, 0, wide, cols_width, (), 2, False
    )
    other = swap(give, 1)
    other_rhs = swap(give_rhs, 1)

    at_row = 4 * (last - 1) * block_rows
    blocks, operands = [], []
    for k in range(last - 1, len(traded)):
        mine = list(traded[k])
        height = block_rows // SPLITS
        theirs = [swap(v, 1) for v in mine]
        blocks += part_blocks(len(operands), height, 0, False)
        blocks += part_blocks(len(operands) + 7, height, 1, False)
        operands += mine + theirs
    most, most_rhs = gram_direct(
        blocks,
        operands,
        rows,
        at_row,
        own,
        cols_width,
        (keep, other, keep_rhs, other_rhs),
        1,
        False,
    )
    at_row += 8 * block_rows
    mine = [far_cols, x3, y3, fa3, fb3]
    theirs = [swap(v, 1) for v in mine]
    their_rest = swap(far_rest, 1)
    blocks, operands = [], []
    for left, group in ((far_lead, mine), (their_rest, theirs)):
        first = len(operands)
        operands += [left] + group
        for n in range(4):
            cols = [(first + 1 + n, 0, 0, cols_width, 0)]
            if n == 3:
                cols = [(first + 4, 0, 0, half, 0), (first + 5, 0, 0, half, half)]
            blocks.append((block_rows, [(first, n * block_rows, 0, own, 0)], cols))
    gram, rhs = gram_direct(
        blocks, operands, rows, at_row, own, cols_width, (most, most_rhs), 1, True
    )
    return (gram, rhs[0], balanced_obs)


def solution(mesh):
    placed = (
        P(("row", "col"), None),
        P(("row", "col")),
        P(("row", "col")),
        P(("row", "col")),
        P(("row", "col"), None),
        P(("row", "col"), None),
        P(("row", "col"), None),
        P(("row", "col")),
        P(),
    )
    rows_axis, cols_axis = mesh.shape["row"], mesh.shape["col"]
    square = rows_axis == 2**3 and cols_axis > 2

    def body(*args):
        if not square:
            return on_device_any(rows_axis, cols_axis, *args)
        return on_device_square(rows_axis, cols_axis, *args)

    return jax.shard_map(
        body,
        mesh=mesh,
        in_specs=placed,
        out_specs=(P("row", "col"), P("row"), P(("row", "col"), None)),
        check_vma=False,
    )
```

```python
import jax
import jax.numpy as jnp
from jax import lax
from jax.experimental import pallas as pl
from jax.experimental.pallas import tpu as pltpu
from jax.sharding import PartitionSpec as P


F32, BF16 = jnp.float32, jnp.bfloat16
ANY = pl.BlockSpec(memory_space=pl.ANY)
VMEM = pl.BlockSpec(memory_space=pltpu.VMEM)
SMEM = pl.BlockSpec(memory_space=pltpu.SMEM)


def factor_math(n, arcs, len_ref, amp_ref, decay_ref, obs_ref, gap_ref, noise_ref):
    lane = lax.broadcasted_iota(jnp.int32, (8, n), 1)
    live = jnp.broadcast_to(gap_ref[...].astype(F32), (8, n))
    noise = jnp.broadcast_to(noise_ref[...], (8, n))
    big_line = lax.broadcasted_iota(jnp.int32, (n, n), 0)
    big_lane = lax.broadcasted_iota(jnp.int32, (n, n), 1)
    arc = jnp.zeros((8, n), jnp.int32)
    first = lane == 0
    arc_line = jnp.zeros((n, n), jnp.int32)
    end = 0
    for k in range(arcs):
        end = end + len_ref[0, k]
        arc = arc + (lane >= end).astype(jnp.int32)
        arc_line = arc_line + (big_line >= end).astype(jnp.int32)
        first = jnp.logical_or(first, lane == end)
    amp = jnp.zeros((8, n), F32)
    decay = jnp.ones((8, n), F32)
    for k in range(arcs):
        amp = jnp.where(arc == k, amp_ref[0, k], amp)
        decay = jnp.where(arc == k, decay_ref[0, k], decay)

    def back(x, shift):
        return pltpu.roll(x, shift, axis=1)

    fresh = (1.0 - decay * decay) * amp
    a = back(decay * decay * noise + fresh * live, 1)
    b = back(fresh * noise, 1)
    c = back(live, 1)
    d = back(noise, 1)
    a = jnp.where(first, 0.0, a)
    b = jnp.where(first, amp, b)
    c = jnp.where(first, 0.0, c)
    d = jnp.where(first, 1.0, d)
    shift = 1
    while shift < n:
        ok = lane >= shift
        pa, pb = jnp.where(ok, back(a, shift), 1.0), jnp.where(ok, back(b, shift), 0.0)
        pc, pd = jnp.where(ok, back(c, shift), 0.0), jnp.where(ok, back(d, shift), 1.0)
        a, b, c, d = a * pa + b * pc, a * pb + b * pd, c * pa + d * pc, c * pb + d * pd
        level = 1.0 / (a + b + c + d)
        a, b, c, d = a * level, b * level, c * level, d * level
        shift *= 2
    variance = b / d
    total = live * variance + noise
    root = 1.0 / jnp.sqrt(total)
    fade = jnp.log(decay * noise / total)
    gain = decay * variance * live / total
    below = big_lane < big_line
    fades = jnp.where(below, jnp.broadcast_to(fade[:1], (n, n)), 0.0)
    mask = below.astype(BF16)
    spans = jnp.zeros((n, n), F32)
    for _ in range(3):
        part = fades.astype(BF16)
        spans = spans + jnp.dot(part, mask, preferred_element_type=F32)
        fades = fades - part.astype(F32)
    diagonal = big_line == big_lane

    def upright(x):
        return jnp.sum(jnp.where(diagonal, jnp.broadcast_to(x[:1], (n, n)), 0.0), axis=1, keepdims=True)

    left = upright(live * root)
    same = jnp.logical_and(below, arc_line == jnp.broadcast_to(arc[:1], (n, n)))
    weight = jnp.where(same, -left * jnp.exp(spans) * jnp.broadcast_to(gain[:1], (n, n)), 0.0)
    weight = jnp.where(diagonal, left, weight)
    white = jnp.sum(weight * jnp.broadcast_to(obs_ref[...], (n, n)), axis=1, keepdims=True)
    white_row = jnp.sum(jnp.where(diagonal, white, 0.0), axis=0, keepdims=True)
    return weight, jnp.broadcast_to(white_row, (8, n))


def factor_kernel(observations, gaps, noise_var, arc_lengths, arc_amp, arc_decay):
    n = observations.shape[0]
    arcs = arc_lengths.shape[1]

    def kernel(len_ref, amp_ref, decay_ref, obs_ref, gap_ref, noise_ref, out_ref):
        out_ref[:n, :], out_ref[n:, :] = factor_math(
            n, arcs, len_ref, amp_ref, decay_ref, obs_ref, gap_ref, noise_ref
        )

    row = (1, n)
    return pl.pallas_call(
        kernel,
        name="factor",
        in_specs=[SMEM] * 3 + [VMEM] * 3,
        out_specs=VMEM,
        out_shape=jax.ShapeDtypeStruct((n + 8, n), F32),
        cost_estimate=pl.CostEstimate(flops=10**8, bytes_accessed=10**5, transcendentals=0),
        compiler_params=pltpu.CompilerParams(vmem_limit_bytes=4 << 20),
    )(
        arc_lengths,
        arc_amp,
        arc_decay,
        observations.reshape(row),
        gaps.reshape(row),
        noise_var.reshape(row),
    )


def split_dot(w, x):
    high = w.astype(BF16)
    low = (w - high.astype(F32)).astype(BF16)
    total = jnp.dot(high, x, preferred_element_type=F32)
    return (total + jnp.dot(low, x, preferred_element_type=F32)).astype(BF16)


def pack(chunk, weight, tile_map, where, rows_axis, cols_axis):
    block_rows, columns = chunk.shape
    tiles = tile_map.shape[0]
    size = columns // tiles
    pairs = rows_axis // 2
    per_row, per_col = tiles // rows_axis, tiles // cols_axis
    wide = (2 * per_row + per_col) * size

    def kernel(map_ref, where_ref, x_ref, *refs):
        outs = refs[-pairs - 1 : -1]
        held = refs[-1]
        row, col = where_ref[0], where_ref[1]

        def fetch(base, count, to):
            for j in range(count):
                at = pl.multiple_of(map_ref[base + j] * size, size)
                held[:, (to + j) * size : (to + j + 1) * size] = x_ref[:, pl.ds(at, size)]

        def finish(start, stop, targets):
            part = held[:, start:stop]
            if weight is not None:
                part = split_dot(refs[0][...], part)
            for target in targets:
                target[:, start:stop] = part

        own = per_row * size
        fetch(col * per_col, per_col, 2 * per_row)
        finish(2 * own, wide, outs)
        for n in range(pairs):
            there = jnp.bitwise_xor(row, 2 * n)
            fetch(there * per_row, per_row, 0)
            fetch(jnp.bitwise_xor(there, 1) * per_row, per_row, per_row)
            finish(0, 2 * own, [outs[n]])

    args = (tile_map, where, chunk) + (() if weight is None else (weight,))
    return pl.pallas_call(
        kernel,
        name="pack",
        in_specs=[SMEM, SMEM] + [VMEM] * (len(args) - 2),
        out_specs=[VMEM] * pairs,
        out_shape=[jax.ShapeDtypeStruct((block_rows, wide), BF16)] * pairs,
        scratch_shapes=[pltpu.VMEM((block_rows, wide), BF16)],
        cost_estimate=pl.CostEstimate(flops=10**9, bytes_accessed=5 * 10**6, transcendentals=0),
        compiler_params=pltpu.CompilerParams(vmem_limit_bytes=24 << 20),
    )(*args)


def gram_first(raw, weights, white, obs, rows_width, cols_width):
    block_rows, wide = raw[0].shape
    count = len(raw) + len(white)
    depth = count * block_rows
    half = rows_width // 2
    step = cols_width // 6 if cols_width % 6 == 0 and (cols_width // 6) % 128 == 0 else 128
    steps = cols_width // step

    def kernel(*refs):
        blocks = refs[:count]
        w_refs = refs[count : count + len(raw)]
        obs_ref = refs[count + len(raw)]
        keep_ref, give_ref, rhs_ref = refs[-7:-4]
        fresh, held, turned, sems = refs[-4:]

        @pl.when(pl.program_id(0) == 0)
        def _():
            copies = []
            for b in range(count):
                to = fresh.at[b] if b < len(raw) else held.at[pl.ds(b * block_rows, block_rows)]
                copies.append(pltpu.make_async_copy(blocks[b], to, sems.at[b]))
                copies[-1].start()
            for b in range(count):
                rows = slice(b * block_rows, (b + 1) * block_rows)
                copies[b].wait()
                if b < len(raw):
                    held[rows, :] = split_dot(w_refs[b][...], fresh[b])
                turned[:, rows] = held[rows, :rows_width].T
            spread = jnp.broadcast_to(obs_ref[...].astype(BF16), (16, depth))
            rhs_ref[...] = jnp.dot(spread, held[:, :rows_width], preferred_element_type=F32)

        at = pl.multiple_of(rows_width + pl.program_id(0) * step, 128)
        right = held[:, pl.ds(at, step)]
        keep_ref[...] = jnp.dot(turned[:half, :], right, preferred_element_type=F32)
        give_ref[...] = jnp.dot(turned[half:, :], right, preferred_element_type=F32)

    tile = pl.BlockSpec((half, step), lambda i: (0, i))
    return pl.pallas_call(
        kernel,
        name="gram_first",
        grid=(steps,),
        in_specs=[ANY] * count + [VMEM] * (len(raw) + 1),
        out_specs=[tile, tile, pl.BlockSpec((16, rows_width), lambda i: (0, 0))],
        out_shape=[jax.ShapeDtypeStruct((half, cols_width), F32)] * 2
        + [jax.ShapeDtypeStruct((16, rows_width), F32)],
        scratch_shapes=[
            pltpu.VMEM((len(raw), block_rows, wide), BF16),
            pltpu.VMEM((depth, wide), BF16),
            pltpu.VMEM((rows_width, depth), BF16),
            pltpu.SemaphoreType.DMA((count,)),
        ],
        cost_estimate=pl.CostEstimate(
            flops=2 * depth * rows_width * cols_width, bytes_accessed=2 * 10**7, transcendentals=0
        ),
        compiler_params=pltpu.CompilerParams(vmem_limit_bytes=48 << 20),
    )(*raw, *white, *weights, obs)


def gram_last(keep, other, mine, theirs, obs, rows_width, cols_width):
    block_rows, wide = mine[0].shape
    count = len(mine) + len(theirs)
    depth = count * block_rows
    half = rows_width // 2
    step = cols_width // 6 if cols_width % 6 == 0 and (cols_width // 6) % 128 == 0 else 128
    steps = cols_width // step

    def kernel(*refs):
        keep_ref, other_ref = refs[:2]
        blocks = refs[2 : 2 + count]
        obs_ref = refs[2 + count]
        out_ref, rhs_ref = refs[-5:-3]
        held, turned, sems = refs[-3:]

        @pl.when(pl.program_id(0) == 0)
        def _():
            copies = []
            for b in range(count):
                to = held.at[pl.ds(b * block_rows, block_rows)]
                copies.append(pltpu.make_async_copy(blocks[b], to, sems.at[b]))
                copies[-1].start()
            total = jnp.zeros((16, half), F32)
            for b in range(count):
                rows = slice(b * block_rows, (b + 1) * block_rows)
                lead = 0 if b < len(mine) else half
                copies[b].wait()
                left = held[rows, lead : lead + half]
                turned[:, rows] = left.T
                spread = jnp.broadcast_to(obs_ref[:, rows].astype(BF16), (16, block_rows))
                total = total + jnp.dot(spread, left, preferred_element_type=F32)
            rhs_ref[...] = total

        at = pl.multiple_of(rows_width + pl.program_id(0) * step, 128)
        right = held[:, pl.ds(at, step)]
        out_ref[...] = (keep_ref[...] + other_ref[...]) + jnp.dot(
            turned[...], right, preferred_element_type=F32
        )

    tile = pl.BlockSpec((half, step), lambda i: (0, i))
    return pl.pallas_call(
        kernel,
        name="gram_last",
        grid=(steps,),
        in_specs=[tile, tile] + [ANY] * count + [VMEM],
        out_specs=[tile, pl.BlockSpec((16, half), lambda i: (0, 0))],
        out_shape=[
            jax.ShapeDtypeStruct((half, cols_width), F32),
            jax.ShapeDtypeStruct((16, half), F32),
        ],
        scratch_shapes=[
            pltpu.VMEM((depth, wide), BF16),
            pltpu.VMEM((half, depth), BF16),
            pltpu.SemaphoreType.DMA((count,)),
        ],
        cost_estimate=pl.CostEstimate(
            flops=2 * depth * half * cols_width, bytes_accessed=2 * 10**7, transcendentals=0
        ),
        compiler_params=pltpu.CompilerParams(vmem_limit_bytes=48 << 20),
    )(keep, other, *mine, *theirs, obs)


def on_device_any(
    rows_axis,
    cols_axis,
    design,
    observations,
    gaps,
    noise_var,
    arc_lengths,
    arc_amp,
    arc_decay,
    plan,
    tile_map,
):
    columns = design.shape[1]
    tiles = tile_map.shape[0]
    size = columns // tiles
    pairs = rows_axis // 2
    rows_width = 2 * (tiles // rows_axis) * size
    cols_width = (tiles // cols_axis) * size
    row, col = lax.axis_index("row"), lax.axis_index("col")
    where = jnp.stack([row, col]).astype(jnp.int32)

    def ring(x, shift):
        return lax.ppermute(x, "col", [(c, (c + shift) % cols_axis) for c in range(cols_axis)])

    def swap(x, mask):
        return lax.ppermute(x, "row", [(r, r ^ mask) for r in range(rows_axis)])

    def spread(parts):
        return [parts[0]] + [swap(parts[n], 2 * n) for n in range(1, pairs)]

    chunks = [design]
    for _ in range(1, cols_axis):
        chunks.append(ring(chunks[-1], 1))

    block_rows = design.shape[0]
    near = factor_kernel(observations, gaps, noise_var, arc_lengths, arc_amp, arc_decay)
    weight = near[:block_rows]
    line = [near] + [ring(near, s) for s in range(1, cols_axis)]
    line_obs = jnp.stack([part[block_rows] for part in line])
    obs_all = jnp.stack([line_obs] + [swap(line_obs, m) for m in range(1, rows_axis)])

    packed = [spread(pack(design, None, tile_map, where, rows_axis, cols_axis))]
    for s in range(1, cols_axis):
        weight_s = line[s][:block_rows]
        packed.append(spread(pack(chunks[s], weight_s, tile_map, where, rows_axis, cols_axis)))

    weights = [weight] + [swap(weight, 2 * n) for n in range(1, pairs)]
    obs_first = obs_all[::2, : cols_axis - 1].swapaxes(0, 1).reshape(1, -1)
    keep, give, rhs_first = gram_first(
        packed[0],
        weights,
        [block for s in range(1, cols_axis - 1) for block in packed[s]],
        obs_first,
        rows_width,
        cols_width,
    )
    half = rows_width // 2
    other = swap(give, 1)
    other_rhs = swap(rhs_first[0, half:], 1)
    theirs = [swap(block, 1) for block in packed[-1]]
    obs_last = jnp.concatenate([obs_all[::2, -1], obs_all[1::2, -1]], axis=0).reshape(1, -1)
    gram, rhs_last = gram_last(
        keep, other, packed[-1], theirs, obs_last, rows_width, cols_width
    )
    normal_rhs = rhs_first[0, :half] + other_rhs + rhs_last[0]
    from_row, from_col = plan // cols_axis, plan % cols_axis
    ahead = (col - from_col + cols_axis) % cols_axis
    place = jnp.bitwise_xor(from_row, row) * cols_axis + ahead
    balanced_obs = jnp.take(obs_all.reshape(-1, block_rows), place, axis=0)
    return (gram, normal_rhs, balanced_obs)


def cut_columns(sizes, fetch, row, outs):
    per_row, per_col, own, half, base = sizes
    across_a, across_b, along_a, along_b, keep = outs
    rows_width = 2 * own

    def rows_of(n, core):
        there = jnp.bitwise_xor(row, 2 * n + core)
        return fetch(there * per_row, per_row)

    part = fetch(base, per_col)
    keep[:, rows_width:] = part
    across_a[:, own:] = part[:, :half]
    along_b[:, rows_width:] = part[:, :half]
    across_b[:, rows_width:] = part[:, half:]
    along_a[:, own:] = part[:, half:]
    across_a[:, :own] = rows_of(3, 0)
    along_a[:, :own] = rows_of(3, 1)
    for n, target in ((1, across_b), (2, along_b), (0, keep)):
        target[:, :own] = rows_of(n, 0)
        target[:, own:rows_width] = rows_of(n, 1)


def cut_widths(own, cols_width):
    half = cols_width // 2
    return [own + half, 2 * own + half, own + half, 2 * own + half, 2 * own + cols_width]


def head(design, small, tables, tile_map, where, rows_axis, cols_axis):
    block_rows, columns = design.shape
    tiles = tile_map.shape[0]
    size = columns // tiles
    per_row, per_col = tiles // rows_axis, tiles // cols_axis
    own, cols_width = per_row * size, per_col * size
    arcs = tables[0].shape[1]

    def kernel(where_ref, *refs):
        sources = refs[:8]
        near_ref = refs[8]
        outs = refs[9:14]
        before_ref = refs[14]
        x_ref, obs_ref, gap_ref, noise_ref, len_ref, amp_ref, decay_ref, map_ref, held, sems = refs[15:]
        targets = (x_ref, obs_ref, gap_ref, noise_ref, len_ref, amp_ref, decay_ref, map_ref)
        copies = [
            pltpu.make_async_copy(source, target, sems.at[k])
            for k, (source, target) in enumerate(zip(sources, targets))
        ]
        for copy in copies[1:] + copies[:1]:
            copy.start()
        for copy in copies[1:]:
            copy.wait()
        weight, white = factor_math(
            block_rows, arcs, len_ref, amp_ref, decay_ref, obs_ref, gap_ref, noise_ref
        )
        near_ref[:block_rows, :] = weight
        near_ref[block_rows:, :] = white
        copies[0].wait()
        row, col = where_ref[0], where_ref[1]

        def fetch(base, count):
            for j in range(count):
                at = pl.multiple_of(map_ref[0, base + j] * size, size)
                held[:, j * size : (j + 1) * size] = x_ref[:, pl.ds(at, size)]
            return split_dot(near_ref[:block_rows, :], held[:, : count * size])

        cut_columns((per_row, per_col, own, cols_width // 2, col * per_col), fetch, row, outs)
        before = jnp.where(col == 0, cols_axis - 1, col - 1)
        before_ref[...] = fetch(before * per_col, per_col)

    line = pltpu.VMEM((1, block_rows), F32)
    outs = [(block_rows + 8, block_rows, F32)]
    outs += [(block_rows, w, BF16) for w in cut_widths(own, cols_width) + [cols_width]]
    return pl.pallas_call(
        kernel,
        name="head",
        in_specs=[SMEM] + [ANY] * 8,
        out_specs=[VMEM] * 7,
        out_shape=[jax.ShapeDtypeStruct((h, w), t) for h, w, t in outs],
        scratch_shapes=[
            pltpu.VMEM((block_rows, columns), BF16),
            line,
            pltpu.VMEM((1, block_rows), jnp.int32),
            line,
            pltpu.SMEM((1, arcs), jnp.int32),
            pltpu.SMEM((1, arcs), F32),
            pltpu.SMEM((1, arcs), F32),
            pltpu.SMEM((1, tiles), jnp.int32),
            pltpu.VMEM((block_rows, max(2 * own, cols_width)), BF16),
            pltpu.SemaphoreType.DMA((8,)),
        ],
        cost_estimate=pl.CostEstimate(flops=10**9, bytes_accessed=5 * 10**6, transcendentals=0),
        compiler_params=pltpu.CompilerParams(vmem_limit_bytes=10 << 20),
    )(where, design, *[v.reshape(1, -1) for v in small], *tables, tile_map.reshape(1, -1))


def pack_cut(chunk, near, tile_map, where, rows_axis, cols_axis):
    block_rows, columns = chunk.shape
    tiles = tile_map.shape[0]
    size = columns // tiles
    per_row, per_col = tiles // rows_axis, tiles // cols_axis
    own, cols_width = per_row * size, per_col * size

    def kernel(map_ref, where_ref, near_ref, x_ref, *refs):
        outs, held = refs[:-1], refs[-1]
        row, col = where_ref[0], where_ref[1]
        weight = near_ref[:block_rows, :]

        def fetch(base, count):
            for j in range(count):
                at = pl.multiple_of(map_ref[base + j] * size, size)
                held[:, j * size : (j + 1) * size] = x_ref[:, pl.ds(at, size)]
            return split_dot(weight, held[:, : count * size])

        cut_columns((per_row, per_col, own, cols_width // 2, col * per_col), fetch, row, outs)

    return pl.pallas_call(
        kernel,
        name="pack_cut",
        in_specs=[SMEM, SMEM, VMEM, VMEM],
        out_specs=[VMEM] * 5,
        out_shape=[
            jax.ShapeDtypeStruct((block_rows, w), BF16) for w in cut_widths(own, cols_width)
        ],
        scratch_shapes=[pltpu.VMEM((block_rows, max(own, cols_width)), BF16)],
        cost_estimate=pl.CostEstimate(flops=10**9, bytes_accessed=5 * 10**6, transcendentals=0),
        compiler_params=pltpu.CompilerParams(vmem_limit_bytes=8 << 20),
    )(tile_map, where, near, chunk)


def row_parts(keep, xb, yb, fa, fb, own):
    block_rows = keep.shape[0]

    def kernel(keep_ref, xb_ref, yb_ref, fa_ref, fb_ref, lead_ref, rest_ref):
        for n, ref in enumerate((keep_ref, xb_ref, yb_ref)):
            lead_ref[:, n * block_rows : (n + 1) * block_rows] = ref[:, :own].T
            rest_ref[:, n * block_rows : (n + 1) * block_rows] = ref[:, own : 2 * own].T
        lead_ref[:, 3 * block_rows :] = fa_ref[:, :own].T
        rest_ref[:, 3 * block_rows :] = fb_ref[:, :own].T

    return pl.pallas_call(
        kernel,
        name="row_parts",
        in_specs=[VMEM] * 5,
        out_specs=[VMEM] * 2,
        out_shape=[jax.ShapeDtypeStruct((own, 4 * block_rows), BF16)] * 2,
        cost_estimate=pl.CostEstimate(flops=10**9, bytes_accessed=5 * 10**6, transcendentals=0),
        compiler_params=pltpu.CompilerParams(vmem_limit_bytes=4 << 20),
    )(keep, xb, yb, fa, fb)


def obs_rows(obs, places, plan, where, cols_axis):
    block_rows = obs[0].shape[1]

    def kernel(plan_ref, where_ref, *refs):
        sources, (rows_ref, picked_ref, held) = refs[:-3], refs[-3:]
        at = 0
        for source in sources:
            held[at : at + source.shape[0], :] = source[...]
            at += source.shape[0]
        at = 0
        for m, s in places:
            line = m * cols_axis + s
            rows_ref[:, at : at + block_rows] = jnp.broadcast_to(
                held[line : line + 1, :], (8, block_rows)
            )
            at += block_rows
        from_row = lax.div(plan_ref[0], cols_axis)
        from_col = lax.rem(plan_ref[0], cols_axis)
        mask = jnp.bitwise_xor(from_row, where_ref[0])
        step = lax.rem(where_ref[1] - from_col + cols_axis, cols_axis)
        picked_ref[...] = held[pl.ds(mask * cols_axis + step, 1), :]

    return pl.pallas_call(
        kernel,
        name="obs_rows",
        in_specs=[SMEM, SMEM] + [VMEM] * len(obs),
        out_specs=[VMEM] * 2,
        out_shape=[
            jax.ShapeDtypeStruct((8, len(places) * block_rows), F32),
            jax.ShapeDtypeStruct((1, block_rows), F32),
        ],
        scratch_shapes=[pltpu.VMEM((sum(v.shape[0] for v in obs), block_rows), F32)],
        cost_estimate=pl.CostEstimate(flops=10**7, bytes_accessed=10**5, transcendentals=0),
        compiler_params=pltpu.CompilerParams(vmem_limit_bytes=4 << 20),
    )(plan, where, *obs)


def gram_direct(
    blocks, ready, operands, rows, at_row, left_width, cols_width, before, halves, out_far
):
    count = len(operands)
    width = left_width // halves
    step = cols_width // 6 if cols_width % 6 == 0 and (cols_width // 6) % 128 == 0 else 128
    steps = cols_width // step
    depth = sum(block[0] for block in blocks)
    total_depth = depth + sum(part[0] for _, group in ready for part in group)

    def kernel(*refs):
        sources = refs[:count]
        rows_ref = refs[count]
        sums = refs[count + 1 : count + 1 + len(before)]
        outs = refs[count + 1 + len(before) : count + 1 + len(before) + 2 * halves]
        scratch = refs[count + 1 + len(before) + 2 * halves :]
        turned = scratch[0]
        total = jnp.zeros((8, left_width), F32)
        top = 0
        for height, lefts, _ in blocks:
            seen = rows_ref[:, at_row + top : at_row + top + height].astype(BF16)
            for which, first, begin, length, to in lefts:
                left = sources[which][first : first + height, begin : begin + length]
                turned[to : to + length, top : top + height] = left.T
            left = jnp.concatenate(
                [
                    sources[which][first : first + height, begin : begin + length]
                    for which, first, begin, length, _ in sorted(lefts, key=lambda p: p[4])
                ],
                axis=1,
            )
            total = total + jnp.dot(seen, left, preferred_element_type=F32)
            top += height
        for which, group in ready:
            height = sum(part[0] for part in group)
            seen = rows_ref[:, at_row + top : at_row + top + height].astype(BF16)
            total = total + lax.dot_general(
                seen, sources[which][...], (((1,), (1,)), ((), ())), preferred_element_type=F32
            )
            top += height
        half_sums = len(before) // 2
        for h in range(halves):
            part = total[:, h * width : (h + 1) * width]
            for extra in sums[half_sums:]:
                part = part + extra[...]
            outs[halves + h][...] = part
        copies = [None, None]
        for t in range(steps):
            begin = t * step

            def cut(group):
                pieces = []
                for height, cols in group:
                    for which, first, start, length, to in cols:
                        if to <= begin < to + length:
                            at = start + begin - to
                            pieces.append(sources[which][first : first + height, at : at + step])
                return jnp.concatenate(pieces, axis=0)

            right = cut([(height, cols) for height, _, cols in blocks])
            rights = [(which, cut(group)) for which, group in ready]
            for h in range(halves):
                part = jnp.dot(
                    turned[h * width : (h + 1) * width, :], right, preferred_element_type=F32
                )
                for which, other in rights:
                    part = part + jnp.dot(
                        sources[which][...], other, preferred_element_type=F32
                    )
                for extra in sums[:half_sums]:
                    part = part + extra[:, begin : begin + step]
                if not out_far:
                    outs[h][:, begin : begin + step] = part
                    continue
                tile, sems = scratch[1:]
                slot = t % 2
                if copies[slot] is not None:
                    copies[slot].wait()
                tile[slot] = part
                copies[slot] = pltpu.make_async_copy(
                    tile.at[slot], outs[0].at[:, pl.ds(begin, step)], sems.at[slot]
                )
                copies[slot].start()
        for copy in copies:
            if copy is not None:
                copy.wait()

    scratch_shapes = [pltpu.VMEM((left_width, depth), BF16)]
    scratch_bytes = 2 * left_width * depth
    if out_far:
        scratch_shapes += [pltpu.VMEM((2, width, step), F32), pltpu.SemaphoreType.DMA((2,))]
        scratch_bytes += 8 * width * step
    return pl.pallas_call(
        kernel,
        in_specs=[VMEM] * (count + 1 + len(before)),
        out_specs=[ANY if out_far else VMEM] * halves + [VMEM] * halves,
        out_shape=[jax.ShapeDtypeStruct((width, cols_width), F32)] * halves
        + [jax.ShapeDtypeStruct((8, width), F32)] * halves,
        scratch_shapes=scratch_shapes,
        cost_estimate=pl.CostEstimate(
            flops=2 * total_depth * left_width * cols_width,
            bytes_accessed=2 * 10**7,
            transcendentals=0,
        ),
        compiler_params=pltpu.CompilerParams(vmem_limit_bytes=scratch_bytes + (4 << 20)),
    )(*operands, rows, *before)


def on_device_square(
    rows_axis,
    cols_axis,
    design,
    observations,
    gaps,
    noise_var,
    arc_lengths,
    arc_amp,
    arc_decay,
    plan,
    tile_map,
):
    block_rows, columns = design.shape
    tiles = tile_map.shape[0]
    size = columns // tiles
    own = (tiles // rows_axis) * size
    wide = 2 * own
    cols_width = (tiles // cols_axis) * size
    half = cols_width // 2
    row, col = lax.axis_index("row"), lax.axis_index("col")
    where = jnp.stack([row, col]).astype(jnp.int32)
    last = cols_axis - 1

    def ring(x, shift):
        return lax.ppermute(x, "col", [(c, (c + shift) % cols_axis) for c in range(cols_axis)])

    def swap(x, mask):
        return lax.ppermute(x, "row", [(r, r ^ mask) for r in range(rows_axis)])

    chunks = [design]
    for _ in range(1, last):
        chunks.append(ring(chunks[-1], 1))
    near, *parts = head(
        design,
        (observations, gaps, noise_var),
        (arc_lengths, arc_amp, arc_decay),
        tile_map,
        where,
        rows_axis,
        cols_axis,
    )
    line = [near] + [ring(near, s) for s in range(1, cols_axis)]
    line_obs = jnp.stack([part[block_rows] for part in line])
    obs = [line_obs] + [swap(line_obs, m) for m in range(1, rows_axis)]

    def trade(xa, xb, ya, yb, keep):
        xa, ya = swap(xa, 2), swap(ya, 4)
        xb, yb = swap(xb, 2), swap(yb, 4)
        return keep, xa, xb, ya, yb, swap(xa, 4), swap(ya, 2)

    traded = [trade(*parts[:5])]
    for s in range(1, last):
        cut = pack_cut(chunks[s], line[s], tile_map, where, rows_axis, cols_axis)
        traded.append(trade(*cut))

    keep, _, xb, _, yb, fa, fb = traded[0]
    lead, rest = row_parts(keep, xb, yb, fa, fb, own)
    far_cols = ring(parts[5], last)
    far_rest = ring(rest, last)
    far_lead = ring(lead, last)
    x3, y3 = swap(far_cols, 2), swap(far_cols, 4)
    fa3 = swap(x3[:, :half], 4)
    fb3 = swap(y3[:, half:], 2)

    def part_blocks(first, height, left, both):
        wide_left = wide if both else own
        begin = 0 if both else left * own
        blocks = []
        for k in (0, 2, 4):
            blocks.append([height, [(first + k, 0, begin, wide_left, 0)], []])
        corner = [(first + 5 + left, 0, 0, own, 0)]
        if both:
            corner.append((first + 6, 0, 0, own, own))
        blocks.append([height, corner, []])
        for n, k, begin, length, to in (
            (0, 0, wide, cols_width, 0),
            (1, 1, own, half, 0),
            (1, 2, wide, half, half),
            (2, 4, wide, half, 0),
            (2, 3, own, half, half),
            (3, 5, own, half, 0),
            (3, 6, own, half, half),
        ):
            blocks[n][2].append((first + k, 0, begin, length, to))
        return blocks

    early = [(2 * n, s) for s in range(last - 1) for n in range(4)]
    mid = [(2 * n + core, last - 1) for core in (0, 1) for n in range(3)]
    late = [(6 + core, last - 1) for core in (0, 1)]
    late += [(2 * n + core, last) for core in (0, 1) for n in range(4)]
    rows, balanced_obs = obs_rows(obs, early + mid + late, plan, where, cols_axis)

    blocks, operands = [], []
    for s in range(last - 1):
        blocks += part_blocks(len(operands), block_rows, 0, True)
        operands += list(traded[s])
    keep, give, keep_rhs, give_rhs = gram_direct(
        blocks, [], operands, rows, 0, wide, cols_width, (), 2, False
    )
    other = swap(give, 1)
    other_rhs = swap(give_rhs, 1)

    mine = list(traded[last - 1])
    theirs = [swap(v, 1) for v in mine]
    sides = [part_blocks(0, block_rows, 0, False), part_blocks(5, block_rows, 1, False)]
    at_row = len(early) * block_rows
    most, most_rhs = gram_direct(
        sides[0][:3] + sides[1][:3],
        [],
        mine[:5] + theirs[:5],
        rows,
        at_row,
        own,
        cols_width,
        (keep, other, keep_rhs, other_rhs),
        1,
        False,
    )
    at_row += len(mid) * block_rows
    mine_far = [far_cols, x3, y3, fa3, fb3]
    theirs_far = [swap(v, 1) for v in mine_far]
    their_rest = swap(far_rest, 1)
    corners, ready = [], []
    operands = []
    for core, group in enumerate((mine, theirs)):
        cols = [(len(operands), 0, own, half, 0), (len(operands) + 1, 0, own, half, half)]
        corners.append((block_rows, [(len(operands) + core, 0, 0, own, 0)], cols))
        operands += group[5:]
    for left, group in ((far_lead, mine_far), (their_rest, theirs_far)):
        first = len(operands)
        operands += [left] + group
        plain = [(block_rows, [(first + 1 + n, 0, 0, cols_width, 0)]) for n in range(3)]
        plain.append((block_rows, [(first + 4, 0, 0, half, 0), (first + 5, 0, 0, half, half)]))
        ready.append((first, plain))
    gram, rhs = gram_direct(
        corners, ready, operands, rows, at_row, own, cols_width, (most, most_rhs), 1, True
    )
    return (gram, rhs[0], balanced_obs)


def solution(mesh):
    placed = (
        P(("row", "col"), None),
        P(("row", "col")),
        P(("row", "col")),
        P(("row", "col")),
        P(("row", "col"), None),
        P(("row", "col"), None),
        P(("row", "col"), None),
        P(("row", "col")),
        P(),
    )
    rows_axis, cols_axis = mesh.shape["row"], mesh.shape["col"]
    square = rows_axis == 2**3 and cols_axis > 2

    def body(*args):
        if not square:
            return on_device_any(rows_axis, cols_axis, *args)
        return on_device_square(rows_axis, cols_axis, *args)

    return jax.shard_map(
        body,
        mesh=mesh,
        in_specs=placed,
        out_specs=(P("row", "col"), P("row"), P(("row", "col"), None)),
        check_vma=False,
    )
```

```python
import jax
import jax.numpy as jnp
from jax import lax
from jax.experimental import pallas as pl
from jax.experimental.pallas import tpu as pltpu
from jax.sharding import PartitionSpec as P


F32, BF16 = jnp.float32, jnp.bfloat16
ANY = pl.BlockSpec(memory_space=pl.ANY)
VMEM = pl.BlockSpec(memory_space=pltpu.VMEM)
SMEM = pl.BlockSpec(memory_space=pltpu.SMEM)


def factor_math(n, arcs, len_ref, amp_ref, decay_ref, obs_ref, gap_ref, noise_ref):
    lane = lax.broadcasted_iota(jnp.int32, (8, n), 1)
    live = jnp.broadcast_to(gap_ref[...].astype(F32), (8, n))
    noise = jnp.broadcast_to(noise_ref[...], (8, n))
    big_line = lax.broadcasted_iota(jnp.int32, (n, n), 0)
    big_lane = lax.broadcasted_iota(jnp.int32, (n, n), 1)
    arc = jnp.zeros((8, n), jnp.int32)
    first = lane == 0
    arc_line = jnp.zeros((n, n), jnp.int32)
    end = 0
    for k in range(arcs):
        end = end + len_ref[0, k]
        arc = arc + (lane >= end).astype(jnp.int32)
        arc_line = arc_line + (big_line >= end).astype(jnp.int32)
        first = jnp.logical_or(first, lane == end)
    amp = jnp.zeros((8, n), F32)
    decay = jnp.ones((8, n), F32)
    for k in range(arcs):
        amp = jnp.where(arc == k, amp_ref[0, k], amp)
        decay = jnp.where(arc == k, decay_ref[0, k], decay)

    def back(x, shift):
        return pltpu.roll(x, shift, axis=1)

    fresh = (1.0 - decay * decay) * amp
    a = back(decay * decay * noise + fresh * live, 1)
    b = back(fresh * noise, 1)
    c = back(live, 1)
    d = back(noise, 1)
    a = jnp.where(first, 0.0, a)
    b = jnp.where(first, amp, b)
    c = jnp.where(first, 0.0, c)
    d = jnp.where(first, 1.0, d)
    shift = 1
    while shift < n:
        ok = lane >= shift
        pa, pb = jnp.where(ok, back(a, shift), 1.0), jnp.where(ok, back(b, shift), 0.0)
        pc, pd = jnp.where(ok, back(c, shift), 0.0), jnp.where(ok, back(d, shift), 1.0)
        a, b, c, d = a * pa + b * pc, a * pb + b * pd, c * pa + d * pc, c * pb + d * pd
        level = 1.0 / (a + b + c + d)
        a, b, c, d = a * level, b * level, c * level, d * level
        shift *= 2
    variance = b / d
    total = live * variance + noise
    root = 1.0 / jnp.sqrt(total)
    fade = jnp.log(decay * noise / total)
    gain = decay * variance * live / total
    below = big_lane < big_line
    fades = jnp.where(below, jnp.broadcast_to(fade[:1], (n, n)), 0.0)
    mask = below.astype(BF16)
    spans = jnp.zeros((n, n), F32)
    for _ in range(3):
        part = fades.astype(BF16)
        spans = spans + jnp.dot(part, mask, preferred_element_type=F32)
        fades = fades - part.astype(F32)
    diagonal = big_line == big_lane

    def upright(x):
        return jnp.sum(jnp.where(diagonal, jnp.broadcast_to(x[:1], (n, n)), 0.0), axis=1, keepdims=True)

    left = upright(live * root)
    same = jnp.logical_and(below, arc_line == jnp.broadcast_to(arc[:1], (n, n)))
    weight = jnp.where(same, -left * jnp.exp(spans) * jnp.broadcast_to(gain[:1], (n, n)), 0.0)
    weight = jnp.where(diagonal, left, weight)
    white = jnp.sum(weight * jnp.broadcast_to(obs_ref[...], (n, n)), axis=1, keepdims=True)
    white_row = jnp.sum(jnp.where(diagonal, white, 0.0), axis=0, keepdims=True)
    return weight, jnp.broadcast_to(white_row, (8, n))


def factor_kernel(observations, gaps, noise_var, arc_lengths, arc_amp, arc_decay):
    n = observations.shape[0]
    arcs = arc_lengths.shape[1]

    def kernel(len_ref, amp_ref, decay_ref, obs_ref, gap_ref, noise_ref, out_ref):
        out_ref[:n, :], out_ref[n:, :] = factor_math(
            n, arcs, len_ref, amp_ref, decay_ref, obs_ref, gap_ref, noise_ref
        )

    row = (1, n)
    return pl.pallas_call(
        kernel,
        name="factor",
        in_specs=[SMEM] * 3 + [VMEM] * 3,
        out_specs=VMEM,
        out_shape=jax.ShapeDtypeStruct((n + 8, n), F32),
        cost_estimate=pl.CostEstimate(flops=10**8, bytes_accessed=10**5, transcendentals=0),
        compiler_params=pltpu.CompilerParams(vmem_limit_bytes=4 << 20),
    )(
        arc_lengths,
        arc_amp,
        arc_decay,
        observations.reshape(row),
        gaps.reshape(row),
        noise_var.reshape(row),
    )


def split_dot(w, x):
    high = w.astype(BF16)
    low = (w - high.astype(F32)).astype(BF16)
    total = jnp.dot(high, x, preferred_element_type=F32)
    return (total + jnp.dot(low, x, preferred_element_type=F32)).astype(BF16)


def pack(chunk, weight, tile_map, where, rows_axis, cols_axis):
    block_rows, columns = chunk.shape
    tiles = tile_map.shape[0]
    size = columns // tiles
    pairs = rows_axis // 2
    per_row, per_col = tiles // rows_axis, tiles // cols_axis
    wide = (2 * per_row + per_col) * size

    def kernel(map_ref, where_ref, x_ref, *refs):
        outs = refs[-pairs - 1 : -1]
        held = refs[-1]
        row, col = where_ref[0], where_ref[1]

        def fetch(base, count, to):
            for j in range(count):
                at = pl.multiple_of(map_ref[base + j] * size, size)
                held[:, (to + j) * size : (to + j + 1) * size] = x_ref[:, pl.ds(at, size)]

        def finish(start, stop, targets):
            part = held[:, start:stop]
            if weight is not None:
                part = split_dot(refs[0][...], part)
            for target in targets:
                target[:, start:stop] = part

        own = per_row * size
        fetch(col * per_col, per_col, 2 * per_row)
        finish(2 * own, wide, outs)
        for n in range(pairs):
            there = jnp.bitwise_xor(row, 2 * n)
            fetch(there * per_row, per_row, 0)
            fetch(jnp.bitwise_xor(there, 1) * per_row, per_row, per_row)
            finish(0, 2 * own, [outs[n]])

    args = (tile_map, where, chunk) + (() if weight is None else (weight,))
    return pl.pallas_call(
        kernel,
        name="pack",
        in_specs=[SMEM, SMEM] + [VMEM] * (len(args) - 2),
        out_specs=[VMEM] * pairs,
        out_shape=[jax.ShapeDtypeStruct((block_rows, wide), BF16)] * pairs,
        scratch_shapes=[pltpu.VMEM((block_rows, wide), BF16)],
        cost_estimate=pl.CostEstimate(flops=10**9, bytes_accessed=5 * 10**6, transcendentals=0),
        compiler_params=pltpu.CompilerParams(vmem_limit_bytes=24 << 20),
    )(*args)


def gram_first(raw, weights, white, obs, rows_width, cols_width):
    block_rows, wide = raw[0].shape
    count = len(raw) + len(white)
    depth = count * block_rows
    half = rows_width // 2
    step = cols_width // 6 if cols_width % 6 == 0 and (cols_width // 6) % 128 == 0 else 128
    steps = cols_width // step

    def kernel(*refs):
        blocks = refs[:count]
        w_refs = refs[count : count + len(raw)]
        obs_ref = refs[count + len(raw)]
        keep_ref, give_ref, rhs_ref = refs[-7:-4]
        fresh, held, turned, sems = refs[-4:]

        @pl.when(pl.program_id(0) == 0)
        def _():
            copies = []
            for b in range(count):
                to = fresh.at[b] if b < len(raw) else held.at[pl.ds(b * block_rows, block_rows)]
                copies.append(pltpu.make_async_copy(blocks[b], to, sems.at[b]))
                copies[-1].start()
            for b in range(count):
                rows = slice(b * block_rows, (b + 1) * block_rows)
                copies[b].wait()
                if b < len(raw):
                    held[rows, :] = split_dot(w_refs[b][...], fresh[b])
                turned[:, rows] = held[rows, :rows_width].T
            spread = jnp.broadcast_to(obs_ref[...].astype(BF16), (16, depth))
            rhs_ref[...] = jnp.dot(spread, held[:, :rows_width], preferred_element_type=F32)

        at = pl.multiple_of(rows_width + pl.program_id(0) * step, 128)
        right = held[:, pl.ds(at, step)]
        keep_ref[...] = jnp.dot(turned[:half, :], right, preferred_element_type=F32)
        give_ref[...] = jnp.dot(turned[half:, :], right, preferred_element_type=F32)

    tile = pl.BlockSpec((half, step), lambda i: (0, i))
    return pl.pallas_call(
        kernel,
        name="gram_first",
        grid=(steps,),
        in_specs=[ANY] * count + [VMEM] * (len(raw) + 1),
        out_specs=[tile, tile, pl.BlockSpec((16, rows_width), lambda i: (0, 0))],
        out_shape=[jax.ShapeDtypeStruct((half, cols_width), F32)] * 2
        + [jax.ShapeDtypeStruct((16, rows_width), F32)],
        scratch_shapes=[
            pltpu.VMEM((len(raw), block_rows, wide), BF16),
            pltpu.VMEM((depth, wide), BF16),
            pltpu.VMEM((rows_width, depth), BF16),
            pltpu.SemaphoreType.DMA((count,)),
        ],
        cost_estimate=pl.CostEstimate(
            flops=2 * depth * rows_width * cols_width, bytes_accessed=2 * 10**7, transcendentals=0
        ),
        compiler_params=pltpu.CompilerParams(vmem_limit_bytes=48 << 20),
    )(*raw, *white, *weights, obs)


def gram_last(keep, other, mine, theirs, obs, rows_width, cols_width):
    block_rows, wide = mine[0].shape
    count = len(mine) + len(theirs)
    depth = count * block_rows
    half = rows_width // 2
    step = cols_width // 6 if cols_width % 6 == 0 and (cols_width // 6) % 128 == 0 else 128
    steps = cols_width // step

    def kernel(*refs):
        keep_ref, other_ref = refs[:2]
        blocks = refs[2 : 2 + count]
        obs_ref = refs[2 + count]
        out_ref, rhs_ref = refs[-5:-3]
        held, turned, sems = refs[-3:]

        @pl.when(pl.program_id(0) == 0)
        def _():
            copies = []
            for b in range(count):
                to = held.at[pl.ds(b * block_rows, block_rows)]
                copies.append(pltpu.make_async_copy(blocks[b], to, sems.at[b]))
                copies[-1].start()
            total = jnp.zeros((16, half), F32)
            for b in range(count):
                rows = slice(b * block_rows, (b + 1) * block_rows)
                lead = 0 if b < len(mine) else half
                copies[b].wait()
                left = held[rows, lead : lead + half]
                turned[:, rows] = left.T
                spread = jnp.broadcast_to(obs_ref[:, rows].astype(BF16), (16, block_rows))
                total = total + jnp.dot(spread, left, preferred_element_type=F32)
            rhs_ref[...] = total

        at = pl.multiple_of(rows_width + pl.program_id(0) * step, 128)
        right = held[:, pl.ds(at, step)]
        out_ref[...] = (keep_ref[...] + other_ref[...]) + jnp.dot(
            turned[...], right, preferred_element_type=F32
        )

    tile = pl.BlockSpec((half, step), lambda i: (0, i))
    return pl.pallas_call(
        kernel,
        name="gram_last",
        grid=(steps,),
        in_specs=[tile, tile] + [ANY] * count + [VMEM],
        out_specs=[tile, pl.BlockSpec((16, half), lambda i: (0, 0))],
        out_shape=[
            jax.ShapeDtypeStruct((half, cols_width), F32),
            jax.ShapeDtypeStruct((16, half), F32),
        ],
        scratch_shapes=[
            pltpu.VMEM((depth, wide), BF16),
            pltpu.VMEM((half, depth), BF16),
            pltpu.SemaphoreType.DMA((count,)),
        ],
        cost_estimate=pl.CostEstimate(
            flops=2 * depth * half * cols_width, bytes_accessed=2 * 10**7, transcendentals=0
        ),
        compiler_params=pltpu.CompilerParams(vmem_limit_bytes=48 << 20),
    )(keep, other, *mine, *theirs, obs)


def on_device_any(
    rows_axis,
    cols_axis,
    design,
    observations,
    gaps,
    noise_var,
    arc_lengths,
    arc_amp,
    arc_decay,
    plan,
    tile_map,
):
    columns = design.shape[1]
    tiles = tile_map.shape[0]
    size = columns // tiles
    pairs = rows_axis // 2
    rows_width = 2 * (tiles // rows_axis) * size
    cols_width = (tiles // cols_axis) * size
    row, col = lax.axis_index("row"), lax.axis_index("col")
    where = jnp.stack([row, col]).astype(jnp.int32)

    def ring(x, shift):
        return lax.ppermute(x, "col", [(c, (c + shift) % cols_axis) for c in range(cols_axis)])

    def swap(x, mask):
        return lax.ppermute(x, "row", [(r, r ^ mask) for r in range(rows_axis)])

    def spread(parts):
        return [parts[0]] + [swap(parts[n], 2 * n) for n in range(1, pairs)]

    chunks = [design]
    for _ in range(1, cols_axis):
        chunks.append(ring(chunks[-1], 1))

    block_rows = design.shape[0]
    near = factor_kernel(observations, gaps, noise_var, arc_lengths, arc_amp, arc_decay)
    weight = near[:block_rows]
    line = [near] + [ring(near, s) for s in range(1, cols_axis)]
    line_obs = jnp.stack([part[block_rows] for part in line])
    obs_all = jnp.stack([line_obs] + [swap(line_obs, m) for m in range(1, rows_axis)])

    packed = [spread(pack(design, None, tile_map, where, rows_axis, cols_axis))]
    for s in range(1, cols_axis):
        weight_s = line[s][:block_rows]
        packed.append(spread(pack(chunks[s], weight_s, tile_map, where, rows_axis, cols_axis)))

    weights = [weight] + [swap(weight, 2 * n) for n in range(1, pairs)]
    obs_first = obs_all[::2, : cols_axis - 1].swapaxes(0, 1).reshape(1, -1)
    keep, give, rhs_first = gram_first(
        packed[0],
        weights,
        [block for s in range(1, cols_axis - 1) for block in packed[s]],
        obs_first,
        rows_width,
        cols_width,
    )
    half = rows_width // 2
    other = swap(give, 1)
    other_rhs = swap(rhs_first[0, half:], 1)
    theirs = [swap(block, 1) for block in packed[-1]]
    obs_last = jnp.concatenate([obs_all[::2, -1], obs_all[1::2, -1]], axis=0).reshape(1, -1)
    gram, rhs_last = gram_last(
        keep, other, packed[-1], theirs, obs_last, rows_width, cols_width
    )
    normal_rhs = rhs_first[0, :half] + other_rhs + rhs_last[0]
    from_row, from_col = plan // cols_axis, plan % cols_axis
    ahead = (col - from_col + cols_axis) % cols_axis
    place = jnp.bitwise_xor(from_row, row) * cols_axis + ahead
    balanced_obs = jnp.take(obs_all.reshape(-1, block_rows), place, axis=0)
    return (gram, normal_rhs, balanced_obs)


def cut_columns(sizes, fetch, row, outs):
    per_row, per_col, own, half, base = sizes
    across_a, across_b, along_a, along_b, keep = outs
    rows_width = 2 * own

    def rows_of(n, core):
        there = jnp.bitwise_xor(row, 2 * n + core)
        return fetch(there * per_row, per_row)

    part = fetch(base, per_col)
    keep[:, rows_width:] = part
    across_a[:, own:] = part[:, :half]
    along_b[:, rows_width:] = part[:, :half]
    across_b[:, rows_width:] = part[:, half:]
    along_a[:, own:] = part[:, half:]
    across_a[:, :own] = rows_of(3, 0)
    along_a[:, :own] = rows_of(3, 1)
    for n, target in ((1, across_b), (2, along_b), (0, keep)):
        target[:, :own] = rows_of(n, 0)
        target[:, own:rows_width] = rows_of(n, 1)


def cut_widths(own, cols_width):
    half = cols_width // 2
    return [own + half, 2 * own + half, own + half, 2 * own + half, 2 * own + cols_width]


def head(design, small, tables, tile_map, where, rows_axis, cols_axis):
    block_rows, columns = design.shape
    tiles = tile_map.shape[0]
    size = columns // tiles
    per_row, per_col = tiles // rows_axis, tiles // cols_axis
    own, cols_width = per_row * size, per_col * size
    arcs = tables[0].shape[1]

    def kernel(where_ref, *refs):
        sources = refs[:8]
        near_ref = refs[8]
        outs = refs[9:14]
        far_ref, near_cols_ref = refs[14:16]
        x_ref, obs_ref, gap_ref, noise_ref, len_ref, amp_ref, decay_ref, map_ref, held, sems = refs[16:]
        targets = (x_ref, obs_ref, gap_ref, noise_ref, len_ref, amp_ref, decay_ref, map_ref)
        copies = [
            pltpu.make_async_copy(source, target, sems.at[k])
            for k, (source, target) in enumerate(zip(sources, targets))
        ]
        for copy in copies[1:] + copies[:1]:
            copy.start()
        for copy in copies[1:]:
            copy.wait()
        weight, white = factor_math(
            block_rows, arcs, len_ref, amp_ref, decay_ref, obs_ref, gap_ref, noise_ref
        )
        near_ref[:block_rows, :] = weight
        near_ref[block_rows:, :] = white
        copies[0].wait()
        row, col = where_ref[0], where_ref[1]

        def fetch(base, count):
            for j in range(count):
                at = pl.multiple_of(map_ref[0, base + j] * size, size)
                held[:, j * size : (j + 1) * size] = x_ref[:, pl.ds(at, size)]
            return split_dot(near_ref[:block_rows, :], held[:, : count * size])

        cut_columns((per_row, per_col, own, cols_width // 2, col * per_col), fetch, row, outs)
        far_ref[...] = fetch(jnp.bitwise_xor(col, 3) * per_col, per_col)
        near_cols_ref[...] = fetch(jnp.bitwise_xor(col, 2) * per_col, per_col)

    line = pltpu.VMEM((1, block_rows), F32)
    outs = [(block_rows + 8, block_rows, F32)]
    outs += [(block_rows, w, BF16) for w in cut_widths(own, cols_width) + [cols_width] * 2]
    return pl.pallas_call(
        kernel,
        name="head",
        in_specs=[SMEM] + [ANY] * 8,
        out_specs=[VMEM] * 8,
        out_shape=[jax.ShapeDtypeStruct((h, w), t) for h, w, t in outs],
        scratch_shapes=[
            pltpu.VMEM((block_rows, columns), BF16),
            line,
            pltpu.VMEM((1, block_rows), jnp.int32),
            line,
            pltpu.SMEM((1, arcs), jnp.int32),
            pltpu.SMEM((1, arcs), F32),
            pltpu.SMEM((1, arcs), F32),
            pltpu.SMEM((1, tiles), jnp.int32),
            pltpu.VMEM((block_rows, max(2 * own, cols_width)), BF16),
            pltpu.SemaphoreType.DMA((8,)),
        ],
        cost_estimate=pl.CostEstimate(flops=10**9, bytes_accessed=5 * 10**6, transcendentals=0),
        compiler_params=pltpu.CompilerParams(vmem_limit_bytes=10 << 20),
    )(where, design, *[v.reshape(1, -1) for v in small], *tables, tile_map.reshape(1, -1))


def pack_cut(chunks, nears, tile_map, where, rows_axis, cols_axis):
    block_rows, columns = chunks[0].shape
    tiles = tile_map.shape[0]
    size = columns // tiles
    per_row, per_col = tiles // rows_axis, tiles // cols_axis
    own, cols_width = per_row * size, per_col * size
    count = len(chunks)

    def kernel(map_ref, where_ref, *refs):
        near_refs, x_refs = refs[:count], refs[count : 2 * count]
        outs, held = refs[2 * count : -1], refs[-1]
        row, col = where_ref[0], where_ref[1]
        at_end = where_ref[2] == 1

        def choose(refs, rows, cols):
            first = refs[0][rows, cols]
            return first if count == 1 else jnp.where(at_end, refs[1][rows, cols], first)

        everything = pl.ds(0, block_rows)
        weight = choose(near_refs, everything, pl.ds(0, block_rows))

        def fetch(base, count):
            for j in range(count):
                at = pl.multiple_of(map_ref[base + j] * size, size)
                held[:, j * size : (j + 1) * size] = choose(x_refs, everything, pl.ds(at, size))
            return split_dot(weight, held[:, : count * size])

        cut_columns((per_row, per_col, own, cols_width // 2, col * per_col), fetch, row, outs)

    return pl.pallas_call(
        kernel,
        name="pack_cut",
        in_specs=[SMEM, SMEM] + [VMEM] * (2 * count),
        out_specs=[VMEM] * 5,
        out_shape=[
            jax.ShapeDtypeStruct((block_rows, w), BF16) for w in cut_widths(own, cols_width)
        ],
        scratch_shapes=[pltpu.VMEM((block_rows, max(own, cols_width)), BF16)],
        cost_estimate=pl.CostEstimate(flops=10**9, bytes_accessed=5 * 10**6, transcendentals=0),
        compiler_params=pltpu.CompilerParams(vmem_limit_bytes=8 << 20),
    )(tile_map, where, *nears, *chunks)


def row_parts(keep, xb, yb, fa, fb, own):
    block_rows = keep.shape[0]

    def kernel(keep_ref, xb_ref, yb_ref, fa_ref, fb_ref, lead_ref, rest_ref):
        for n, ref in enumerate((keep_ref, xb_ref, yb_ref)):
            lead_ref[:, n * block_rows : (n + 1) * block_rows] = ref[:, :own].T
            rest_ref[:, n * block_rows : (n + 1) * block_rows] = ref[:, own : 2 * own].T
        lead_ref[:, 3 * block_rows :] = fa_ref[:, :own].T
        rest_ref[:, 3 * block_rows :] = fb_ref[:, :own].T

    return pl.pallas_call(
        kernel,
        name="row_parts",
        in_specs=[VMEM] * 5,
        out_specs=[VMEM] * 2,
        out_shape=[jax.ShapeDtypeStruct((own, 4 * block_rows), BF16)] * 2,
        cost_estimate=pl.CostEstimate(flops=10**9, bytes_accessed=5 * 10**6, transcendentals=0),
        compiler_params=pltpu.CompilerParams(vmem_limit_bytes=4 << 20),
    )(keep, xb, yb, fa, fb)


def obs_rows(obs, places, plan, where, cols_axis):
    block_rows = obs[0].shape[1]

    def kernel(plan_ref, where_ref, *refs):
        sources, (rows_ref, picked_ref, held) = refs[:-3], refs[-3:]
        at = 0
        for source in sources:
            held[at : at + source.shape[0], :] = source[...]
            at += source.shape[0]
        at = 0
        end = where_ref[2]
        planes = (0, 1, 3 - end, 2 + end)
        for m, s in places:
            rows_ref[:, at : at + block_rows] = jnp.broadcast_to(
                held[pl.ds(m * cols_axis + planes[s], 1), :], (8, block_rows)
            )
            at += block_rows
        from_row = lax.div(plan_ref[0], cols_axis)
        from_col = lax.rem(plan_ref[0], cols_axis)
        mask = jnp.bitwise_xor(from_row, where_ref[0])
        step = jnp.bitwise_xor(where_ref[1], from_col)
        picked_ref[...] = held[pl.ds(mask * cols_axis + step, 1), :]

    return pl.pallas_call(
        kernel,
        name="obs_rows",
        in_specs=[SMEM, SMEM] + [VMEM] * len(obs),
        out_specs=[VMEM] * 2,
        out_shape=[
            jax.ShapeDtypeStruct((8, len(places) * block_rows), F32),
            jax.ShapeDtypeStruct((1, block_rows), F32),
        ],
        scratch_shapes=[pltpu.VMEM((sum(v.shape[0] for v in obs), block_rows), F32)],
        cost_estimate=pl.CostEstimate(flops=10**7, bytes_accessed=10**5, transcendentals=0),
        compiler_params=pltpu.CompilerParams(vmem_limit_bytes=4 << 20),
    )(plan, where, *obs)


def gram_direct(
    blocks, ready, operands, rows, at_row, left_width, cols_width, before, halves, out_far
):
    count = len(operands)
    width = left_width // halves
    step = cols_width // 6 if cols_width % 6 == 0 and (cols_width // 6) % 128 == 0 else 128
    steps = cols_width // step
    depth = sum(block[0] for block in blocks)
    total_depth = depth + sum(part[0] for _, group in ready for part in group)

    def kernel(*refs):
        sources = refs[:count]
        rows_ref = refs[count]
        sums = refs[count + 1 : count + 1 + len(before)]
        outs = refs[count + 1 + len(before) : count + 1 + len(before) + 2 * halves]
        scratch = refs[count + 1 + len(before) + 2 * halves :]
        turned = scratch[0]
        total = jnp.zeros((8, left_width), F32)
        top = 0
        for height, lefts, _ in blocks:
            seen = rows_ref[:, at_row + top : at_row + top + height].astype(BF16)
            for which, first, begin, length, to in lefts:
                left = sources[which][first : first + height, begin : begin + length]
                turned[to : to + length, top : top + height] = left.T
            left = jnp.concatenate(
                [
                    sources[which][first : first + height, begin : begin + length]
                    for which, first, begin, length, _ in sorted(lefts, key=lambda p: p[4])
                ],
                axis=1,
            )
            total = total + jnp.dot(seen, left, preferred_element_type=F32)
            top += height
        for which, group in ready:
            height = sum(part[0] for part in group)
            seen = rows_ref[:, at_row + top : at_row + top + height].astype(BF16)
            total = total + lax.dot_general(
                seen, sources[which][...], (((1,), (1,)), ((), ())), preferred_element_type=F32
            )
            top += height
        half_sums = len(before) // 2
        for h in range(halves):
            part = total[:, h * width : (h + 1) * width]
            for extra in sums[half_sums:]:
                part = part + extra[...]
            outs[halves + h][...] = part
        copies = [None, None]
        for t in range(steps):
            begin = t * step

            def cut(group):
                pieces = []
                for height, cols in group:
                    for which, first, start, length, to in cols:
                        if to <= begin < to + length:
                            at = start + begin - to
                            pieces.append(sources[which][first : first + height, at : at + step])
                return jnp.concatenate(pieces, axis=0)

            right = cut([(height, cols) for height, _, cols in blocks])
            rights = [(which, cut(group)) for which, group in ready]
            for h in range(halves):
                part = jnp.dot(
                    turned[h * width : (h + 1) * width, :], right, preferred_element_type=F32
                )
                for which, other in rights:
                    part = part + jnp.dot(
                        sources[which][...], other, preferred_element_type=F32
                    )
                for extra in sums[:half_sums]:
                    part = part + extra[:, begin : begin + step]
                if not out_far:
                    outs[h][:, begin : begin + step] = part
                    continue
                tile, sems = scratch[1:]
                slot = t % 2
                if copies[slot] is not None:
                    copies[slot].wait()
                tile[slot] = part
                copies[slot] = pltpu.make_async_copy(
                    tile.at[slot], outs[0].at[:, pl.ds(begin, step)], sems.at[slot]
                )
                copies[slot].start()
        for copy in copies:
            if copy is not None:
                copy.wait()

    scratch_shapes = [pltpu.VMEM((left_width, depth), BF16)]
    scratch_bytes = 2 * left_width * depth
    if out_far:
        scratch_shapes += [pltpu.VMEM((2, width, step), F32), pltpu.SemaphoreType.DMA((2,))]
        scratch_bytes += 8 * width * step
    return pl.pallas_call(
        kernel,
        in_specs=[VMEM] * (count + 1 + len(before)),
        out_specs=[ANY if out_far else VMEM] * halves + [VMEM] * halves,
        out_shape=[jax.ShapeDtypeStruct((width, cols_width), F32)] * halves
        + [jax.ShapeDtypeStruct((8, width), F32)] * halves,
        scratch_shapes=scratch_shapes,
        cost_estimate=pl.CostEstimate(
            flops=2 * total_depth * left_width * cols_width,
            bytes_accessed=2 * 10**7,
            transcendentals=0,
        ),
        compiler_params=pltpu.CompilerParams(vmem_limit_bytes=scratch_bytes + (4 << 20)),
    )(*operands, rows, *before)


def on_device_square(
    rows_axis,
    cols_axis,
    design,
    observations,
    gaps,
    noise_var,
    arc_lengths,
    arc_amp,
    arc_decay,
    plan,
    tile_map,
):
    block_rows, columns = design.shape
    tiles = tile_map.shape[0]
    size = columns // tiles
    own = (tiles // rows_axis) * size
    wide = 2 * own
    cols_width = (tiles // cols_axis) * size
    half = cols_width // 2
    row, col = lax.axis_index("row"), lax.axis_index("col")
    last = cols_axis - 1
    at_end = jnp.logical_or(col == 0, col == last)
    where = jnp.stack([row, col, at_end.astype(jnp.int32)]).astype(jnp.int32)

    def hop(x, pairs):
        return lax.ppermute(x, "col", pairs)

    def cross(x, mask):
        return hop(x, [(c, c ^ mask) for c in range(cols_axis)])

    def swap(x, mask):
        return lax.ppermute(x, "row", [(r, r ^ mask) for r in range(rows_axis)])

    outward = [(1, 0), (last - 1, last)]
    inward = [(last, 1), (0, last - 1)]
    beside = cross(design, 1)
    inner = hop(design, [(1, last - 1), (last - 1, 1)])
    outer = hop(inner, outward)
    near, *parts = head(
        design,
        (observations, gaps, noise_var),
        (arc_lengths, arc_amp, arc_decay),
        tile_map,
        where,
        rows_axis,
        cols_axis,
    )
    line = [near] + [cross(near, s) for s in range(1, cols_axis)]
    line_obs = jnp.stack([part[block_rows] for part in line])
    obs = [line_obs] + [swap(line_obs, m) for m in range(1, rows_axis)]

    def trade(xa, xb, ya, yb, keep):
        xa, ya = swap(xa, 2), swap(ya, 4)
        xb, yb = swap(xb, 2), swap(yb, 4)
        return keep, xa, xb, ya, yb, swap(xa, 4), swap(ya, 2)

    traded = [trade(*parts[:5])]
    sources = ([beside], [line[1]]), ([inner, outer], [line[3], line[2]])
    for s, (raw, nears) in enumerate(sources, 1):
        cut = pack_cut(raw, nears, tile_map, where, rows_axis, cols_axis)
        traded.append(trade(*cut))

    keep, _, xb, _, yb, fa, fb = traded[0]
    lead, rest = row_parts(keep, xb, yb, fa, fb, own)
    far_ends = hop(parts[5], [(last, 0), (0, last)])
    far_inner = hop(parts[6], inward)
    far_cols = jnp.where(at_end, far_ends, far_inner)
    rest_inner = hop(rest, inward)
    lead_inner = hop(lead, inward)
    far_rest = jnp.where(at_end, hop(rest_inner, outward), rest_inner)
    far_lead = jnp.where(at_end, hop(lead_inner, outward), lead_inner)
    x3, y3 = swap(far_cols, 2), swap(far_cols, 4)
    fa3 = swap(x3[:, :half], 4)
    fb3 = swap(y3[:, half:], 2)

    def part_blocks(first, height, left, both):
        wide_left = wide if both else own
        begin = 0 if both else left * own
        blocks = []
        for k in (0, 2, 4):
            blocks.append([height, [(first + k, 0, begin, wide_left, 0)], []])
        corner = [(first + 5 + left, 0, 0, own, 0)]
        if both:
            corner.append((first + 6, 0, 0, own, own))
        blocks.append([height, corner, []])
        for n, k, begin, length, to in (
            (0, 0, wide, cols_width, 0),
            (1, 1, own, half, 0),
            (1, 2, wide, half, half),
            (2, 4, wide, half, 0),
            (2, 3, own, half, half),
            (3, 5, own, half, 0),
            (3, 6, own, half, half),
        ):
            blocks[n][2].append((first + k, 0, begin, length, to))
        return blocks

    early = [(2 * n, s) for s in range(last - 1) for n in range(4)]
    mid = [(2 * n + core, last - 1) for core in (0, 1) for n in range(3)]
    late = [(6 + core, last - 1) for core in (0, 1)]
    late += [(2 * n + core, last) for core in (0, 1) for n in range(4)]
    rows, balanced_obs = obs_rows(obs, early + mid + late, plan, where, cols_axis)

    blocks, operands = [], []
    for s in range(last - 1):
        blocks += part_blocks(len(operands), block_rows, 0, True)
        operands += list(traded[s])
    keep, give, keep_rhs, give_rhs = gram_direct(
        blocks, [], operands, rows, 0, wide, cols_width, (), 2, False
    )
    other = swap(give, 1)
    other_rhs = swap(give_rhs, 1)

    mine = list(traded[last - 1])
    theirs = [swap(v, 1) for v in mine]
    sides = [part_blocks(0, block_rows, 0, False), part_blocks(5, block_rows, 1, False)]
    at_row = len(early) * block_rows
    most, most_rhs = gram_direct(
        sides[0][:3] + sides[1][:3],
        [],
        mine[:5] + theirs[:5],
        rows,
        at_row,
        own,
        cols_width,
        (keep, other, keep_rhs, other_rhs),
        1,
        False,
    )
    at_row += len(mid) * block_rows
    mine_far = [far_cols, x3, y3, fa3, fb3]
    theirs_far = [swap(v, 1) for v in mine_far]
    their_rest = swap(far_rest, 1)
    corners, ready = [], []
    operands = []
    for core, group in enumerate((mine, theirs)):
        cols = [(len(operands), 0, own, half, 0), (len(operands) + 1, 0, own, half, half)]
        corners.append((block_rows, [(len(operands) + core, 0, 0, own, 0)], cols))
        operands += group[5:]
    for left, group in ((far_lead, mine_far), (their_rest, theirs_far)):
        first = len(operands)
        operands += [left] + group
        plain = [(block_rows, [(first + 1 + n, 0, 0, cols_width, 0)]) for n in range(3)]
        plain.append((block_rows, [(first + 4, 0, 0, half, 0), (first + 5, 0, 0, half, half)]))
        ready.append((first, plain))
    gram, rhs = gram_direct(
        corners, ready, operands, rows, at_row, own, cols_width, (most, most_rhs), 1, True
    )
    return (gram, rhs[0], balanced_obs)


def solution(mesh):
    placed = (
        P(("row", "col"), None),
        P(("row", "col")),
        P(("row", "col")),
        P(("row", "col")),
        P(("row", "col"), None),
        P(("row", "col"), None),
        P(("row", "col"), None),
        P(("row", "col")),
        P(),
    )
    rows_axis, cols_axis = mesh.shape["row"], mesh.shape["col"]
    square = rows_axis == 2**3 and cols_axis == 2**2

    def body(*args):
        if not square:
            return on_device_any(rows_axis, cols_axis, *args)
        return on_device_square(rows_axis, cols_axis, *args)

    return jax.shard_map(
        body,
        mesh=mesh,
        in_specs=placed,
        out_specs=(P("row", "col"), P("row"), P(("row", "col"), None)),
        check_vma=False,
    )
```

```python
import jax
import jax.numpy as jnp
from jax import lax
from jax.experimental import pallas as pl
from jax.experimental.pallas import tpu as pltpu
from jax.sharding import PartitionSpec as P


F32, BF16 = jnp.float32, jnp.bfloat16
ANY = pl.BlockSpec(memory_space=pl.ANY)
VMEM = pl.BlockSpec(memory_space=pltpu.VMEM)
SMEM = pl.BlockSpec(memory_space=pltpu.SMEM)


def factor_math(n, arcs, len_ref, amp_ref, decay_ref, obs_ref, gap_ref, noise_ref):
    lane = lax.broadcasted_iota(jnp.int32, (8, n), 1)
    live = jnp.broadcast_to(gap_ref[...].astype(F32), (8, n))
    noise = jnp.broadcast_to(noise_ref[...], (8, n))
    big_line = lax.broadcasted_iota(jnp.int32, (n, n), 0)
    big_lane = lax.broadcasted_iota(jnp.int32, (n, n), 1)
    arc = jnp.zeros((8, n), jnp.int32)
    first = lane == 0
    arc_line = jnp.zeros((n, n), jnp.int32)
    end = 0
    for k in range(arcs):
        end = end + len_ref[0, k]
        arc = arc + (lane >= end).astype(jnp.int32)
        arc_line = arc_line + (big_line >= end).astype(jnp.int32)
        first = jnp.logical_or(first, lane == end)
    amp = jnp.zeros((8, n), F32)
    decay = jnp.ones((8, n), F32)
    for k in range(arcs):
        amp = jnp.where(arc == k, amp_ref[0, k], amp)
        decay = jnp.where(arc == k, decay_ref[0, k], decay)

    def back(x, shift):
        return pltpu.roll(x, shift, axis=1)

    fresh = (1.0 - decay * decay) * amp
    a = back(decay * decay * noise + fresh * live, 1)
    b = back(fresh * noise, 1)
    c = back(live, 1)
    d = back(noise, 1)
    a = jnp.where(first, 0.0, a)
    b = jnp.where(first, amp, b)
    c = jnp.where(first, 0.0, c)
    d = jnp.where(first, 1.0, d)
    shift = 1
    while shift < n:
        ok = lane >= shift
        pa, pb = jnp.where(ok, back(a, shift), 1.0), jnp.where(ok, back(b, shift), 0.0)
        pc, pd = jnp.where(ok, back(c, shift), 0.0), jnp.where(ok, back(d, shift), 1.0)
        a, b, c, d = a * pa + b * pc, a * pb + b * pd, c * pa + d * pc, c * pb + d * pd
        level = 1.0 / (a + b + c + d)
        a, b, c, d = a * level, b * level, c * level, d * level
        shift *= 2
    variance = b / d
    total = live * variance + noise
    root = 1.0 / jnp.sqrt(total)
    fade = jnp.log(decay * noise / total)
    gain = decay * variance * live / total
    below = big_lane < big_line
    fades = jnp.where(below, jnp.broadcast_to(fade[:1], (n, n)), 0.0)
    mask = below.astype(BF16)
    spans = jnp.zeros((n, n), F32)
    for _ in range(3):
        part = fades.astype(BF16)
        spans = spans + jnp.dot(part, mask, preferred_element_type=F32)
        fades = fades - part.astype(F32)
    diagonal = big_line == big_lane

    def upright(x):
        return jnp.sum(jnp.where(diagonal, jnp.broadcast_to(x[:1], (n, n)), 0.0), axis=1, keepdims=True)

    left = upright(live * root)
    same = jnp.logical_and(below, arc_line == jnp.broadcast_to(arc[:1], (n, n)))
    weight = jnp.where(same, -left * jnp.exp(spans) * jnp.broadcast_to(gain[:1], (n, n)), 0.0)
    weight = jnp.where(diagonal, left, weight)
    white = jnp.sum(weight * jnp.broadcast_to(obs_ref[...], (n, n)), axis=1, keepdims=True)
    white_row = jnp.sum(jnp.where(diagonal, white, 0.0), axis=0, keepdims=True)
    return weight, jnp.broadcast_to(white_row, (8, n))


def factor_kernel(observations, gaps, noise_var, arc_lengths, arc_amp, arc_decay):
    n = observations.shape[0]
    arcs = arc_lengths.shape[1]

    def kernel(len_ref, amp_ref, decay_ref, obs_ref, gap_ref, noise_ref, out_ref):
        out_ref[:n, :], out_ref[n:, :] = factor_math(
            n, arcs, len_ref, amp_ref, decay_ref, obs_ref, gap_ref, noise_ref
        )

    row = (1, n)
    return pl.pallas_call(
        kernel,
        name="factor",
        in_specs=[SMEM] * 3 + [VMEM] * 3,
        out_specs=VMEM,
        out_shape=jax.ShapeDtypeStruct((n + 8, n), F32),
        cost_estimate=pl.CostEstimate(flops=10**8, bytes_accessed=10**5, transcendentals=0),
        compiler_params=pltpu.CompilerParams(vmem_limit_bytes=4 << 20),
    )(
        arc_lengths,
        arc_amp,
        arc_decay,
        observations.reshape(row),
        gaps.reshape(row),
        noise_var.reshape(row),
    )


def split_dot(w, x):
    high = w.astype(BF16)
    low = (w - high.astype(F32)).astype(BF16)
    total = jnp.dot(high, x, preferred_element_type=F32)
    return (total + jnp.dot(low, x, preferred_element_type=F32)).astype(BF16)


def pack(chunk, weight, tile_map, where, rows_axis, cols_axis):
    block_rows, columns = chunk.shape
    tiles = tile_map.shape[0]
    size = columns // tiles
    pairs = rows_axis // 2
    per_row, per_col = tiles // rows_axis, tiles // cols_axis
    wide = (2 * per_row + per_col) * size

    def kernel(map_ref, where_ref, x_ref, *refs):
        outs = refs[-pairs - 1 : -1]
        held = refs[-1]
        row, col = where_ref[0], where_ref[1]

        def fetch(base, count, to):
            for j in range(count):
                at = pl.multiple_of(map_ref[base + j] * size, size)
                held[:, (to + j) * size : (to + j + 1) * size] = x_ref[:, pl.ds(at, size)]

        def finish(start, stop, targets):
            part = held[:, start:stop]
            if weight is not None:
                part = split_dot(refs[0][...], part)
            for target in targets:
                target[:, start:stop] = part

        own = per_row * size
        fetch(col * per_col, per_col, 2 * per_row)
        finish(2 * own, wide, outs)
        for n in range(pairs):
            there = jnp.bitwise_xor(row, 2 * n)
            fetch(there * per_row, per_row, 0)
            fetch(jnp.bitwise_xor(there, 1) * per_row, per_row, per_row)
            finish(0, 2 * own, [outs[n]])

    args = (tile_map, where, chunk) + (() if weight is None else (weight,))
    return pl.pallas_call(
        kernel,
        name="pack",
        in_specs=[SMEM, SMEM] + [VMEM] * (len(args) - 2),
        out_specs=[VMEM] * pairs,
        out_shape=[jax.ShapeDtypeStruct((block_rows, wide), BF16)] * pairs,
        scratch_shapes=[pltpu.VMEM((block_rows, wide), BF16)],
        cost_estimate=pl.CostEstimate(flops=10**9, bytes_accessed=5 * 10**6, transcendentals=0),
        compiler_params=pltpu.CompilerParams(vmem_limit_bytes=24 << 20),
    )(*args)


def gram_first(raw, weights, white, obs, rows_width, cols_width):
    block_rows, wide = raw[0].shape
    count = len(raw) + len(white)
    depth = count * block_rows
    half = rows_width // 2
    step = cols_width // 6 if cols_width % 6 == 0 and (cols_width // 6) % 128 == 0 else 128
    steps = cols_width // step

    def kernel(*refs):
        blocks = refs[:count]
        w_refs = refs[count : count + len(raw)]
        obs_ref = refs[count + len(raw)]
        keep_ref, give_ref, rhs_ref = refs[-7:-4]
        fresh, held, turned, sems = refs[-4:]

        @pl.when(pl.program_id(0) == 0)
        def _():
            copies = []
            for b in range(count):
                to = fresh.at[b] if b < len(raw) else held.at[pl.ds(b * block_rows, block_rows)]
                copies.append(pltpu.make_async_copy(blocks[b], to, sems.at[b]))
                copies[-1].start()
            for b in range(count):
                rows = slice(b * block_rows, (b + 1) * block_rows)
                copies[b].wait()
                if b < len(raw):
                    held[rows, :] = split_dot(w_refs[b][...], fresh[b])
                turned[:, rows] = held[rows, :rows_width].T
            spread = jnp.broadcast_to(obs_ref[...].astype(BF16), (16, depth))
            rhs_ref[...] = jnp.dot(spread, held[:, :rows_width], preferred_element_type=F32)

        at = pl.multiple_of(rows_width + pl.program_id(0) * step, 128)
        right = held[:, pl.ds(at, step)]
        keep_ref[...] = jnp.dot(turned[:half, :], right, preferred_element_type=F32)
        give_ref[...] = jnp.dot(turned[half:, :], right, preferred_element_type=F32)

    tile = pl.BlockSpec((half, step), lambda i: (0, i))
    return pl.pallas_call(
        kernel,
        name="gram_first",
        grid=(steps,),
        in_specs=[ANY] * count + [VMEM] * (len(raw) + 1),
        out_specs=[tile, tile, pl.BlockSpec((16, rows_width), lambda i: (0, 0))],
        out_shape=[jax.ShapeDtypeStruct((half, cols_width), F32)] * 2
        + [jax.ShapeDtypeStruct((16, rows_width), F32)],
        scratch_shapes=[
            pltpu.VMEM((len(raw), block_rows, wide), BF16),
            pltpu.VMEM((depth, wide), BF16),
            pltpu.VMEM((rows_width, depth), BF16),
            pltpu.SemaphoreType.DMA((count,)),
        ],
        cost_estimate=pl.CostEstimate(
            flops=2 * depth * rows_width * cols_width, bytes_accessed=2 * 10**7, transcendentals=0
        ),
        compiler_params=pltpu.CompilerParams(vmem_limit_bytes=48 << 20),
    )(*raw, *white, *weights, obs)


def gram_last(keep, other, mine, theirs, obs, rows_width, cols_width):
    block_rows, wide = mine[0].shape
    count = len(mine) + len(theirs)
    depth = count * block_rows
    half = rows_width // 2
    step = cols_width // 6 if cols_width % 6 == 0 and (cols_width // 6) % 128 == 0 else 128
    steps = cols_width // step

    def kernel(*refs):
        keep_ref, other_ref = refs[:2]
        blocks = refs[2 : 2 + count]
        obs_ref = refs[2 + count]
        out_ref, rhs_ref = refs[-5:-3]
        held, turned, sems = refs[-3:]

        @pl.when(pl.program_id(0) == 0)
        def _():
            copies = []
            for b in range(count):
                to = held.at[pl.ds(b * block_rows, block_rows)]
                copies.append(pltpu.make_async_copy(blocks[b], to, sems.at[b]))
                copies[-1].start()
            total = jnp.zeros((16, half), F32)
            for b in range(count):
                rows = slice(b * block_rows, (b + 1) * block_rows)
                lead = 0 if b < len(mine) else half
                copies[b].wait()
                left = held[rows, lead : lead + half]
                turned[:, rows] = left.T
                spread = jnp.broadcast_to(obs_ref[:, rows].astype(BF16), (16, block_rows))
                total = total + jnp.dot(spread, left, preferred_element_type=F32)
            rhs_ref[...] = total

        at = pl.multiple_of(rows_width + pl.program_id(0) * step, 128)
        right = held[:, pl.ds(at, step)]
        out_ref[...] = (keep_ref[...] + other_ref[...]) + jnp.dot(
            turned[...], right, preferred_element_type=F32
        )

    tile = pl.BlockSpec((half, step), lambda i: (0, i))
    return pl.pallas_call(
        kernel,
        name="gram_last",
        grid=(steps,),
        in_specs=[tile, tile] + [ANY] * count + [VMEM],
        out_specs=[tile, pl.BlockSpec((16, half), lambda i: (0, 0))],
        out_shape=[
            jax.ShapeDtypeStruct((half, cols_width), F32),
            jax.ShapeDtypeStruct((16, half), F32),
        ],
        scratch_shapes=[
            pltpu.VMEM((depth, wide), BF16),
            pltpu.VMEM((half, depth), BF16),
            pltpu.SemaphoreType.DMA((count,)),
        ],
        cost_estimate=pl.CostEstimate(
            flops=2 * depth * half * cols_width, bytes_accessed=2 * 10**7, transcendentals=0
        ),
        compiler_params=pltpu.CompilerParams(vmem_limit_bytes=48 << 20),
    )(keep, other, *mine, *theirs, obs)


def on_device_any(
    rows_axis,
    cols_axis,
    design,
    observations,
    gaps,
    noise_var,
    arc_lengths,
    arc_amp,
    arc_decay,
    plan,
    tile_map,
):
    columns = design.shape[1]
    tiles = tile_map.shape[0]
    size = columns // tiles
    pairs = rows_axis // 2
    rows_width = 2 * (tiles // rows_axis) * size
    cols_width = (tiles // cols_axis) * size
    row, col = lax.axis_index("row"), lax.axis_index("col")
    where = jnp.stack([row, col]).astype(jnp.int32)

    def ring(x, shift):
        return lax.ppermute(x, "col", [(c, (c + shift) % cols_axis) for c in range(cols_axis)])

    def swap(x, mask):
        return lax.ppermute(x, "row", [(r, r ^ mask) for r in range(rows_axis)])

    def spread(parts):
        return [parts[0]] + [swap(parts[n], 2 * n) for n in range(1, pairs)]

    chunks = [design]
    for _ in range(1, cols_axis):
        chunks.append(ring(chunks[-1], 1))

    block_rows = design.shape[0]
    near = factor_kernel(observations, gaps, noise_var, arc_lengths, arc_amp, arc_decay)
    weight = near[:block_rows]
    line = [near] + [ring(near, s) for s in range(1, cols_axis)]
    line_obs = jnp.stack([part[block_rows] for part in line])
    obs_all = jnp.stack([line_obs] + [swap(line_obs, m) for m in range(1, rows_axis)])

    packed = [spread(pack(design, None, tile_map, where, rows_axis, cols_axis))]
    for s in range(1, cols_axis):
        weight_s = line[s][:block_rows]
        packed.append(spread(pack(chunks[s], weight_s, tile_map, where, rows_axis, cols_axis)))

    weights = [weight] + [swap(weight, 2 * n) for n in range(1, pairs)]
    obs_first = obs_all[::2, : cols_axis - 1].swapaxes(0, 1).reshape(1, -1)
    keep, give, rhs_first = gram_first(
        packed[0],
        weights,
        [block for s in range(1, cols_axis - 1) for block in packed[s]],
        obs_first,
        rows_width,
        cols_width,
    )
    half = rows_width // 2
    other = swap(give, 1)
    other_rhs = swap(rhs_first[0, half:], 1)
    theirs = [swap(block, 1) for block in packed[-1]]
    obs_last = jnp.concatenate([obs_all[::2, -1], obs_all[1::2, -1]], axis=0).reshape(1, -1)
    gram, rhs_last = gram_last(
        keep, other, packed[-1], theirs, obs_last, rows_width, cols_width
    )
    normal_rhs = rhs_first[0, :half] + other_rhs + rhs_last[0]
    from_row, from_col = plan // cols_axis, plan % cols_axis
    ahead = (col - from_col + cols_axis) % cols_axis
    place = jnp.bitwise_xor(from_row, row) * cols_axis + ahead
    balanced_obs = jnp.take(obs_all.reshape(-1, block_rows), place, axis=0)
    return (gram, normal_rhs, balanced_obs)


def cut_columns(sizes, fetch, row, outs):
    per_row, per_col, own, half, base = sizes
    across_a, across_b, along_a, along_b, keep = outs
    rows_width = 2 * own

    def rows_of(n, core):
        there = jnp.bitwise_xor(row, 2 * n + core)
        return fetch(there * per_row, per_row)

    part = fetch(base, per_col)
    keep[:, rows_width:] = part
    across_a[:, own:] = part[:, :half]
    along_b[:, rows_width:] = part[:, :half]
    across_b[:, rows_width:] = part[:, half:]
    along_a[:, own:] = part[:, half:]
    across_a[:, :own] = rows_of(3, 0)
    along_a[:, :own] = rows_of(3, 1)
    for n, target in ((1, across_b), (2, along_b), (0, keep)):
        target[:, :own] = rows_of(n, 0)
        target[:, own:rows_width] = rows_of(n, 1)


def cut_widths(own, cols_width):
    half = cols_width // 2
    return [own + half, 2 * own + half, own + half, 2 * own + half, 2 * own + cols_width]


def head(design, small, tables, tile_map, where, rows_axis, cols_axis):
    block_rows, columns = design.shape
    tiles = tile_map.shape[0]
    size = columns // tiles
    per_row, per_col = tiles // rows_axis, tiles // cols_axis
    own, cols_width = per_row * size, per_col * size
    arcs = tables[0].shape[1]

    def kernel(where_ref, *refs):
        sources = refs[:8]
        near_ref = refs[8]
        outs = refs[9:14]
        far_ref, near_cols_ref = refs[14:16]
        x_ref, obs_ref, gap_ref, noise_ref, len_ref, amp_ref, decay_ref, map_ref, held, sems = refs[16:]
        targets = (x_ref, obs_ref, gap_ref, noise_ref, len_ref, amp_ref, decay_ref, map_ref)
        copies = [
            pltpu.make_async_copy(source, target, sems.at[k])
            for k, (source, target) in enumerate(zip(sources, targets))
        ]
        for copy in copies[1:] + copies[:1]:
            copy.start()
        for copy in copies[1:]:
            copy.wait()
        weight, white = factor_math(
            block_rows, arcs, len_ref, amp_ref, decay_ref, obs_ref, gap_ref, noise_ref
        )
        near_ref[:block_rows, :] = weight
        near_ref[block_rows:, :] = white
        copies[0].wait()
        row, col = where_ref[0], where_ref[1]

        def fetch(base, count):
            for j in range(count):
                at = pl.multiple_of(map_ref[0, base + j] * size, size)
                held[:, j * size : (j + 1) * size] = x_ref[:, pl.ds(at, size)]
            return split_dot(near_ref[:block_rows, :], held[:, : count * size])

        cut_columns((per_row, per_col, own, cols_width // 2, col * per_col), fetch, row, outs)
        far_ref[...] = fetch(jnp.bitwise_xor(col, 3) * per_col, per_col)
        near_cols_ref[...] = fetch(jnp.bitwise_xor(col, 2) * per_col, per_col)

    line = pltpu.VMEM((1, block_rows), F32)
    outs = [(block_rows + 8, block_rows, F32)]
    outs += [(block_rows, w, BF16) for w in cut_widths(own, cols_width) + [cols_width] * 2]
    return pl.pallas_call(
        kernel,
        name="head",
        in_specs=[SMEM] + [ANY] * 8,
        out_specs=[VMEM] * 8,
        out_shape=[jax.ShapeDtypeStruct((h, w), t) for h, w, t in outs],
        scratch_shapes=[
            pltpu.VMEM((block_rows, columns), BF16),
            line,
            pltpu.VMEM((1, block_rows), jnp.int32),
            line,
            pltpu.SMEM((1, arcs), jnp.int32),
            pltpu.SMEM((1, arcs), F32),
            pltpu.SMEM((1, arcs), F32),
            pltpu.SMEM((1, tiles), jnp.int32),
            pltpu.VMEM((block_rows, max(2 * own, cols_width)), BF16),
            pltpu.SemaphoreType.DMA((8,)),
        ],
        cost_estimate=pl.CostEstimate(flops=10**9, bytes_accessed=5 * 10**6, transcendentals=0),
        compiler_params=pltpu.CompilerParams(vmem_limit_bytes=10 << 20),
    )(where, design, *[v.reshape(1, -1) for v in small], *tables, tile_map.reshape(1, -1))


def pack_cut(chunks, nears, tile_map, where, rows_axis, cols_axis):
    block_rows, columns = chunks[0].shape
    tiles = tile_map.shape[0]
    size = columns // tiles
    per_row, per_col = tiles // rows_axis, tiles // cols_axis
    own, cols_width = per_row * size, per_col * size
    count = len(chunks)

    def kernel(map_ref, where_ref, *refs):
        near_refs, x_refs = refs[:count], refs[count : 2 * count]
        outs, held = refs[2 * count : -1], refs[-1]
        row, col = where_ref[0], where_ref[1]
        at_end = where_ref[2] == 1

        def choose(refs, rows, cols):
            first = refs[0][rows, cols]
            return first if count == 1 else jnp.where(at_end, refs[1][rows, cols], first)

        everything = pl.ds(0, block_rows)
        weight = choose(near_refs, everything, pl.ds(0, block_rows))

        def fetch(base, count):
            for j in range(count):
                at = pl.multiple_of(map_ref[base + j] * size, size)
                held[:, j * size : (j + 1) * size] = choose(x_refs, everything, pl.ds(at, size))
            return split_dot(weight, held[:, : count * size])

        cut_columns((per_row, per_col, own, cols_width // 2, col * per_col), fetch, row, outs)

    return pl.pallas_call(
        kernel,
        name="pack_cut",
        in_specs=[SMEM, SMEM] + [VMEM] * (2 * count),
        out_specs=[VMEM] * 5,
        out_shape=[
            jax.ShapeDtypeStruct((block_rows, w), BF16) for w in cut_widths(own, cols_width)
        ],
        scratch_shapes=[pltpu.VMEM((block_rows, max(own, cols_width)), BF16)],
        cost_estimate=pl.CostEstimate(flops=10**9, bytes_accessed=5 * 10**6, transcendentals=0),
        compiler_params=pltpu.CompilerParams(vmem_limit_bytes=8 << 20),
    )(tile_map, where, *nears, *chunks)


def row_parts(keep, xb, yb, fa, fb, own):
    block_rows = keep.shape[0]

    def kernel(keep_ref, xb_ref, yb_ref, fa_ref, fb_ref, lead_ref, rest_ref):
        for n, ref in enumerate((keep_ref, xb_ref, yb_ref)):
            lead_ref[:, n * block_rows : (n + 1) * block_rows] = ref[:, :own].T
            rest_ref[:, n * block_rows : (n + 1) * block_rows] = ref[:, own : 2 * own].T
        lead_ref[:, 3 * block_rows :] = fa_ref[:, :own].T
        rest_ref[:, 3 * block_rows :] = fb_ref[:, :own].T

    return pl.pallas_call(
        kernel,
        name="row_parts",
        in_specs=[VMEM] * 5,
        out_specs=[VMEM] * 2,
        out_shape=[jax.ShapeDtypeStruct((own, 4 * block_rows), BF16)] * 2,
        cost_estimate=pl.CostEstimate(flops=10**9, bytes_accessed=5 * 10**6, transcendentals=0),
        compiler_params=pltpu.CompilerParams(vmem_limit_bytes=4 << 20),
    )(keep, xb, yb, fa, fb)


def obs_rows(obs, places, plan, where, cols_axis, pick):
    block_rows = obs[0].shape[1]

    def kernel(plan_ref, where_ref, *refs):
        sources, (rows_ref, picked_ref, held) = refs[:-3], refs[-3:]
        at = 0
        for source in sources:
            held[at : at + source.shape[0], :] = source[...]
            at += source.shape[0]
        at = 0
        end = where_ref[2]
        planes = (0, 1, 3 - end, 2 + end)
        for m, s in places:
            line = (m % 2 * 4 + m // 2) * cols_axis + planes[s]
            rows_ref[:, at : at + block_rows] = jnp.broadcast_to(
                held[pl.ds(line, 1), :], (8, block_rows)
            )
            at += block_rows
        if pick:
            from_row = lax.div(plan_ref[0], cols_axis)
            from_col = lax.rem(plan_ref[0], cols_axis)
            mask = jnp.bitwise_xor(from_row, where_ref[0])
            line = lax.rem(mask, 2) * 4 + lax.div(mask, 2)
            step = jnp.bitwise_xor(where_ref[1], from_col)
            picked_ref[...] = held[pl.ds(line * cols_axis + step, 1), :]
        else:
            picked_ref[...] = held[:1, :]

    return pl.pallas_call(
        kernel,
        name="obs_rows",
        in_specs=[SMEM, SMEM] + [VMEM] * len(obs),
        out_specs=[VMEM] * 2,
        out_shape=[
            jax.ShapeDtypeStruct((8, len(places) * block_rows), F32),
            jax.ShapeDtypeStruct((1, block_rows), F32),
        ],
        scratch_shapes=[pltpu.VMEM((sum(v.shape[0] for v in obs), block_rows), F32)],
        cost_estimate=pl.CostEstimate(flops=10**7, bytes_accessed=10**5, transcendentals=0),
        compiler_params=pltpu.CompilerParams(vmem_limit_bytes=4 << 20),
    )(plan, where, *obs)


def gram_direct(
    blocks, ready, operands, rows, at_row, left_width, cols_width, before, halves, out_far
):
    count = len(operands)
    width = left_width // halves
    step = cols_width // 6 if cols_width % 6 == 0 and (cols_width // 6) % 128 == 0 else 128
    steps = cols_width // step
    depth = sum(block[0] for block in blocks)
    total_depth = depth + sum(part[0] for _, group in ready for part in group)

    def kernel(*refs):
        sources = refs[:count]
        rows_ref = refs[count]
        sums = refs[count + 1 : count + 1 + len(before)]
        outs = refs[count + 1 + len(before) : count + 1 + len(before) + 2 * halves]
        scratch = refs[count + 1 + len(before) + 2 * halves :]
        turned = scratch[0]
        total = jnp.zeros((8, left_width), F32)
        top = 0
        for height, lefts, _ in blocks:
            seen = rows_ref[:, at_row + top : at_row + top + height].astype(BF16)
            for which, first, begin, length, to in lefts:
                left = sources[which][first : first + height, begin : begin + length]
                turned[to : to + length, top : top + height] = left.T
            left = jnp.concatenate(
                [
                    sources[which][first : first + height, begin : begin + length]
                    for which, first, begin, length, _ in sorted(lefts, key=lambda p: p[4])
                ],
                axis=1,
            )
            total = total + jnp.dot(seen, left, preferred_element_type=F32)
            top += height
        for which, group in ready:
            height = sum(part[0] for part in group)
            seen = rows_ref[:, at_row + top : at_row + top + height].astype(BF16)
            total = total + lax.dot_general(
                seen, sources[which][...], (((1,), (1,)), ((), ())), preferred_element_type=F32
            )
            top += height
        half_sums = len(before) // 2
        for h in range(halves):
            part = total[:, h * width : (h + 1) * width]
            for extra in sums[half_sums:]:
                part = part + extra[...]
            outs[halves + h][...] = part
        copies = [None, None]
        for t in range(steps):
            begin = t * step

            def cut(group):
                pieces = []
                for height, cols in group:
                    for which, first, start, length, to in cols:
                        if to <= begin < to + length:
                            at = start + begin - to
                            pieces.append(sources[which][first : first + height, at : at + step])
                return jnp.concatenate(pieces, axis=0)

            right = cut([(height, cols) for height, _, cols in blocks])
            rights = [(which, cut(group)) for which, group in ready]
            for h in range(halves):
                part = jnp.dot(
                    turned[h * width : (h + 1) * width, :], right, preferred_element_type=F32
                )
                for which, other in rights:
                    part = part + jnp.dot(
                        sources[which][...], other, preferred_element_type=F32
                    )
                for extra in sums[:half_sums]:
                    part = part + extra[:, begin : begin + step]
                if not out_far:
                    outs[h][:, begin : begin + step] = part
                    continue
                tile, sems = scratch[1:]
                slot = t % 2
                if copies[slot] is not None:
                    copies[slot].wait()
                tile[slot] = part
                copies[slot] = pltpu.make_async_copy(
                    tile.at[slot], outs[0].at[:, pl.ds(begin, step)], sems.at[slot]
                )
                copies[slot].start()
        for copy in copies:
            if copy is not None:
                copy.wait()

    scratch_shapes = [pltpu.VMEM((left_width, depth), BF16)]
    scratch_bytes = 2 * left_width * depth
    if out_far:
        scratch_shapes += [pltpu.VMEM((2, width, step), F32), pltpu.SemaphoreType.DMA((2,))]
        scratch_bytes += 8 * width * step
    return pl.pallas_call(
        kernel,
        in_specs=[VMEM] * (count + 1 + len(before)),
        out_specs=[ANY if out_far else VMEM] * halves + [VMEM] * halves,
        out_shape=[jax.ShapeDtypeStruct((width, cols_width), F32)] * halves
        + [jax.ShapeDtypeStruct((8, width), F32)] * halves,
        scratch_shapes=scratch_shapes,
        cost_estimate=pl.CostEstimate(
            flops=2 * total_depth * left_width * cols_width,
            bytes_accessed=2 * 10**7,
            transcendentals=0,
        ),
        compiler_params=pltpu.CompilerParams(
            vmem_limit_bytes=max(scratch_bytes + (4 << 20), 9 << 20)
        ),
    )(*operands, rows, *before)


def on_device_square(
    rows_axis,
    cols_axis,
    design,
    observations,
    gaps,
    noise_var,
    arc_lengths,
    arc_amp,
    arc_decay,
    plan,
    tile_map,
):
    block_rows, columns = design.shape
    tiles = tile_map.shape[0]
    size = columns // tiles
    own = (tiles // rows_axis) * size
    wide = 2 * own
    cols_width = (tiles // cols_axis) * size
    half = cols_width // 2
    row, col = lax.axis_index("row"), lax.axis_index("col")
    last = cols_axis - 1
    at_end = jnp.logical_or(col == 0, col == last)
    where = jnp.stack([row, col, at_end.astype(jnp.int32)]).astype(jnp.int32)

    def hop(x, pairs):
        return lax.ppermute(x, "col", pairs)

    def cross(x, mask):
        return hop(x, [(c, c ^ mask) for c in range(cols_axis)])

    def swap(x, mask):
        return lax.ppermute(x, "row", [(r, r ^ mask) for r in range(rows_axis)])

    outward = [(1, 0), (last - 1, last)]
    inward = [(last, 1), (0, last - 1)]
    beside = cross(design, 1)
    inner = hop(design, [(1, last - 1), (last - 1, 1)])
    outer = hop(inner, outward)
    near, *parts = head(
        design,
        (observations, gaps, noise_var),
        (arc_lengths, arc_amp, arc_decay),
        tile_map,
        where,
        rows_axis,
        cols_axis,
    )
    line = [near] + [cross(near, s) for s in range(1, cols_axis)]
    line_obs = jnp.stack([part[block_rows] for part in line])
    obs = [line_obs] + [swap(line_obs, 2 * n) for n in range(1, 4)]
    obs_all = obs + [swap(jnp.concatenate(obs, axis=0), 1)]

    def trade(xa, xb, ya, yb, keep):
        xa, ya = swap(xa, 2), swap(ya, 4)
        xb, yb = swap(xb, 2), swap(yb, 4)
        return keep, xa, xb, ya, yb, swap(xa, 4), swap(ya, 2)

    traded = [trade(*parts[:5])]
    sources = ([beside], [line[1]]), ([inner, outer], [line[3], line[2]])
    for s, (raw, nears) in enumerate(sources, 1):
        cut = pack_cut(raw, nears, tile_map, where, rows_axis, cols_axis)
        traded.append(trade(*cut))

    keep, _, xb, _, yb, fa, fb = traded[0]
    lead, rest = row_parts(keep, xb, yb, fa, fb, own)
    far_ends = hop(parts[5], [(last, 0), (0, last)])
    far_inner = hop(parts[6], inward)
    far_cols = jnp.where(at_end, far_ends, far_inner)
    rest_inner = hop(rest, inward)
    lead_inner = hop(lead, inward)
    far_rest = jnp.where(at_end, hop(rest_inner, outward), rest_inner)
    far_lead = jnp.where(at_end, hop(lead_inner, outward), lead_inner)
    x3, y3 = swap(far_cols, 2), swap(far_cols, 4)
    fa3 = swap(x3[:, :half], 4)
    fb3 = swap(y3[:, half:], 2)

    def part_blocks(first, height, left, both):
        wide_left = wide if both else own
        begin = 0 if both else left * own
        blocks = []
        for k in (0, 2, 4):
            blocks.append([height, [(first + k, 0, begin, wide_left, 0)], []])
        corner = [(first + 5 + left, 0, 0, own, 0)]
        if both:
            corner.append((first + 6, 0, 0, own, own))
        blocks.append([height, corner, []])
        for n, k, begin, length, to in (
            (0, 0, wide, cols_width, 0),
            (1, 1, own, half, 0),
            (1, 2, wide, half, half),
            (2, 4, wide, half, 0),
            (2, 3, own, half, half),
            (3, 5, own, half, 0),
            (3, 6, own, half, half),
        ):
            blocks[n][2].append((first + k, 0, begin, length, to))
        return blocks

    early = [(2 * n, s) for s in range(last - 1) for n in range(4)]
    mid = [(2 * n + core, last - 1) for core in (0, 1) for n in range(3)]
    late = [(6 + core, last - 1) for core in (0, 1)]
    late += [(2 * n + core, last) for core in (0, 1) for n in range(4)]
    rows_early, _ = obs_rows(obs, early, plan, where, cols_axis, False)
    rows, balanced_obs = obs_rows(obs_all, mid + late, plan, where, cols_axis, True)

    blocks, operands = [], []
    for s in range(last - 1):
        blocks += part_blocks(len(operands), block_rows, 0, True)
        operands += list(traded[s])
    keep, give, keep_rhs, give_rhs = gram_direct(
        blocks, [], operands, rows_early, 0, wide, cols_width, (), 2, False
    )
    other = swap(give, 1)
    other_rhs = swap(give_rhs, 1)

    mine = list(traded[last - 1])
    theirs = [swap(v, 1) for v in mine]
    sides = [part_blocks(0, block_rows, 0, False), part_blocks(5, block_rows, 1, False)]
    most, most_rhs = gram_direct(
        sides[0][:3] + sides[1][:3],
        [],
        mine[:5] + theirs[:5],
        rows,
        0,
        own,
        cols_width,
        (keep, other, keep_rhs, other_rhs),
        1,
        False,
    )
    at_row = len(mid) * block_rows
    mine_far = [far_cols, x3, y3, fa3, fb3]
    theirs_far = [swap(v, 1) for v in mine_far]
    their_rest = swap(far_rest, 1)
    corners, ready = [], []
    operands = []
    for core, group in enumerate((mine, theirs)):
        cols = [(len(operands), 0, own, half, 0), (len(operands) + 1, 0, own, half, half)]
        corners.append((block_rows, [(len(operands) + core, 0, 0, own, 0)], cols))
        operands += group[5:]
    for left, group in ((far_lead, mine_far), (their_rest, theirs_far)):
        first = len(operands)
        operands += [left] + group
        plain = [(block_rows, [(first + 1 + n, 0, 0, cols_width, 0)]) for n in range(3)]
        plain.append((block_rows, [(first + 4, 0, 0, half, 0), (first + 5, 0, 0, half, half)]))
        ready.append((first, plain))
    gram, rhs = gram_direct(
        corners, ready, operands, rows, at_row, own, cols_width, (most, most_rhs), 1, True
    )
    return (gram, rhs[0], balanced_obs)


def solution(mesh):
    placed = (
        P(("row", "col"), None),
        P(("row", "col")),
        P(("row", "col")),
        P(("row", "col")),
        P(("row", "col"), None),
        P(("row", "col"), None),
        P(("row", "col"), None),
        P(("row", "col")),
        P(),
    )
    rows_axis, cols_axis = mesh.shape["row"], mesh.shape["col"]
    square = rows_axis == 2**3 and cols_axis == 2**2

    def body(*args):
        if not square:
            return on_device_any(rows_axis, cols_axis, *args)
        return on_device_square(rows_axis, cols_axis, *args)

    return jax.shard_map(
        body,
        mesh=mesh,
        in_specs=placed,
        out_specs=(P("row", "col"), P("row"), P(("row", "col"), None)),
        check_vma=False,
    )
```
